128 devices in a mesh: rows: 32 (over y, x, core), cols: 4 (over z).
Axes of the slice: x: 4, y: 4, z: 4, core: 2. Of those that a mesh axis runs over, the one named last changes fastest.
Arguments:
- terminal_value: float32 [4096, 2048], P('rows', 'cols'), may hold values from -6 to 6
- density_start: float32 [4096, 2048], P('rows', 'cols'), may hold values from 0.2 to 3
- start_cells: int32 [524288], P(('rows', 'cols')), may hold values from 0 to 65535
- offsets: float32 [2, 524288], P(None, ('rows', 'cols')), may hold values from -4 to 4
- weights: float32 [524288], P(('rows', 'cols')), may hold values from 0.3 to 9
- dest_tiles: int32 [4096], P(('rows', 'cols')), may hold values from 0 to 127, as said below
- end_cells: int32 [524288], P(('rows', 'cols')), may hold values from 0 to 65535
Outputs:
- value: float32 [4096, 2048], P('rows', 'cols')
- density: float32 [4096, 2048], P('rows', 'cols')
The draws below stay inside these ranges and needn't reach their ends.
Inputs may be any that keep to these rules, and one draw needn't show every extreme that they name: `dest_tiles`: block b's tile lies in the band of the tile where b starts or in a band next to it. At most 8 blocks that start in one tile go to any one tile, and for every starting tile there is one destination tile that receives exactly 8 of its blocks.
All inputs are finite; a program needn't handle non-finite values.
Results may differ from the reference program's by a relative error of at most 0.0003.
Values sent between devices are 32-bit elements; how exact they have to be, the bound alone decides.
A program may use at most 64 MiB of HBM per device.

```python
import math
import jax
import jax.numpy as jnp

TR = 128
TC = 512
BLOCK = 128
BLOCKS_DEV = 32
CAP = 8
HJB_STEPS = 4
ITERS = 2
NX = 4096
NY = 2048
AGENTS = 524288
N_ROWS = 32
N_COLS = 4


def draw_weights(key, part):
    agent = jnp.arange(AGENTS, dtype=jnp.int32)
    tile = agent // (BLOCK * BLOCKS_DEV)
    band = tile // N_COLS
    ramp = 1.0 + 2.0 * band.astype(jnp.float32) / (N_ROWS - 1)
    base = jnp.exp(jax.random.uniform(key, (AGENTS,), jnp.float32, jnp.log(0.5), jnp.log(2.0)))
    return (base * ramp).astype(jnp.float32)


def draw_dest_tiles(key, part):
    tile_list = N_ROWS * N_COLS
    choices_count = 3 * N_COLS
    agent_tokens = choices_count * CAP
    random_keys = jax.random.split(jax.random.fold_in(key, 7), 5)
    device = jnp.arange(tile_list, dtype=jnp.int32)
    band = device // N_COLS
    main_band = jnp.clip(band + jax.random.randint(random_keys[0], (tile_list,), -1, 2), 0, N_ROWS - 1)
    main_col = jax.random.randint(random_keys[1], (tile_list,), 0, N_COLS)
    main_pick = (main_band - band + 1) * N_COLS + main_col
    token = jnp.arange(agent_tokens, dtype=jnp.int32)
    pick = token // CAP
    cand_band = band[:, None] + pick[None, :] // N_COLS - 1
    cand_col = jnp.broadcast_to(pick[None, :] % N_COLS, (tile_list, agent_tokens))
    valid = (cand_band >= 0) & (cand_band < N_ROWS)
    candidate_tile = jnp.clip(cand_band, 0, N_ROWS - 1) * N_COLS + cand_col
    preference = jax.random.randint(random_keys[2], (tile_list,), 0, 3)
    reward_extra = preference[candidate_tile] * 400
    tile_rating = jax.random.randint(random_keys[3], (tile_list, agent_tokens), 0, 1024) - reward_extra
    tile_rating = jnp.where(pick[None, :] == main_pick[:, None], -2000, tile_rating)
    tile_rating = jnp.where(valid, tile_rating, 4096)
    tile_rating = (tile_rating + 4096) * agent_tokens + token[None, :]
    order = jnp.argsort(tile_rating, axis=1)[:, :BLOCKS_DEV]
    chosen = jnp.take_along_axis(candidate_tile, order, axis=1)
    mixing = jax.random.randint(random_keys[4], (tile_list, BLOCKS_DEV), 0, 1 << 20) * BLOCKS_DEV
    mixing = mixing + jnp.arange(BLOCKS_DEV, dtype=jnp.int32)[None, :]
    shuffle = jnp.argsort(mixing, axis=1)
    chosen = jnp.take_along_axis(chosen, shuffle, axis=1)
    return chosen.reshape(-1).astype(jnp.int32)


def touch_ends(result, stream_key, smallest, high):
    longest = result.shape.index(max(result.shape))
    spots = []
    for shift in (0, 1):
        where = [jax.random.randint(jax.random.fold_in(stream_key, axis), (), 0, length) for axis, length in enumerate(result.shape)]
        where[longest] = (where[longest] + shift) % result.shape[longest]
        spots.append(tuple(where))
    return result.at[spots[0]].set(smallest).at[spots[1]].set(high)


def block_scale(rng, dims, cuts, low, top_value):
    loudness, own = 1.0, jax.random.fold_in(rng, 6)
    for axis_at, shards_of in cuts:
        steps = jnp.exp(jax.random.uniform(jax.random.fold_in(own, axis_at), (shards_of,), jnp.float32, low / len(cuts), top_value / len(cuts)))
        loudness = loudness * jnp.repeat(steps, dims[axis_at] // shards_of).reshape([-1 if axis == axis_at else 1 for axis in range(len(dims))])
    return loudness


def normal_values(own_key, extent, width, bound, shards=(), kind=jnp.bfloat16):
    array = width * jax.random.normal(own_key, extent, jnp.float32)
    if shards:
        array = array * block_scale(own_key, extent, shards, -0.22, 0.18)
    return jnp.clip(array, -bound, bound).astype(kind)


def setup_inputs(seed: int = 0) -> dict:
    key_list = jax.random.split(jax.random.key(seed), 8)
    return {
        "terminal_value": normal_values(key_list[0], (NX, NY), 1.0, 6.0, ((0, 32), (1, 4)), jnp.float32),
        "density_start": jnp.clip(jnp.exp(math.log(3.0) - 2.7080502 * jax.random.uniform(key_list[1], (NX, NY), jnp.float32) ** block_scale(key_list[1], (NX, NY), ((0, 32), (1, 4)), -0.2, 0.2)), 0.2, 3.0),
        "start_cells": touch_ends(jax.random.randint(key_list[2], (AGENTS,), 0, TR * TC), jax.random.fold_in(key_list[2], 1), 0, (TR * TC) - 1).astype(jnp.int32),
        "offsets": normal_values(key_list[3], (2, AGENTS), 1.0, 4.0, ((1, 128),), jnp.float32),
        "weights": draw_weights(jax.random.fold_in(key_list[7], 71), 0),
        "dest_tiles": draw_dest_tiles(jax.random.fold_in(key_list[7], 71), 0),
        "end_cells": touch_ends(jax.random.randint(key_list[6], (AGENTS,), 0, TR * TC), jax.random.fold_in(key_list[6], 1), 0, (TR * TC) - 1).astype(jnp.int32),
    }


def hjb_step(value, density):
    padded = jnp.pad(value, 1)
    up = padded[:-2, 1:-1]
    down = padded[2:, 1:-1]
    left = padded[1:-1, :-2]
    right = padded[1:-1, 2:]
    back_x = jnp.maximum(value - up, 0.0)
    fore_x = jnp.minimum(down - value, 0.0)
    back_y = jnp.maximum(value - left, 0.0)
    fore_y = jnp.minimum(right - value, 0.0)
    square_x = jnp.maximum(back_x * back_x, fore_x * fore_x)
    square_y = jnp.maximum(back_y * back_y, fore_y * fore_y)
    spread = up + down + left + right - 4.0 * value
    return value + 0.25 * (0.5 * spread - 0.5 * (square_x + square_y) + 0.5 * density)


def reference(terminal_value, density_start, start_cells, offsets, weights, dest_tiles, end_cells):
    per_tile = BLOCK * BLOCKS_DEV
    agent = jnp.arange(AGENTS, dtype=jnp.int32)
    source = agent // per_tile
    row_start = (source // N_COLS) * TR + start_cells // TC
    col_start = (source % N_COLS) * TC + start_cells % TC
    target = jnp.repeat(dest_tiles, BLOCK)
    row_end = (target // N_COLS) * TR + end_cells // TC
    col_end = (target % N_COLS) * TC + end_cells % TC
    row_next = jnp.minimum(row_end + 1, NX - 1).astype(jnp.int32)
    col_next = jnp.minimum(col_end + 1, NY - 1).astype(jnp.int32)
    frac_x = 0.5 + 0.45 * jnp.tanh(offsets[0])
    frac_y = 0.5 + 0.45 * jnp.tanh(offsets[1])
    total = jnp.sum(weights)
    density = density_start
    value = terminal_value
    for outer in range(ITERS):
        value = terminal_value
        for inner in range(HJB_STEPS):
            value = hjb_step(value, density)
        padded = jnp.pad(value, 1)
        corner_a = padded[row_start + 1, col_start + 1]
        corner_b = padded[row_start + 2, col_start + 1]
        corner_c = padded[row_start + 1, col_start + 2]
        corner_d = padded[row_start + 2, col_start + 2]
        grad_x = (1.0 - frac_y) * (corner_b - corner_a) + frac_y * (corner_d - corner_c)
        grad_y = (1.0 - frac_x) * (corner_c - corner_a) + frac_x * (corner_d - corner_b)
        moved_x = 0.5 + 0.45 * jnp.tanh(offsets[0] - grad_x)
        moved_y = 0.5 + 0.45 * jnp.tanh(offsets[1] - grad_y)
        deposit = jnp.zeros((NX, NY), jnp.float32)
        deposit = deposit.at[row_end, col_end].add(weights * (1.0 - moved_x) * (1.0 - moved_y))
        deposit = deposit.at[row_next, col_end].add(weights * moved_x * (1.0 - moved_y))
        deposit = deposit.at[row_end, col_next].add(weights * (1.0 - moved_x) * moved_y)
        deposit = deposit.at[row_next, col_next].add(weights * moved_x * moved_y)
        fresh = deposit * (NX * NY / total)
        density = 0.5 * density + 0.5 * fresh
    return value, density
```

```python
import functools

import jax
import jax.numpy as jnp
from jax import lax
from jax.experimental import pallas as pl
from jax.experimental.pallas import tpu as pltpu
from jax.sharding import PartitionSpec as P

HJB_STEPS = 4
ITERS = 2
CAP = 8
RT = 16
LT = 4
DR = 144
F32 = jnp.float32
BF16 = jnp.bfloat16
I16 = jnp.int16
GROUP = 12
SELF = 4


def hjb_step(src, dst, den, lane, sub, row_in, side_in):
    tiles, n_t, n_j = {}, RT + 2, LT + 1
    rolled = {}

    def cell(t, j):
        if (t, j) not in tiles:
            tiles[t, j] = src[t, :, 128 * j : 128 * j + 128]
        return tiles[t, j]

    def roll(t, j, shift, axis):
        key = (t, j, shift, axis)
        if key not in rolled:
            rolled[key] = pltpu.roll(cell(t, j), shift, axis)
        return rolled[key]

    for t in range(n_t):
        for j in range(n_j):
            v = cell(t, j)
            up = jnp.where(sub == 0, roll((t - 1) % n_t, j, 1, 0), roll(t, j, 1, 0))
            down = jnp.where(sub == 7, roll((t + 1) % n_t, j, 7, 0), roll(t, j, 7, 0))
            left = jnp.where(lane == 0, roll(t, (j - 1) % n_j, 1, 1), roll(t, j, 1, 1))
            right = jnp.where(lane == 127, roll(t, (j + 1) % n_j, 127, 1), roll(t, j, 127, 1))
            px = jnp.maximum(v - jnp.minimum(up, down), 0.0)
            py = jnp.maximum(v - jnp.minimum(left, right), 0.0)
            spread = up + down + left + right - 4.0 * v
            d = den[t, :, 128 * j : 128 * j + 128]
            new = v + 0.25 * (0.5 * spread - 0.5 * (px * px + py * py) + 0.5 * d)
            if t >= RT:
                new = jnp.where(row_in[t - RT], new, 0.0)
            if j == LT:
                new = jnp.where(side_in, new, 0.0)
            dst[t, :, 128 * j : 128 * j + 128] = new


def sample(u, u1, cells, corners):
    zero = jnp.zeros((8, 128), F32)

    def agents(a, carry):
        cell = cells[a]
        key = cell >> 7
        idx = cell & 127
        u00, u10, u01, u11 = zero, zero, zero, zero
        for r in range(8 * RT + 1):
            for j in range(LT):
                part = (r // 8, slice(r % 8, r % 8 + 1), slice(128 * j, 128 * j + 128))
                here = jnp.take_along_axis(jnp.broadcast_to(u[part], (8, 128)), idx, axis=1)
                next_ = jnp.take_along_axis(jnp.broadcast_to(u1[part], (8, 128)), idx, axis=1)
                if r < 8 * RT:
                    hit = key == r * LT + j
                    u00 = jnp.where(hit, here, u00)
                    u01 = jnp.where(hit, next_, u01)
                if r > 0:
                    hit = key == (r - 1) * LT + j
                    u10 = jnp.where(hit, here, u10)
                    u11 = jnp.where(hit, next_, u11)
        for n, v in enumerate((u00, u10, u01, u11)):
            corners[n, a] = v
        return carry

    lax.fori_loop(0, 4, agents, 0)


def exact_parts(v):
    high = v.astype(BF16)
    rest = v - high.astype(F32)
    mid = rest.astype(BF16)
    return high, mid, (rest - mid.astype(F32)).astype(BF16)


def place(placing, v):
    out = None
    for part in exact_parts(v):
        term = jnp.dot(placing, part, preferred_element_type=F32)
        out = term if out is None else out + term
    return out


def build_and_add(static, moves, lhs, hot, acc):
    cell = static[0].astype(jnp.int32)
    mass = static[1]
    x, y = moves[0], moves[1]
    row, col = cell >> 9, cell & 511
    upper, lower = mass * (1.0 - x), mass * x
    row_iota = lax.broadcasted_iota(I16, (DR, 128), 0)
    col_iota = lax.broadcasted_iota(I16, (512, 128), 0)
    parts = []
    for v in (upper * (1.0 - y), lower * (1.0 - y), upper * y, lower * y):
        high = v.astype(BF16).astype(F32)
        parts.append((high, v - high))

    def spread(v, b, dtype, copies):
        tile = jnp.broadcast_to(v[b : b + 1], (16, 128)).astype(dtype)
        return jnp.tile(tile, (copies, 1))

    for b in range(CAP):
        r = spread(row, b, I16, DR // 16)
        q = spread(col, b, I16, 32)
        on_upper = row_iota == r
        on_lower = row_iota == r + I16(1)
        for kind in range(2):
            for p in range(2):
                v = spread(parts[2 * kind][p], b, BF16, DR // 16)
                w = spread(parts[2 * kind + 1][p], b, BF16, DR // 16)
                lhs[pl.ds((2 * kind + p) * DR, DR), pl.ds(128 * b, 128)] = jnp.where(
                    on_upper, v, jnp.where(on_lower, w, BF16(0))
                )
        hot[:, pl.ds(128 * b, 128)] = jnp.where(col_iota == q, BF16(1), BF16(0))
    acc[...] += lax.dot_general(
        lhs[...], hot[...], (((1,), (1,)), ((), ())), preferred_element_type=F32
    )


def kernel(
    n_rows, n_cols,
    u_in, m_in, cells_in, off_in, w_in, dest_in, end_in,
    value_out, density_out,
    um, ua, ub, grid, cells, off_raw, off, frac, w, ends, dest, corners,
    side_send, side_recv, corner_recv,
    static_send, static_recv, move_send, move_recv,
    lhs, hot, acc,
    g_side_l, g_side_r, g_from_u, g_from_d, g_from_l, g_from_r, g_from_ul, g_from_ur, g_from_dl, g_from_dr,
    red_send, red_recv, result,
    load_sem, out_sem,
    halo_s, halo_r, static_s, static_r, move_s, move_r, g_s, g_r, red_s, red_r,
):
    row = lax.axis_index("rows")
    col = lax.axis_index("cols")

    def at(dr, dc):
        return (lax.rem(row + dr + n_rows, n_rows), lax.rem(col + dc + n_cols, n_cols))

    def remote(src, dst, s, r, to):
        return pltpu.make_async_remote_copy(
            src_ref=src, dst_ref=dst, send_sem=s, recv_sem=r,
            device_id=to, device_id_type=pl.DeviceIdType.MESH,
        )

    loads = [
        (u_in, um.at[0, pl.ds(0, RT), :, pl.ds(0, 512)]),
        (m_in, um.at[1, pl.ds(0, RT), :, pl.ds(0, 512)]),
        (dest_in, dest), (w_in, w), (end_in, ends), (off_in, off_raw), (cells_in, cells),
    ]
    loads = [pltpu.make_async_copy(a, b, load_sem.at[i]) for i, (a, b) in enumerate(loads)]
    for c in loads:
        c.start()

    group = [(dr, k) for dr in (-1, 0, 1) for k in range(n_cols)]
    near = row % 8
    base = row - near
    row_peers = [base + (near + j) % 8 for j in range(1, 8)]
    far_peers = [lax.rem(row + 8 * j, n_rows) for j in range(1, 4)]

    barrier = pltpu.get_barrier_semaphore()
    greet = [at(dr, k) for dr, k in group if (dr, k) != (0, 0)]
    greet += [(p, col) for p in row_peers + far_peers]
    for to in greet:
        pl.semaphore_signal(barrier, inc=1, device_id=to, device_id_type=pl.DeviceIdType.MESH)

    lane = lax.broadcasted_iota(jnp.int32, (8, 128), 1)
    sub = lax.broadcasted_iota(jnp.int32, (8, 128), 0)
    has_up, has_down = row > 0, row < n_rows - 1
    has_left, has_right = col > 0, col < n_cols - 1
    row_in = (has_down, has_up)
    lane_right = lane < jnp.where(has_right, 8, 0)
    lane_left = lane >= jnp.where(has_left, 120, 128)
    side_in = lane_right | lane_left

    for c in loads[:2]:
        c.wait()
    for v in range(2):
        first = um[v, 0:RT, :, 0:128].reshape(128, 128).T
        last = um[v, 0:RT, :, 384:512].reshape(128, 128).T
        side_send[0, v] = first[0:8]
        side_send[1, v] = last[120:128]
    pl.semaphore_wait(barrier, len(greet))

    halo = [
        remote(um.at[:, 0, :, pl.ds(0, 512)], um.at[:, RT, :, pl.ds(0, 512)], halo_s.at[0], halo_r.at[0], at(-1, 0)),
        remote(um.at[:, RT - 1, :, pl.ds(0, 512)], um.at[:, RT + 1, :, pl.ds(0, 512)], halo_s.at[1], halo_r.at[1], at(1, 0)),
        remote(um.at[:, 0, :, pl.ds(0, 128)], corner_recv.at[0], halo_s.at[2], halo_r.at[2], at(-1, -1)),
        remote(um.at[:, 0, :, pl.ds(384, 128)], corner_recv.at[1], halo_s.at[3], halo_r.at[3], at(-1, 1)),
        remote(um.at[:, RT - 1, :, pl.ds(0, 128)], corner_recv.at[2], halo_s.at[4], halo_r.at[4], at(1, -1)),
        remote(um.at[:, RT - 1, :, pl.ds(384, 128)], corner_recv.at[3], halo_s.at[5], halo_r.at[5], at(1, 1)),
        remote(side_send.at[0], side_recv.at[0], halo_s.at[6], halo_r.at[6], at(0, -1)),
        remote(side_send.at[1], side_recv.at[1], halo_s.at[7], halo_r.at[7], at(0, 1)),
    ]
    for c in halo:
        c.start()

    loads[3].wait()
    red_send[0] = w[0] + w[1] + w[2] + w[3]
    stages = [
        [(0, at(0, k)) for k in range(1, n_cols)],
        [(1, (p, col)) for p in row_peers],
        [(2, (p, col)) for p in far_peers],
    ]
    red, count = [], 0
    for stage in stages:
        copies = []
        for s, to in stage:
            copies.append(remote(red_send.at[s], red_recv.at[count], red_s.at[count], red_r.at[count], to))
            count += 1
        red.append(copies)
    for c in red[0]:
        c.start()

    def reduce_stage(s):
        total, first = red_send[s], sum(len(x) for x in red[:s])
        for i, c in enumerate(red[s]):
            c.wait()
            total = total + red_recv[first + i]
        if s + 1 < len(red):
            red_send[s + 1] = total
            for c in red[s + 1]:
                c.start()
        return total

    loads[2].wait()
    d = dest[...]
    along = jnp.broadcast_to(d.astype(F32), (32, 32))
    same = along == along.T
    order_b = lax.broadcasted_iota(jnp.int32, (32, 32), 0)
    order_a = lax.broadcasted_iota(jnp.int32, (32, 32), 1)
    rank = jnp.sum(jnp.where(same & (order_b < order_a), 1.0, 0.0), axis=0, keepdims=True).astype(jnp.int32)
    slot = ((d >> 2) - row + 1) * (n_cols * CAP) + (((d & 3) - col) & 3) * CAP + rank
    slot_iota = lax.broadcasted_iota(jnp.int32, (GROUP * CAP, 32), 0)
    placing = jnp.where(slot_iota == slot, 1.0, 0.0).astype(BF16)

    def send_group(send, recv, ss, rs):
        copies = {}
        for i, (dr, k) in enumerate(group):
            if i != SELF:
                copies[i] = remote(send.at[i], recv.at[i], ss.at[i], rs.at[i], at(dr, k))
                copies[i].start()
        return copies

    loads[4].wait()
    block_static = jnp.concatenate(
        [ends[...].reshape(32, 128).astype(F32), w[...].reshape(32, 128)], axis=1
    )
    placed = place(placing, block_static)
    for n in range(2):
        static_send[:, n] = placed[:, 128 * n : 128 * n + 128].reshape(GROUP, CAP, 128)
    for n in range(2):
        static_recv[SELF, n] = placed[SELF * CAP : SELF * CAP + CAP, 128 * n : 128 * n + 128]
    static_copies = send_group(static_send, static_recv, static_s, static_r)

    loads[5].wait()
    loads[6].wait()
    for b in range(32):
        both = off_raw[:, 128 * b : 128 * b + 128]
        for n in range(2):
            off[n, b // 8, b % 8 : b % 8 + 1, :] = both[n : n + 1]
    for n in range(2):
        frac[n] = 0.5 + 0.45 * jnp.tanh(off[n])

    for c in halo:
        c.wait()
    zero_mid = jnp.zeros((112, 128), F32)
    for v in range(2):
        strip = jnp.concatenate([side_recv[0, v], zero_mid, side_recv[1, v]], axis=0).T
        strip = strip.reshape(RT, 8, 128)
        um[v, 0:RT, :, 512:640] = jnp.where(side_in, strip, 0.0) if v == 0 else strip
        below = jnp.where(lane < 64, corner_recv[0, v], corner_recv[1, v])
        above = jnp.where(lane < 64, corner_recv[2, v], corner_recv[3, v])
        if v == 0:
            below = jnp.where(side_in & has_down, below, 0.0)
            above = jnp.where(side_in & has_up, above, 0.0)
            um[0, RT, :, 0:512] = jnp.where(has_down, um[0, RT, :, 0:512], 0.0)
            um[0, RT + 1, :, 0:512] = jnp.where(has_up, um[0, RT + 1, :, 0:512], 0.0)
        um[v, RT, :, 512:640] = below
        um[v, RT + 1, :, 512:640] = above

    def exchange(it):
        full = it + 1 < ITERS
        ss, rs = g_s.at[it], g_r.at[it]
        third = grid[0:RT, :, 384:512].reshape(128, 128).T
        fourth = grid[0:RT, :, 512:640].reshape(128, 128).T
        g_side_r[it, 0] = third[120:128]
        g_side_r[it, 1] = fourth[0:8]
        g_side_r[it, 2] = grid[RT, :, 384:512]
        g_side_r[it, 3] = grid[RT, :, 512:640]
        if full:
            first = grid[0:RT, :, 0:128].reshape(128, 128).T
            g_side_l[0] = first[0:8]
            g_side_l[1] = grid[RT, :, 0:128]
        copies = [
            remote(grid.at[pl.ds(RT - 1, 2)], g_from_u.at[it], ss.at[0], rs.at[0], at(1, 0)),
            remote(g_side_r.at[it], g_from_l.at[it], ss.at[1], rs.at[1], at(0, 1)),
            remote(grid.at[pl.ds(RT - 1, 2), :, pl.ds(384, 256)], g_from_ul.at[it], ss.at[2], rs.at[2], at(1, 1)),
        ]
        if full:
            copies += [
                remote(grid.at[0], g_from_d, ss.at[3], rs.at[3], at(-1, 0)),
                remote(g_side_l, g_from_r, ss.at[4], rs.at[4], at(0, -1)),
                remote(grid.at[pl.ds(RT - 1, 2), :, pl.ds(0, 128)], g_from_ur, ss.at[5], rs.at[5], at(1, -1)),
                remote(grid.at[0, :, pl.ds(384, 256)], g_from_dl, ss.at[6], rs.at[6], at(-1, 1)),
                remote(grid.at[0, :, pl.ds(0, 128)], g_from_dr, ss.at[7], rs.at[7], at(-1, -1)),
            ]
        for c in copies:
            c.start()
        return copies

    def gather_edges(it):
        full = it + 1 < ITERS
        top = sub == 0
        left0 = (lane == 0) & has_left
        l4, z = slice(512, 640), 0.0
        grid[RT + 1] = jnp.where(has_up, g_from_u[it, 0], z)
        for j in range(LT + 1):
            js = slice(128 * j, 128 * j + 128)
            grid[0, :, js] += jnp.where(top & has_up, g_from_u[it, 1, :, js], z)
        if full:
            grid[RT] += jnp.where(has_down, g_from_d[...], z)
        right_rows = g_from_r[0] if full else jnp.zeros((8, 128), F32)
        strip = jnp.concatenate([right_rows, zero_mid, g_from_l[it, 0]], axis=0).T.reshape(RT, 8, 128)
        grid[0:RT, :, l4] += jnp.where(side_in, strip, z)
        spill = jnp.concatenate([g_from_l[it, 1], jnp.zeros((120, 128), F32)], axis=0).T.reshape(RT, 8, 128)
        grid[0:RT, :, 0:128] += jnp.where(left0, spill, z)
        edge = jnp.where(lane_left, g_from_l[it, 2], z)
        if full:
            edge = edge + jnp.where(lane_right, g_from_r[1], z)
        grid[RT, :, l4] += edge
        grid[RT, :, 0:128] += jnp.where(left0, g_from_l[it, 3], z)
        corner = jnp.where(lane_left, g_from_ul[it, 0, :, 0:128], z)
        corner_top = jnp.where(lane_left, g_from_ul[it, 1, :, 0:128], z)
        if full:
            corner = corner + jnp.where(lane_right, g_from_ur[0], z)
            corner_top = corner_top + jnp.where(lane_right, g_from_ur[1], z)
        grid[RT + 1, :, l4] += jnp.where(has_up, corner, z)
        grid[RT + 1, :, 0:128] += jnp.where(left0 & has_up, g_from_ul[it, 0, :, 128:256], z)
        grid[0, :, l4] += jnp.where(top & has_up, corner_top, z)
        grid[0, :, 0:128] += jnp.where(top & left0 & has_up, g_from_ul[it, 1, :, 128:256], z)
        if full:
            corner = jnp.where(lane_left, g_from_dl[:, 0:128], z) + jnp.where(lane_right, g_from_dr[...], z)
            grid[RT, :, l4] += jnp.where(has_down, corner, z)
            grid[RT, :, 0:128] += jnp.where(left0 & has_down, g_from_dl[:, 128:256], z)
        for j in range(LT + 1):
            js = slice(128 * j, 128 * j + 128)
            folded = pltpu.roll(grid[RT, :, js], 7, 0)
            grid[RT - 1, :, js] += jnp.where((sub == 7) & jnp.logical_not(has_down), folded, z)
        for t in range(RT + 2):
            folded = pltpu.roll(grid[t, :, l4], 127, 1)
            grid[t, :, 384:512] += jnp.where((lane == 127) & jnp.logical_not(has_right), folded, z)

    scale = None
    for it in range(ITERS):
        hjb = functools.partial(hjb_step, lane=lane, sub=sub, row_in=row_in, side_in=side_in)
        den = um.at[1]
        hjb(um.at[0], ua, den)
        hjb(ua, ub, den)
        hjb(ub, ua, den)
        hjb(ua, ub, den)
        if it == 0:
            reduce_stage(0)
        else:
            value_copy = pltpu.make_async_copy(ub.at[pl.ds(0, RT), :, pl.ds(0, 512)], value_out, out_sem.at[0])
            value_copy.start()
        ua[0 : RT + 1] = pltpu.roll(ub[0 : RT + 1].reshape(8 * RT + 8, 640), 639, 1).reshape(RT + 1, 8, 640)
        sample(ub, ua, cells, corners)
        dx0, dx1 = corners[1] - corners[0], corners[3] - corners[2]
        dy0, dy1 = corners[2] - corners[0], corners[3] - corners[1]
        fx, fy = frac[0], frac[1]
        gx = (1.0 - fy) * dx0 + fy * dx1
        gy = (1.0 - fx) * dy0 + fx * dy1
        hx = 0.5 + 0.45 * jnp.tanh(off[0] - gx)
        hy = 0.5 + 0.45 * jnp.tanh(off[1] - gy)
        placed = place(placing, jnp.concatenate([hx.reshape(32, 128), hy.reshape(32, 128)], axis=1))
        for n in range(2):
            move_send[it, :, n] = placed[:, 128 * n : 128 * n + 128].reshape(GROUP, CAP, 128)
            move_recv[it, SELF, n] = placed[SELF * CAP : SELF * CAP + CAP, 128 * n : 128 * n + 128]
        move_copies = send_group(move_send.at[it], move_recv.at[it], move_s.at[it], move_r.at[it])
        acc[...] = jnp.zeros_like(acc)
        if it == 0:
            reduce_stage(1)

        def arrivals(i, carry):
            s = lax.rem(i + SELF, GROUP)

            @pl.when(i > 0)
            def _():
                remote(move_send.at[it, s], move_recv.at[it, s], move_s.at[it, s], move_r.at[it, s], at(0, 1)).wait_recv()
                if it == 0:
                    remote(static_send.at[s], static_recv.at[s], static_s.at[s], static_r.at[s], at(0, 1)).wait_recv()

            build_and_add(static_recv[s], move_recv[it, s], lhs, hot, acc)
            return carry

        lax.fori_loop(0, GROUP, arrivals, 0)
        zero = jnp.zeros((DR, 128), F32)
        here = acc[0:DR] + acc[DR : 2 * DR]
        beside = acc[2 * DR : 3 * DR] + acc[3 * DR : 4 * DR]
        whole = jnp.concatenate([here, zero], axis=1) + pltpu.roll(jnp.concatenate([beside, zero], axis=1), 1, 1)
        grid[...] = whole.reshape(RT + 2, 8, 640)
        copies = exchange(it)
        if it == 0:
            total = reduce_stage(2)
            scale = jnp.float32(n_rows * n_cols * 128 * 512) / jnp.sum(total, keepdims=True)
        for c in list(move_copies.values()) + (list(static_copies.values()) if it == 0 else []):
            c.wait_send()
        for c in copies:
            c.wait()
        gather_edges(it)
        if it + 1 < ITERS:
            um[1] = 0.5 * um[1] + 0.5 * (grid[...] * scale.reshape(1, 1, 1))
        else:
            result[...] = 0.5 * um[1, 0:RT, :, 0:512] + 0.5 * (grid[0:RT, :, 0:512] * scale.reshape(1, 1, 1))
            density_copy = pltpu.make_async_copy(result, density_out, out_sem.at[1])
            density_copy.start()
            value_copy.wait()
            density_copy.wait()


def body(n_rows, n_cols, terminal_value, density_start, start_cells, offsets, weights, dest_tiles, end_cells):
    any_ = pl.BlockSpec(memory_space=pl.ANY)
    vmem = pltpu.VMEM
    dma = pltpu.SemaphoreType.DMA
    tile = jax.ShapeDtypeStruct((RT, 8, 512), F32)
    value, density = pl.pallas_call(
        functools.partial(kernel, n_rows, n_cols),
        out_shape=(tile, tile),
        in_specs=[any_] * 7,
        out_specs=(any_, any_),
        scratch_shapes=[
            vmem((2, RT + 2, 8, 640), F32), vmem((RT + 2, 8, 640), F32), vmem((RT + 2, 8, 640), F32),
            vmem((RT + 2, 8, 640), F32),
            vmem((4, 8, 128), jnp.int32), vmem((2, 4096), F32), vmem((2, 4, 8, 128), F32), vmem((2, 4, 8, 128), F32),
            vmem((4, 8, 128), F32), vmem((4, 8, 128), jnp.int32), vmem((1, 32), jnp.int32), vmem((4, 4, 8, 128), F32),
            vmem((2, 2, 8, 128), F32), vmem((2, 2, 8, 128), F32), vmem((4, 2, 8, 128), F32),
            vmem((GROUP, 2, CAP, 128), F32), vmem((GROUP, 2, CAP, 128), F32),
            vmem((ITERS, GROUP, 2, CAP, 128), F32), vmem((ITERS, GROUP, 2, CAP, 128), F32),
            vmem((4 * DR, 1024), BF16), vmem((512, 1024), BF16), vmem((4 * DR, 512), F32),
            vmem((2, 8, 128), F32), vmem((ITERS, 4, 8, 128), F32),
            vmem((ITERS, 2, 8, 640), F32), vmem((8, 640), F32), vmem((ITERS, 4, 8, 128), F32), vmem((2, 8, 128), F32),
            vmem((ITERS, 2, 8, 256), F32), vmem((2, 8, 128), F32), vmem((8, 256), F32), vmem((8, 128), F32),
            vmem((3, 8, 128), F32), vmem((13, 8, 128), F32), vmem((RT, 8, 512), F32),
            dma((7,)), dma((2,)),
            dma((8,)), dma((8,)), dma((GROUP,)), dma((GROUP,)),
            dma((ITERS, GROUP)), dma((ITERS, GROUP)), dma((ITERS, 8)), dma((ITERS, 8)), dma((13,)), dma((13,)),
        ],
        compiler_params=pltpu.CompilerParams(collective_id=0, has_side_effects=True),
        name="crowd",
    )(
        terminal_value.reshape(RT, 8, 512),
        density_start.reshape(RT, 8, 512),
        start_cells.reshape(4, 8, 128),
        offsets,
        weights.reshape(4, 8, 128),
        dest_tiles.reshape(1, 32),
        end_cells.reshape(4, 8, 128),
    )
    return value.reshape(128, 512), density.reshape(128, 512)


def solution(mesh):
    both = ("rows", "cols")
    return jax.shard_map(
        functools.partial(body, mesh.shape["rows"], mesh.shape["cols"]),
        mesh=mesh,
        in_specs=(P("rows", "cols"), P("rows", "cols"), P(both), P(None, both), P(both), P(both), P(both)),
        out_specs=(P("rows", "cols"), P("rows", "cols")),
        check_vma=False,
    )
```

```python
import functools

import jax
import jax.numpy as jnp
from jax import lax
from jax.experimental import pallas as pl
from jax.experimental.pallas import tpu as pltpu
from jax.sharding import PartitionSpec as P

HJB_STEPS = 4
ITERS = 2
CAP = 8
RT = 16
LT = 4
ORDER = ((1, 0), (2, 0), (1, 1), (1, 3), (2, 1), (2, 3), (0, 0), (1, 2), (2, 2), (0, 1), (0, 3), (0, 2))
F32 = jnp.float32
BF16 = jnp.bfloat16
I16 = jnp.int16
GROUP = 12
SELF = 4


def hjb_step(src, dst, den, lane, sub, row_in, side_in):
    tiles, n_t, n_j = {}, RT + 2, LT + 1
    rolled = {}

    def cell(t, j):
        if (t, j) not in tiles:
            tiles[t, j] = src[t, :, 128 * j : 128 * j + 128]
        return tiles[t, j]

    def roll(t, j, shift, axis):
        key = (t, j, shift, axis)
        if key not in rolled:
            rolled[key] = pltpu.roll(cell(t, j), shift, axis)
        return rolled[key]

    for t in range(n_t):
        for j in range(n_j):
            v = cell(t, j)
            up = jnp.where(sub == 0, roll((t - 1) % n_t, j, 1, 0), roll(t, j, 1, 0))
            down = jnp.where(sub == 7, roll((t + 1) % n_t, j, 7, 0), roll(t, j, 7, 0))
            left = jnp.where(lane == 0, roll(t, (j - 1) % n_j, 1, 1), roll(t, j, 1, 1))
            right = jnp.where(lane == 127, roll(t, (j + 1) % n_j, 127, 1), roll(t, j, 127, 1))
            px = jnp.maximum(v - jnp.minimum(up, down), 0.0)
            py = jnp.maximum(v - jnp.minimum(left, right), 0.0)
            spread = up + down + left + right - 4.0 * v
            d = den[t, :, 128 * j : 128 * j + 128]
            new = v + 0.25 * (0.5 * spread - 0.5 * (px * px + py * py) + 0.5 * d)
            if t >= RT:
                new = jnp.where(row_in[t - RT], new, 0.0)
            if j == LT:
                new = jnp.where(side_in, new, 0.0)
            dst[t, :, 128 * j : 128 * j + 128] = new


def slopes(u, table, lane, sub):
    def split(block, first, count):
        turned = block.T[0:count]
        high = turned.astype(BF16)
        table[pl.ds(first, count), pl.ds(0, 128)] = high
        table[pl.ds(first, count), pl.ds(128, 128)] = (turned - high.astype(F32)).astype(BF16)
    for j in range(LT + 1):
        js = slice(128 * j, 128 * j + 128)
        tiles = [u[t, :, js] for t in range(RT + 1)]
        ups = [pltpu.roll(x, 7, 0) for x in tiles]
        dx = [jnp.where(sub == 7, ups[t + 1], ups[t]) - tiles[t] for t in range(RT)]
        split(jnp.concatenate(dx, axis=0), 128 * j, 128 if j < LT else 16)
        if j < LT:
            dy = []
            for t in range(RT):
                near = pltpu.roll(tiles[t], 127, 1)
                far = pltpu.roll(u[t, :, 128 * j + 128 : 128 * j + 256], 127, 1)
                dy.append(jnp.where(lane == 127, far, near) - tiles[t])
            split(jnp.concatenate(dy, axis=0), 528 + 128 * j, 128)


def sample(table, cells, corners):
    def agents(a, carry):
        cell = cells[a]
        row, col = cell >> 9, cell & 511
        for h in range(2):
            hot, places = [], []
            for b in range(4 * h, 4 * h + 4):
                r = jnp.tile(jnp.broadcast_to(row[b : b + 1], (16, 128)).astype(I16), (8, 1))
                one = jnp.where(lax.broadcasted_iota(I16, (128, 128), 0) == r, BF16(1), BF16(0))
                hot.append(jnp.concatenate([one, one], axis=0))
                places.append(jnp.broadcast_to(col[b : b + 1], (8, 128)))
            picked = jnp.dot(table[...], jnp.concatenate(hot, axis=1), preferred_element_type=F32)
            place = jnp.concatenate(places, axis=1) - lax.broadcasted_iota(jnp.int32, (8, 512), 0)
            zero = jnp.zeros((8, 512), F32)
            d0, d1, e0 = zero, zero, zero
            for i in range(64):
                here = place == 8 * i
                x = picked[8 * i : 8 * i + 8]
                d0 = jnp.where(here, x, d0)
                d1 = jnp.where(place == 8 * i - 1, x, d1)
                e0 = jnp.where(here, picked[528 + 8 * i : 536 + 8 * i], e0)
            d1 = jnp.where(place == 511, picked[512:520], d1)
            for n, v in enumerate((d0, d1, e0)):
                v = jnp.sum(v, axis=0, keepdims=True)
                for b in range(4):
                    corners[n, a, 4 * h + b : 4 * h + b + 1, :] = v[:, 128 * b : 128 * b + 128]
        return carry
    lax.fori_loop(0, 4, agents, 0)


def exact_parts(v):
    high = v.astype(BF16)
    rest = v - high.astype(F32)
    mid = rest.astype(BF16)
    return high, mid, (rest - mid.astype(F32)).astype(BF16)


def place(placing, v):
    out = None
    for part in exact_parts(v):
        term = jnp.dot(placing, part, preferred_element_type=F32)
        out = term if out is None else out + term
    return out


def deposit(static, moves, acc):
    cell = static[0].astype(jnp.int32)
    mass = static[1]
    x, y = moves[0], moves[1]
    row, col = cell >> 9, cell & 511
    upper, lower = mass * (1.0 - x), mass * x
    row_iota = lax.broadcasted_iota(I16, (128, 128), 0)
    col_iota = lax.broadcasted_iota(I16, (512, 128), 0)
    spill_iota = lax.broadcasted_iota(I16, (16, 128), 0)
    parts = []
    for v in (upper * (1.0 - y), lower * (1.0 - y), upper * y, lower * y):
        high = v.astype(BF16).astype(F32)
        parts.append((high, v - high))

    def spread(v, b, dtype, copies):
        tile = jnp.broadcast_to(v[b : b + 1], (16, 128)).astype(dtype)
        return jnp.tile(tile, (copies, 1)) if copies > 1 else tile

    zero = BF16(0)
    masses, columns = [], []
    for b in range(CAP):
        r = spread(row, b, I16, 8)
        q = spread(col, b, I16, 32)
        on_upper = row_iota == r
        on_lower = row_iota == r + I16(1)
        spill = jnp.zeros((16, 128), BF16)
        block = []
        for n in range(4):
            kind, p = n // 2, n % 2
            v = spread(parts[2 * kind][p], b, BF16, 8)
            w = spread(parts[2 * kind + 1][p], b, BF16, 8)
            block.append(jnp.where(on_upper, v, jnp.where(on_lower, w, zero)))
            spill = jnp.where(spill_iota == I16(n), w[0:16], spill)
        block.append(jnp.where(r[0:16] == I16(127), spill, zero))
        masses.append(jnp.concatenate(block, axis=0))
        columns.append(jnp.where(col_iota == q, BF16(1), zero))
    acc[...] += lax.dot_general(
        jnp.concatenate(masses, axis=1),
        jnp.concatenate(columns, axis=1),
        (((1,), (1,)), ((), ())),
        preferred_element_type=F32,
    )


def kernel(
    n_rows, n_cols,
    u_in, m_in, cells_in, off_in, w_in, dest_in, end_in,
    value_out, density_out,
    um, ua, ub, grid, cells, off_raw, off, frac, w, ends, dest, corners, table,
    side_send, side_recv, corner_recv,
    static_send, static_recv, move_send, move_recv,
    acc,
    g_side_l, g_side_r, g_from_u, g_from_d, g_from_l, g_from_r, g_from_ul, g_from_ur, g_from_dl, g_from_dr,
    red_send, red_recv,
    load_sem,
    halo_s, halo_r, static_s, static_r, move_s, move_r, g_s, g_r, red_s, red_r,
):
    row = lax.axis_index("rows")
    col = lax.axis_index("cols")

    def at(dr, dc):
        return (lax.rem(row + dr + n_rows, n_rows), lax.rem(col + dc + n_cols, n_cols))

    def remote(src, dst, s, r, to):
        return pltpu.make_async_remote_copy(
            src_ref=src, dst_ref=dst, send_sem=s, recv_sem=r,
            device_id=to, device_id_type=pl.DeviceIdType.MESH,
        )

    loads = [
        (u_in, um.at[0, pl.ds(0, RT), :, pl.ds(0, 512)]),
        (m_in, um.at[1, pl.ds(0, RT), :, pl.ds(0, 512)]),
        (dest_in, dest), (w_in, w), (end_in, ends), (off_in, off_raw), (cells_in, cells),
    ]
    loads = [pltpu.make_async_copy(a, b, load_sem.at[i]) for i, (a, b) in enumerate(loads)]
    for c in loads:
        c.start()

    group = [(dr, k) for dr in (-1, 0, 1) for k in range(n_cols)]
    near = row % 8
    base = row - near
    row_peers = [base + (near + j) % 8 for j in range(1, 8)]
    far_peers = [lax.rem(row + 8 * j, n_rows) for j in range(1, 4)]

    barrier = pltpu.get_barrier_semaphore()
    has_up, has_down = row > 0, row < n_rows - 1
    has_left, has_right = col > 0, col < n_cols - 1

    def there(dr, dc=0):
        rows_ok = {-1: has_up, 0: None, 1: has_down}[dr]
        cols_ok = {-1: has_left, 0: None, 1: has_right}[dc]
        if rows_ok is None or cols_ok is None:
            return cols_ok if rows_ok is None else rows_ok
        return rows_ok & cols_ok

    def only(cond, act):
        if cond is None:
            act()
        else:
            pl.when(cond)(act)

    greet = [(there(dr), at(dr, k)) for dr, k in group if (dr, k) != (0, 0)]
    greet += [(None, (p, col)) for p in row_peers + far_peers]
    for cond, to in greet:
        only(cond, lambda to=to: pl.semaphore_signal(
            barrier, inc=1, device_id=to, device_id_type=pl.DeviceIdType.MESH
        ))
    greeted = len(greet) - n_cols * ((1 - has_up.astype(jnp.int32)) + (1 - has_down.astype(jnp.int32)))

    lane = lax.broadcasted_iota(jnp.int32, (8, 128), 1)
    sub = lax.broadcasted_iota(jnp.int32, (8, 128), 0)
    row_in = (has_down, has_up)
    lane_right = lane < jnp.where(has_right, 8, 0)
    lane_left = lane >= jnp.where(has_left, 120, 128)
    side_in = lane_right | lane_left

    for c in loads[:2]:
        c.wait()
    for v in range(2):
        first = um[v, 0:RT, :, 0:128].reshape(128, 128).T
        last = um[v, 0:RT, :, 384:512].reshape(128, 128).T
        side_send[0, v] = first[0:8]
        side_send[1, v] = last[120:128]
    pl.semaphore_wait(barrier, greeted)

    halo_to = [(-1, 0), (1, 0), (-1, -1), (-1, 1), (1, -1), (1, 1), (0, -1), (0, 1)]
    halo = [
        remote(um.at[:, 0, :, pl.ds(0, 512)], um.at[:, RT, :, pl.ds(0, 512)], halo_s.at[0], halo_r.at[0], at(-1, 0)),
        remote(um.at[:, RT - 1, :, pl.ds(0, 512)], um.at[:, RT + 1, :, pl.ds(0, 512)], halo_s.at[1], halo_r.at[1], at(1, 0)),
        remote(um.at[:, 0, :, pl.ds(0, 128)], corner_recv.at[0], halo_s.at[2], halo_r.at[2], at(-1, -1)),
        remote(um.at[:, 0, :, pl.ds(384, 128)], corner_recv.at[1], halo_s.at[3], halo_r.at[3], at(-1, 1)),
        remote(um.at[:, RT - 1, :, pl.ds(0, 128)], corner_recv.at[2], halo_s.at[4], halo_r.at[4], at(1, -1)),
        remote(um.at[:, RT - 1, :, pl.ds(384, 128)], corner_recv.at[3], halo_s.at[5], halo_r.at[5], at(1, 1)),
        remote(side_send.at[0], side_recv.at[0], halo_s.at[6], halo_r.at[6], at(0, -1)),
        remote(side_send.at[1], side_recv.at[1], halo_s.at[7], halo_r.at[7], at(0, 1)),
    ]
    for c, to in zip(halo, halo_to):
        only(there(*to), c.start)

    def finish(copies, targets):
        for c, (dr, dc) in zip(copies, targets):
            only(there(dr, dc), c.wait_send)
            only(there(-dr, -dc), c.wait_recv)

    for v in range(2):
        for s_, cond in ((2, has_up), (0, has_down)):

            @pl.when(jnp.logical_not(cond))
            def _(s_=s_, v=v):
                missing = jnp.zeros((n_cols, 2, CAP, 128), F32)
                if v == 0:
                    static_recv[n_cols * s_ : n_cols * s_ + n_cols] = missing
                for i in range(ITERS // 2):
                    move_recv[v * (ITERS // 2) + i, n_cols * s_ : n_cols * s_ + n_cols] = missing


    loads[3].wait()
    red_send[0] = w[0] + w[1] + w[2] + w[3]
    stages = [
        [(0, at(0, k)) for k in range(1, n_cols)],
        [(1, (p, col)) for p in row_peers],
        [(2, (p, col)) for p in far_peers],
    ]
    red, count = [], 0
    for stage in stages:
        copies = []
        for s, to in stage:
            copies.append(remote(red_send.at[s], red_recv.at[count], red_s.at[count], red_r.at[count], to))
            count += 1
        red.append(copies)
    for c in red[0]:
        c.start()

    def reduce_stage(s):
        total, first = red_send[s], sum(len(x) for x in red[:s])
        for i, c in enumerate(red[s]):
            c.wait()
            total = total + red_recv[first + i]
        if s + 1 < len(red):
            red_send[s + 1] = total
            for c in red[s + 1]:
                c.start()
        return total

    loads[2].wait()
    d = dest[...]
    along = jnp.broadcast_to(d.astype(F32), (32, 32))
    same = along == along.T
    order_b = lax.broadcasted_iota(jnp.int32, (32, 32), 0)
    order_a = lax.broadcasted_iota(jnp.int32, (32, 32), 1)
    rank = jnp.sum(jnp.where(same & (order_b < order_a), 1.0, 0.0), axis=0, keepdims=True).astype(jnp.int32)
    slot = ((d >> 2) - row + 1) * (n_cols * CAP) + (((d & 3) - col) & 3) * CAP + rank
    slot_iota = lax.broadcasted_iota(jnp.int32, (GROUP * CAP, 32), 0)
    placing = jnp.where(slot_iota == slot, 1.0, 0.0).astype(BF16)

    def send_group(send, recv, ss, rs):
        copies = {}
        for i, (dr, k) in enumerate(group):
            if i != SELF:
                copies[i] = remote(send.at[i], recv.at[i], ss.at[i], rs.at[i], at(dr, k))
                only(there(dr), copies[i].start)
        return copies

    loads[4].wait()
    block_static = jnp.concatenate(
        [ends[...].reshape(32, 128).astype(F32), w[...].reshape(32, 128)], axis=1
    )
    placed = place(placing, block_static)
    for n in range(2):
        static_send[:, n] = placed[:, 128 * n : 128 * n + 128].reshape(GROUP, CAP, 128)
    for n in range(2):
        static_recv[SELF, n] = placed[SELF * CAP : SELF * CAP + CAP, 128 * n : 128 * n + 128]
    static_copies = send_group(static_send, static_recv, static_s, static_r)

    loads[5].wait()
    loads[6].wait()
    for b in range(32):
        both = off_raw[:, 128 * b : 128 * b + 128]
        for n in range(2):
            off[n, b // 8, b % 8 : b % 8 + 1, :] = both[n : n + 1]
    for n in range(2):
        frac[n] = 0.5 + 0.45 * jnp.tanh(off[n])

    finish(halo, halo_to)
    zero_mid = jnp.zeros((112, 128), F32)
    for v in range(2):
        strip = jnp.concatenate([side_recv[0, v], zero_mid, side_recv[1, v]], axis=0).T
        strip = strip.reshape(RT, 8, 128)
        um[v, 0:RT, :, 512:640] = jnp.where(side_in, strip, 0.0) if v == 0 else strip
        below = jnp.where(lane < 64, corner_recv[0, v], corner_recv[1, v])
        above = jnp.where(lane < 64, corner_recv[2, v], corner_recv[3, v])
        if v == 0:
            below = jnp.where(side_in & has_down, below, 0.0)
            above = jnp.where(side_in & has_up, above, 0.0)
            um[0, RT, :, 0:512] = jnp.where(has_down, um[0, RT, :, 0:512], 0.0)
            um[0, RT + 1, :, 0:512] = jnp.where(has_up, um[0, RT + 1, :, 0:512], 0.0)
        um[v, RT, :, 512:640] = below
        um[v, RT + 1, :, 512:640] = above

    def exchange(it):
        full = it + 1 < ITERS
        ss, rs = g_s.at[it], g_r.at[it]
        third = grid[0:RT, :, 384:512].reshape(128, 128).T
        fourth = grid[0:RT, :, 512:640].reshape(128, 128).T
        g_side_r[it, 0] = third[120:128]
        g_side_r[it, 1] = fourth[0:8]
        g_side_r[it, 2] = grid[RT, :, 384:512]
        g_side_r[it, 3] = grid[RT, :, 512:640]
        if full:
            first = grid[0:RT, :, 0:128].reshape(128, 128).T
            g_side_l[0] = first[0:8]
            g_side_l[1] = grid[RT, :, 0:128]
        copies = [
            remote(grid.at[pl.ds(RT - 1, 2)], g_from_u.at[it], ss.at[0], rs.at[0], at(1, 0)),
            remote(g_side_r.at[it], g_from_l.at[it], ss.at[1], rs.at[1], at(0, 1)),
            remote(grid.at[pl.ds(RT - 1, 2), :, pl.ds(384, 256)], g_from_ul.at[it], ss.at[2], rs.at[2], at(1, 1)),
        ]
        if full:
            copies += [
                remote(grid.at[0], g_from_d, ss.at[3], rs.at[3], at(-1, 0)),
                remote(g_side_l, g_from_r, ss.at[4], rs.at[4], at(0, -1)),
                remote(grid.at[pl.ds(RT - 1, 2), :, pl.ds(0, 128)], g_from_ur, ss.at[5], rs.at[5], at(1, -1)),
                remote(grid.at[0, :, pl.ds(384, 256)], g_from_dl, ss.at[6], rs.at[6], at(-1, 1)),
                remote(grid.at[0, :, pl.ds(0, 128)], g_from_dr, ss.at[7], rs.at[7], at(-1, -1)),
            ]
        targets = [(1, 0), (0, 1), (1, 1), (-1, 0), (0, -1), (1, -1), (-1, 1), (-1, -1)][: len(copies)]
        for c, to in zip(copies, targets):
            only(there(*to), c.start)
        return copies, targets

    def gather_edges(it):
        full = it + 1 < ITERS
        top = sub == 0
        left0 = (lane == 0) & has_left
        l4, z = slice(512, 640), 0.0
        grid[RT + 1] = jnp.where(has_up, g_from_u[it, 0], z)
        for j in range(LT + 1):
            js = slice(128 * j, 128 * j + 128)
            grid[0, :, js] += jnp.where(top & has_up, g_from_u[it, 1, :, js], z)
        if full:
            grid[RT] += jnp.where(has_down, g_from_d[...], z)
        right_rows = g_from_r[0] if full else jnp.zeros((8, 128), F32)
        strip = jnp.concatenate([right_rows, zero_mid, g_from_l[it, 0]], axis=0).T.reshape(RT, 8, 128)
        grid[0:RT, :, l4] += jnp.where(side_in, strip, z)
        spill = jnp.concatenate([g_from_l[it, 1], jnp.zeros((120, 128), F32)], axis=0).T.reshape(RT, 8, 128)
        grid[0:RT, :, 0:128] += jnp.where(left0, spill, z)
        edge = jnp.where(lane_left, g_from_l[it, 2], z)
        if full:
            edge = edge + jnp.where(lane_right, g_from_r[1], z)
        grid[RT, :, l4] += edge
        grid[RT, :, 0:128] += jnp.where(left0, g_from_l[it, 3], z)
        corner = jnp.where(lane_left, g_from_ul[it, 0, :, 0:128], z)
        corner_top = jnp.where(lane_left, g_from_ul[it, 1, :, 0:128], z)
        if full:
            corner = corner + jnp.where(lane_right, g_from_ur[0], z)
            corner_top = corner_top + jnp.where(lane_right, g_from_ur[1], z)
        grid[RT + 1, :, l4] += jnp.where(has_up, corner, z)
        grid[RT + 1, :, 0:128] += jnp.where(left0 & has_up, g_from_ul[it, 0, :, 128:256], z)
        grid[0, :, l4] += jnp.where(top & has_up, corner_top, z)
        grid[0, :, 0:128] += jnp.where(top & left0 & has_up, g_from_ul[it, 1, :, 128:256], z)
        if full:
            corner = jnp.where(lane_left, g_from_dl[:, 0:128], z) + jnp.where(lane_right, g_from_dr[...], z)
            grid[RT, :, l4] += jnp.where(has_down, corner, z)
            grid[RT, :, 0:128] += jnp.where(left0 & has_down, g_from_dl[:, 128:256], z)
        for j in range(LT + 1):
            js = slice(128 * j, 128 * j + 128)
            folded = pltpu.roll(grid[RT, :, js], 7, 0)
            grid[RT - 1, :, js] += jnp.where((sub == 7) & jnp.logical_not(has_down), folded, z)
        for t in range(RT + 2):
            folded = pltpu.roll(grid[t, :, l4], 127, 1)
            grid[t, :, 384:512] += jnp.where((lane == 127) & jnp.logical_not(has_right), folded, z)

    scale = None
    for it in range(ITERS):
        hjb = functools.partial(hjb_step, lane=lane, sub=sub, row_in=row_in, side_in=side_in)
        den = um.at[1]
        hjb(um.at[0], ua, den)
        hjb(ua, ub, den)
        hjb(ub, ua, den)
        hjb(ua, ub, den)
        if it == 0:
            reduce_stage(0)
        else:
            value_out[...] = ub[0:RT, :, 0:512]
        slopes(ub, table, lane, sub)
        sample(table, cells, corners)
        dx0, dx1, dy0 = corners[0], corners[1], corners[2]
        fx, fy = frac[0], frac[1]
        gx = (1.0 - fy) * dx0 + fy * dx1
        gy = (1.0 - fx) * dy0 + fx * (dy0 + (dx1 - dx0))
        hx = 0.5 + 0.45 * jnp.tanh(off[0] - gx)
        hy = 0.5 + 0.45 * jnp.tanh(off[1] - gy)
        placed = place(placing, jnp.concatenate([hx.reshape(32, 128), hy.reshape(32, 128)], axis=1))
        for n in range(2):
            move_send[it, :, n] = placed[:, 128 * n : 128 * n + 128].reshape(GROUP, CAP, 128)
            move_recv[it, SELF, n] = placed[SELF * CAP : SELF * CAP + CAP, 128 * n : 128 * n + 128]
        move_copies = send_group(move_send.at[it], move_recv.at[it], move_s.at[it], move_r.at[it])
        acc[...] = jnp.zeros_like(acc)
        if it == 0:
            reduce_stage(1)

        step = 4 * (2 * lax.rem(row, 2) - 1)
        kinds = sum(kind * 3**i for i, (kind, _) in enumerate(ORDER))
        dists = sum(k * 4**i for i, (_, k) in enumerate(ORDER))

        def arrive(i, kinds, dists):
            kind, k = lax.rem(kinds, 3) - 1, lax.rem(dists, 4)
            s = SELF + kind * step + k
            from_up, from_down = kind * step > 0, kind * step < 0

            def wait():
                remote(move_send.at[it, s], move_recv.at[it, s], move_s.at[it, s], move_r.at[it, s], at(0, 1)).wait_recv()
                if it == 0:
                    remote(static_send.at[s], static_recv.at[s], static_s.at[s], static_r.at[s], at(0, 1)).wait_recv()

            absent = (from_up & (row == 0)) | (from_down & (row == n_rows - 1))
            pl.when((i > 0) & jnp.logical_not(absent))(wait)
            return s, kinds // 3, dists // 4

        def arrivals(i, carry):
            s, kinds, dists = arrive(i, *carry)
            deposit(static_recv[s], move_recv[it, s], acc)
            return kinds, dists

        lax.fori_loop(0, GROUP, arrivals, (jnp.int32(kinds), jnp.int32(dists)))
        tops = jnp.zeros((7, 512), F32)
        here = jnp.concatenate([acc[0:128] + acc[128:256], acc[512:513] + acc[513:514], tops, jnp.zeros((8, 512), F32)], axis=0)
        beside = jnp.concatenate([acc[256:384] + acc[384:512], acc[514:515] + acc[515:516], tops, jnp.zeros((8, 512), F32)], axis=0)
        zero = jnp.zeros((144, 128), F32)
        whole = jnp.concatenate([here, zero], axis=1) + pltpu.roll(jnp.concatenate([beside, zero], axis=1), 1, 1)
        grid[...] = whole.reshape(RT + 2, 8, 640)
        copies, targets = exchange(it)
        if it == 0:
            total = reduce_stage(2)
            scale = jnp.float32(n_rows * n_cols * 128 * 512) / jnp.sum(total, keepdims=True)
        for sent in (move_copies, static_copies) if it == 0 else (move_copies,):
            for i, c in sent.items():
                only(there(group[i][0]), c.wait_send)
        finish(copies, targets)
        gather_edges(it)
        if it + 1 < ITERS:
            um[1] = 0.5 * um[1] + 0.5 * (grid[...] * scale.reshape(1, 1, 1))
        else:
            density_out[...] = 0.5 * um[1, 0:RT, :, 0:512] + 0.5 * (grid[0:RT, :, 0:512] * scale.reshape(1, 1, 1))


def body(n_rows, n_cols, terminal_value, density_start, start_cells, offsets, weights, dest_tiles, end_cells):
    any_ = pl.BlockSpec(memory_space=pltpu.HBM)
    vmem = pltpu.VMEM
    dma = pltpu.SemaphoreType.DMA
    tile = jax.ShapeDtypeStruct((RT, 8, 512), F32)
    value, density = pl.pallas_call(
        functools.partial(kernel, n_rows, n_cols),
        out_shape=(tile, tile),
        in_specs=[any_] * 7,
        out_specs=(pl.BlockSpec(memory_space=pltpu.VMEM),) * 2,
        scratch_shapes=[
            vmem((2, RT + 2, 8, 640), F32), vmem((RT + 2, 8, 640), F32), vmem((RT + 2, 8, 640), F32),
            vmem((RT + 2, 8, 640), F32),
            vmem((4, 8, 128), jnp.int32), vmem((2, 4096), F32), vmem((2, 4, 8, 128), F32), vmem((2, 4, 8, 128), F32),
            vmem((4, 8, 128), F32), vmem((4, 8, 128), jnp.int32), vmem((1, 32), jnp.int32), vmem((3, 4, 8, 128), F32), vmem((1040, 256), BF16),
            vmem((2, 2, 8, 128), F32), vmem((2, 2, 8, 128), F32), vmem((4, 2, 8, 128), F32),
            vmem((GROUP, 2, CAP, 128), F32), vmem((GROUP, 2, CAP, 128), F32),
            vmem((ITERS, GROUP, 2, CAP, 128), F32), vmem((ITERS, GROUP, 2, CAP, 128), F32),
            vmem((528, 512), F32),
            vmem((2, 8, 128), F32), vmem((ITERS, 4, 8, 128), F32),
            vmem((ITERS, 2, 8, 640), F32), vmem((8, 640), F32), vmem((ITERS, 4, 8, 128), F32), vmem((2, 8, 128), F32),
            vmem((ITERS, 2, 8, 256), F32), vmem((2, 8, 128), F32), vmem((8, 256), F32), vmem((8, 128), F32),
            vmem((3, 8, 128), F32), vmem((13, 8, 128), F32),
            dma((7,)),
            dma((8,)), dma((8,)), dma((GROUP,)), dma((GROUP,)),
            dma((ITERS, GROUP)), dma((ITERS, GROUP)), dma((ITERS, 8)), dma((ITERS, 8)), dma((13,)), dma((13,)),
        ],
        compiler_params=pltpu.CompilerParams(collective_id=0, has_side_effects=True, vmem_limit_bytes=20 << 20),
        name="crowd",
    )(
        terminal_value.reshape(RT, 8, 512),
        density_start.reshape(RT, 8, 512),
        start_cells.reshape(4, 8, 128),
        offsets,
        weights.reshape(4, 8, 128),
        dest_tiles.reshape(1, 32),
        end_cells.reshape(4, 8, 128),
    )
    return value.reshape(128, 512), density.reshape(128, 512)


def solution(mesh):
    both = ("rows", "cols")
    return jax.shard_map(
        functools.partial(body, mesh.shape["rows"], mesh.shape["cols"]),
        mesh=mesh,
        in_specs=(P("rows", "cols"), P("rows", "cols"), P(both), P(None, both), P(both), P(both), P(both)),
        out_specs=(P("rows", "cols"), P("rows", "cols")),
        check_vma=False,
    )
```

```python
import functools

import jax
import jax.numpy as jnp
from jax import lax
from jax.experimental import pallas as pl
from jax.experimental.pallas import tpu as pltpu
from jax.sharding import PartitionSpec as P

HJB_STEPS = 4
ITERS = 2
CAP = 8
RT = 16
LT = 4
ORDER = ((1, 0), (2, 0), (1, 1), (1, 3), (2, 1), (2, 3), (0, 0), (1, 2), (2, 2), (0, 1), (0, 3), (0, 2))
BATCHES = ((0, 6, 2),)
F32 = jnp.float32
BF16 = jnp.bfloat16
I16 = jnp.int16
GROUP = 12
SELF = 4


def hjb_step(src, dst, den, lane, sub, row_in, side_in):
    tiles, n_t, n_j = {}, RT + 2, LT + 1
    rolled = {}

    def cell(t, j):
        if (t, j) not in tiles:
            tiles[t, j] = src[t, :, 128 * j : 128 * j + 128]
        return tiles[t, j]

    def roll(t, j, shift, axis):
        key = (t, j, shift, axis)
        if key not in rolled:
            rolled[key] = pltpu.roll(cell(t, j), shift, axis)
        return rolled[key]

    for t in range(n_t):
        for j in range(n_j):
            v = cell(t, j)
            up = jnp.where(sub == 0, roll((t - 1) % n_t, j, 1, 0), roll(t, j, 1, 0))
            down = jnp.where(sub == 7, roll((t + 1) % n_t, j, 7, 0), roll(t, j, 7, 0))
            left = jnp.where(lane == 0, roll(t, (j - 1) % n_j, 1, 1), roll(t, j, 1, 1))
            right = jnp.where(lane == 127, roll(t, (j + 1) % n_j, 127, 1), roll(t, j, 127, 1))
            px = jnp.maximum(v - jnp.minimum(up, down), 0.0)
            py = jnp.maximum(v - jnp.minimum(left, right), 0.0)
            spread = up + down + left + right - 4.0 * v
            d = den[t, :, 128 * j : 128 * j + 128]
            new = v + 0.25 * (0.5 * spread - 0.5 * (px * px + py * py) + 0.5 * d)
            if t >= RT:
                new = jnp.where(row_in[t - RT], new, 0.0)
            if j == LT:
                new = jnp.where(side_in, new, 0.0)
            dst[t, :, 128 * j : 128 * j + 128] = new


def slopes(u, table, lane, sub):
    def split(block, first, count):
        turned = block.T[0:count]
        high = turned.astype(BF16)
        table[pl.ds(first, count), pl.ds(0, 128)] = high
        table[pl.ds(first, count), pl.ds(128, 128)] = (turned - high.astype(F32)).astype(BF16)
    for j in range(LT + 1):
        js = slice(128 * j, 128 * j + 128)
        tiles = [u[t, :, js] for t in range(RT + 1)]
        ups = [pltpu.roll(x, 7, 0) for x in tiles]
        dx = [jnp.where(sub == 7, ups[t + 1], ups[t]) - tiles[t] for t in range(RT)]
        split(jnp.concatenate(dx, axis=0), 128 * j, 128 if j < LT else 16)
        if j < LT:
            dy = []
            for t in range(RT):
                near = pltpu.roll(tiles[t], 127, 1)
                far = pltpu.roll(u[t, :, 128 * j + 128 : 128 * j + 256], 127, 1)
                dy.append(jnp.where(lane == 127, far, near) - tiles[t])
            split(jnp.concatenate(dy, axis=0), 528 + 128 * j, 128)


def sample(table, cells, corners):
    def agents(a, carry):
        cell = cells[a]
        row, col = cell >> 9, cell & 511
        for h in range(2):
            hot, places = [], []
            for b in range(4 * h, 4 * h + 4):
                r = jnp.tile(jnp.broadcast_to(row[b : b + 1], (16, 128)).astype(I16), (8, 1))
                one = jnp.where(lax.broadcasted_iota(I16, (128, 128), 0) == r, BF16(1), BF16(0))
                hot.append(jnp.concatenate([one, one], axis=0))
                places.append(jnp.broadcast_to(col[b : b + 1], (8, 128)))
            picked = jnp.dot(table[...], jnp.concatenate(hot, axis=1), preferred_element_type=F32)
            place = jnp.concatenate(places, axis=1) - lax.broadcasted_iota(jnp.int32, (8, 512), 0)
            zero = jnp.zeros((8, 512), F32)
            d0, d1, e0 = zero, zero, zero
            for i in range(64):
                here = place == 8 * i
                x = picked[8 * i : 8 * i + 8]
                d0 = jnp.where(here, x, d0)
                d1 = jnp.where(place == 8 * i - 1, x, d1)
                e0 = jnp.where(here, picked[528 + 8 * i : 536 + 8 * i], e0)
            d1 = jnp.where(place == 511, picked[512:520], d1)
            for n, v in enumerate((d0, d1, e0)):
                v = jnp.sum(v, axis=0, keepdims=True)
                for b in range(4):
                    corners[n, a, 4 * h + b : 4 * h + b + 1, :] = v[:, 128 * b : 128 * b + 128]
        return carry
    lax.fori_loop(0, 4, agents, 0)


def exact_parts(v):
    high = v.astype(BF16)
    rest = v - high.astype(F32)
    mid = rest.astype(BF16)
    return high, mid, (rest - mid.astype(F32)).astype(BF16)


def place(placing, v):
    out = None
    for part in exact_parts(v):
        term = jnp.dot(placing, part, preferred_element_type=F32)
        out = term if out is None else out + term
    return out


def factors(static, moves, masses, columns):
    cell = static[0].astype(jnp.int32)
    mass = static[1]
    x, y = moves[0], moves[1]
    row, col = cell >> 9, cell & 511
    upper, lower = mass * (1.0 - x), mass * x
    row_iota = lax.broadcasted_iota(I16, (128, 128), 0)
    col_iota = lax.broadcasted_iota(I16, (512, 128), 0)
    spill_iota = lax.broadcasted_iota(I16, (16, 128), 0)
    parts = []
    for v in (upper * (1.0 - y), lower * (1.0 - y), upper * y, lower * y):
        high = v.astype(BF16).astype(F32)
        parts.append((high, v - high))

    def spread(v, b, dtype, copies):
        tile = jnp.broadcast_to(v[b : b + 1], (16, 128)).astype(dtype)
        return jnp.tile(tile, (copies, 1)) if copies > 1 else tile

    zero = BF16(0)
    for b in range(CAP):
        r = spread(row, b, I16, 8)
        q = spread(col, b, I16, 32)
        on_upper = row_iota == r
        on_lower = row_iota == r + I16(1)
        spill = jnp.zeros((16, 128), BF16)
        block = []
        for n in range(4):
            kind, p = n // 2, n % 2
            v = spread(parts[2 * kind][p], b, BF16, 8)
            w = spread(parts[2 * kind + 1][p], b, BF16, 8)
            block.append(jnp.where(on_upper, v, jnp.where(on_lower, w, zero)))
            spill = jnp.where(spill_iota == I16(n), w[0:16], spill)
        block.append(jnp.where(r[0:16] == I16(127), spill, zero))
        masses.append(jnp.concatenate(block, axis=0))
        columns.append(jnp.where(col_iota == q, BF16(1), zero))


def deposit(slots, acc):
    masses, columns = [], []
    for static, moves in slots:
        factors(static, moves, masses, columns)
    acc[...] += lax.dot_general(
        jnp.concatenate(masses, axis=1),
        jnp.concatenate(columns, axis=1),
        (((1,), (1,)), ((), ())),
        preferred_element_type=F32,
    )


def kernel(
    n_rows, n_cols,
    u_in, m_in, cells_in, off_in, w_in, dest_in, end_in,
    value_out, density_out,
    um, ua, ub, grid, cells, off_raw, off, frac, w, ends, dest, corners, table,
    side_send, side_recv, corner_recv,
    static_send, static_recv, move_send, move_recv,
    acc,
    g_side_l, g_side_r, g_from_u, g_from_d, g_from_l, g_from_r, g_from_ul, g_from_ur, g_from_dl, g_from_dr,
    red_send, red_recv,
    load_sem,
    halo_s, halo_r, static_s, static_r, move_s, move_r, g_s, g_r, red_s, red_r,
):
    row = lax.axis_index("rows")
    col = lax.axis_index("cols")

    def at(dr, dc):
        return (lax.rem(row + dr + n_rows, n_rows), lax.rem(col + dc + n_cols, n_cols))

    def remote(src, dst, s, r, to):
        return pltpu.make_async_remote_copy(
            src_ref=src, dst_ref=dst, send_sem=s, recv_sem=r,
            device_id=to, device_id_type=pl.DeviceIdType.MESH,
        )

    loads = [
        (u_in, um.at[0, pl.ds(0, RT), :, pl.ds(0, 512)]),
        (m_in, um.at[1, pl.ds(0, RT), :, pl.ds(0, 512)]),
        (dest_in, dest), (w_in, w), (end_in, ends), (off_in, off_raw), (cells_in, cells),
    ]
    loads = [pltpu.make_async_copy(a, b, load_sem.at[i]) for i, (a, b) in enumerate(loads)]
    for c in loads:
        c.start()

    group = [(dr, k) for dr in (-1, 0, 1) for k in range(n_cols)]
    near = row % 8
    base = row - near
    row_peers = [base + (near + j) % 8 for j in range(1, 8)]
    far_peers = [lax.rem(row + 8 * j, n_rows) for j in range(1, 4)]

    barrier = pltpu.get_barrier_semaphore()
    has_up, has_down = row > 0, row < n_rows - 1
    has_left, has_right = col > 0, col < n_cols - 1

    def there(dr, dc=0):
        rows_ok = {-1: has_up, 0: None, 1: has_down}[dr]
        cols_ok = {-1: has_left, 0: None, 1: has_right}[dc]
        if rows_ok is None or cols_ok is None:
            return cols_ok if rows_ok is None else rows_ok
        return rows_ok & cols_ok

    def only(cond, act):
        if cond is None:
            act()
        else:
            pl.when(cond)(act)

    greet = [(there(dr), at(dr, k)) for dr, k in group if (dr, k) != (0, 0)]
    greet += [(None, (p, col)) for p in row_peers + far_peers]
    for cond, to in greet:
        only(cond, lambda to=to: pl.semaphore_signal(
            barrier, inc=1, device_id=to, device_id_type=pl.DeviceIdType.MESH
        ))
    greeted = len(greet) - n_cols * ((1 - has_up.astype(jnp.int32)) + (1 - has_down.astype(jnp.int32)))

    lane = lax.broadcasted_iota(jnp.int32, (8, 128), 1)
    sub = lax.broadcasted_iota(jnp.int32, (8, 128), 0)
    row_in = (has_down, has_up)
    lane_right = lane < jnp.where(has_right, 8, 0)
    lane_left = lane >= jnp.where(has_left, 120, 128)
    side_in = lane_right | lane_left

    for c in loads[:2]:
        c.wait()
    for v in range(2):
        first = um[v, 0:RT, :, 0:128].reshape(128, 128).T
        last = um[v, 0:RT, :, 384:512].reshape(128, 128).T
        side_send[0, v] = first[0:8]
        side_send[1, v] = last[120:128]
    pl.semaphore_wait(barrier, greeted)

    halo_to = [(-1, 0), (1, 0), (-1, -1), (-1, 1), (1, -1), (1, 1), (0, -1), (0, 1)]
    halo = [
        remote(um.at[:, 0, :, pl.ds(0, 512)], um.at[:, RT, :, pl.ds(0, 512)], halo_s.at[0], halo_r.at[0], at(-1, 0)),
        remote(um.at[:, RT - 1, :, pl.ds(0, 512)], um.at[:, RT + 1, :, pl.ds(0, 512)], halo_s.at[1], halo_r.at[1], at(1, 0)),
        remote(um.at[:, 0, :, pl.ds(0, 128)], corner_recv.at[0], halo_s.at[2], halo_r.at[2], at(-1, -1)),
        remote(um.at[:, 0, :, pl.ds(384, 128)], corner_recv.at[1], halo_s.at[3], halo_r.at[3], at(-1, 1)),
        remote(um.at[:, RT - 1, :, pl.ds(0, 128)], corner_recv.at[2], halo_s.at[4], halo_r.at[4], at(1, -1)),
        remote(um.at[:, RT - 1, :, pl.ds(384, 128)], corner_recv.at[3], halo_s.at[5], halo_r.at[5], at(1, 1)),
        remote(side_send.at[0], side_recv.at[0], halo_s.at[6], halo_r.at[6], at(0, -1)),
        remote(side_send.at[1], side_recv.at[1], halo_s.at[7], halo_r.at[7], at(0, 1)),
    ]
    for c, to in zip(halo, halo_to):
        only(there(*to), c.start)

    def finish(copies, targets):
        for c, (dr, dc) in zip(copies, targets):
            only(there(dr, dc), c.wait_send)
            only(there(-dr, -dc), c.wait_recv)

    for v in range(2):
        for s_, cond in ((2, has_up), (0, has_down)):

            @pl.when(jnp.logical_not(cond))
            def _(s_=s_, v=v):
                missing = jnp.zeros((n_cols, 2, CAP, 128), F32)
                if v == 0:
                    static_recv[n_cols * s_ : n_cols * s_ + n_cols] = missing
                for i in range(ITERS // 2):
                    move_recv[v * (ITERS // 2) + i, n_cols * s_ : n_cols * s_ + n_cols] = missing


    loads[3].wait()
    red_send[0] = w[0] + w[1] + w[2] + w[3]
    stages = [
        [(0, at(0, k)) for k in range(1, n_cols)],
        [(1, (p, col)) for p in row_peers],
        [(2, (p, col)) for p in far_peers],
    ]
    red, count = [], 0
    for stage in stages:
        copies = []
        for s, to in stage:
            copies.append(remote(red_send.at[s], red_recv.at[count], red_s.at[count], red_r.at[count], to))
            count += 1
        red.append(copies)
    for c in red[0]:
        c.start()

    def reduce_stage(s):
        total, first = red_send[s], sum(len(x) for x in red[:s])
        for i, c in enumerate(red[s]):
            c.wait()
            total = total + red_recv[first + i]
        if s + 1 < len(red):
            red_send[s + 1] = total
            for c in red[s + 1]:
                c.start()
        return total

    loads[2].wait()
    d = dest[...]
    along = jnp.broadcast_to(d.astype(F32), (32, 32))
    same = along == along.T
    order_b = lax.broadcasted_iota(jnp.int32, (32, 32), 0)
    order_a = lax.broadcasted_iota(jnp.int32, (32, 32), 1)
    rank = jnp.sum(jnp.where(same & (order_b < order_a), 1.0, 0.0), axis=0, keepdims=True).astype(jnp.int32)
    slot = ((d >> 2) - row + 1) * (n_cols * CAP) + (((d & 3) - col) & 3) * CAP + rank
    slot_iota = lax.broadcasted_iota(jnp.int32, (GROUP * CAP, 32), 0)
    placing = jnp.where(slot_iota == slot, 1.0, 0.0).astype(BF16)

    def send_group(send, recv, ss, rs):
        copies = {}
        for i, (dr, k) in enumerate(group):
            if i != SELF:
                copies[i] = remote(send.at[i], recv.at[i], ss.at[i], rs.at[i], at(dr, k))
                only(there(dr), copies[i].start)
        return copies

    loads[4].wait()
    block_static = jnp.concatenate(
        [ends[...].reshape(32, 128).astype(F32), w[...].reshape(32, 128)], axis=1
    )
    placed = place(placing, block_static)
    for n in range(2):
        static_send[:, n] = placed[:, 128 * n : 128 * n + 128].reshape(GROUP, CAP, 128)
    for n in range(2):
        static_recv[SELF, n] = placed[SELF * CAP : SELF * CAP + CAP, 128 * n : 128 * n + 128]
    static_copies = send_group(static_send, static_recv, static_s, static_r)

    loads[5].wait()
    loads[6].wait()
    for b in range(32):
        both = off_raw[:, 128 * b : 128 * b + 128]
        for n in range(2):
            off[n, b // 8, b % 8 : b % 8 + 1, :] = both[n : n + 1]
    for n in range(2):
        frac[n] = 0.5 + 0.45 * jnp.tanh(off[n])

    finish(halo, halo_to)
    zero_mid = jnp.zeros((112, 128), F32)
    for v in range(2):
        strip = jnp.concatenate([side_recv[0, v], zero_mid, side_recv[1, v]], axis=0).T
        strip = strip.reshape(RT, 8, 128)
        um[v, 0:RT, :, 512:640] = jnp.where(side_in, strip, 0.0) if v == 0 else strip
        below = jnp.where(lane < 64, corner_recv[0, v], corner_recv[1, v])
        above = jnp.where(lane < 64, corner_recv[2, v], corner_recv[3, v])
        if v == 0:
            below = jnp.where(side_in & has_down, below, 0.0)
            above = jnp.where(side_in & has_up, above, 0.0)
            um[0, RT, :, 0:512] = jnp.where(has_down, um[0, RT, :, 0:512], 0.0)
            um[0, RT + 1, :, 0:512] = jnp.where(has_up, um[0, RT + 1, :, 0:512], 0.0)
        um[v, RT, :, 512:640] = below
        um[v, RT + 1, :, 512:640] = above

    def exchange(it):
        full = it + 1 < ITERS
        ss, rs = g_s.at[it], g_r.at[it]
        sends = [
            (grid.at[pl.ds(RT - 1, 2)], g_from_u.at[it], (1, 0)),
            (grid.at[pl.ds(RT - 1, 2), :, pl.ds(384, 256)], g_from_ul.at[it], (1, 1)),
        ]
        if full:
            sends += [
                (grid.at[0], g_from_d, (-1, 0)),
                (grid.at[pl.ds(RT - 1, 2), :, pl.ds(0, 128)], g_from_ur, (1, -1)),
                (grid.at[0, :, pl.ds(384, 256)], g_from_dl, (-1, 1)),
                (grid.at[0, :, pl.ds(0, 128)], g_from_dr, (-1, -1)),
            ]
        copies, targets = [], []

        def send(src, dst, to):
            n = len(copies)
            copies.append(remote(src, dst, ss.at[n], rs.at[n], at(*to)))
            targets.append(to)
            only(there(*to), copies[-1].start)

        for x in sends:
            send(*x)
        third = grid[0:RT, :, 384:512].reshape(128, 128).T
        fourth = grid[0:RT, :, 512:640].reshape(128, 128).T
        g_side_r[it, 0] = third[120:128]
        g_side_r[it, 1] = fourth[0:8]
        g_side_r[it, 2] = grid[RT, :, 384:512]
        g_side_r[it, 3] = grid[RT, :, 512:640]
        if full:
            first = grid[0:RT, :, 0:128].reshape(128, 128).T
            g_side_l[0] = first[0:8]
            g_side_l[1] = grid[RT, :, 0:128]
        send(g_side_r.at[it], g_from_l.at[it], (0, 1))
        if full:
            send(g_side_l, g_from_r, (0, -1))
        return copies, targets

    def gather_edges(it):
        full = it + 1 < ITERS
        top = sub == 0
        left0 = (lane == 0) & has_left
        l4, z = slice(512, 640), 0.0
        grid[RT + 1] = jnp.where(has_up, g_from_u[it, 0], z)
        for j in range(LT + 1):
            js = slice(128 * j, 128 * j + 128)
            grid[0, :, js] += jnp.where(top & has_up, g_from_u[it, 1, :, js], z)
        if full:
            grid[RT] += jnp.where(has_down, g_from_d[...], z)
        right_rows = g_from_r[0] if full else jnp.zeros((8, 128), F32)
        strip = jnp.concatenate([right_rows, zero_mid, g_from_l[it, 0]], axis=0).T.reshape(RT, 8, 128)
        grid[0:RT, :, l4] += jnp.where(side_in, strip, z)
        spill = jnp.concatenate([g_from_l[it, 1], jnp.zeros((120, 128), F32)], axis=0).T.reshape(RT, 8, 128)
        grid[0:RT, :, 0:128] += jnp.where(left0, spill, z)
        edge = jnp.where(lane_left, g_from_l[it, 2], z)
        if full:
            edge = edge + jnp.where(lane_right, g_from_r[1], z)
        grid[RT, :, l4] += edge
        grid[RT, :, 0:128] += jnp.where(left0, g_from_l[it, 3], z)
        corner = jnp.where(lane_left, g_from_ul[it, 0, :, 0:128], z)
        corner_top = jnp.where(lane_left, g_from_ul[it, 1, :, 0:128], z)
        if full:
            corner = corner + jnp.where(lane_right, g_from_ur[0], z)
            corner_top = corner_top + jnp.where(lane_right, g_from_ur[1], z)
        grid[RT + 1, :, l4] += jnp.where(has_up, corner, z)
        grid[RT + 1, :, 0:128] += jnp.where(left0 & has_up, g_from_ul[it, 0, :, 128:256], z)
        grid[0, :, l4] += jnp.where(top & has_up, corner_top, z)
        grid[0, :, 0:128] += jnp.where(top & left0 & has_up, g_from_ul[it, 1, :, 128:256], z)
        if full:
            corner = jnp.where(lane_left, g_from_dl[:, 0:128], z) + jnp.where(lane_right, g_from_dr[...], z)
            grid[RT, :, l4] += jnp.where(has_down, corner, z)
            grid[RT, :, 0:128] += jnp.where(left0 & has_down, g_from_dl[:, 128:256], z)
        for j in range(LT + 1):
            js = slice(128 * j, 128 * j + 128)
            folded = pltpu.roll(grid[RT, :, js], 7, 0)
            grid[RT - 1, :, js] += jnp.where((sub == 7) & jnp.logical_not(has_down), folded, z)
        for t in range(RT + 2):
            folded = pltpu.roll(grid[t, :, l4], 127, 1)
            grid[t, :, 384:512] += jnp.where((lane == 127) & jnp.logical_not(has_right), folded, z)

    scale = None
    for it in range(ITERS):
        hjb = functools.partial(hjb_step, lane=lane, sub=sub, row_in=row_in, side_in=side_in)
        den = um.at[1]
        hjb(um.at[0], ua, den)
        hjb(ua, ub, den)
        hjb(ub, ua, den)
        hjb(ua, ub, den)
        if it == 0:
            reduce_stage(0)
        slopes(ub, table, lane, sub)
        sample(table, cells, corners)
        dx0, dx1, dy0 = corners[0], corners[1], corners[2]
        fx, fy = frac[0], frac[1]
        gx = (1.0 - fy) * dx0 + fy * dx1
        gy = (1.0 - fx) * dy0 + fx * (dy0 + (dx1 - dx0))
        hx = 0.5 + 0.45 * jnp.tanh(off[0] - gx)
        hy = 0.5 + 0.45 * jnp.tanh(off[1] - gy)
        placed = place(placing, jnp.concatenate([hx.reshape(32, 128), hy.reshape(32, 128)], axis=1))
        for n in range(2):
            move_send[it, :, n] = placed[:, 128 * n : 128 * n + 128].reshape(GROUP, CAP, 128)
            move_recv[it, SELF, n] = placed[SELF * CAP : SELF * CAP + CAP, 128 * n : 128 * n + 128]
        move_copies = send_group(move_send.at[it], move_recv.at[it], move_s.at[it], move_r.at[it])
        acc[...] = jnp.zeros_like(acc)
        if it + 1 == ITERS:
            value_out[...] = ub[0:RT, :, 0:512]

        step = 4 * (2 * lax.rem(row, 2) - 1)
        kinds = sum(kind * 3**i for i, (kind, _) in enumerate(ORDER))
        dists = sum(k * 4**i for i, (_, k) in enumerate(ORDER))

        def arrive(i, kinds, dists):
            kind, k = lax.rem(kinds, 3) - 1, lax.rem(dists, 4)
            s = SELF + kind * step + k
            from_up, from_down = kind * step > 0, kind * step < 0

            def wait():
                remote(move_send.at[it, s], move_recv.at[it, s], move_s.at[it, s], move_r.at[it, s], at(0, 1)).wait_recv()
                if it == 0:
                    remote(static_send.at[s], static_recv.at[s], static_s.at[s], static_r.at[s], at(0, 1)).wait_recv()

            absent = (from_up & (row == 0)) | (from_down & (row == n_rows - 1))
            pl.when((i > 0) & jnp.logical_not(absent))(wait)
            return s, kinds // 3, dists // 4

        def arrivals(first, batch, i, carry):
            slots = []
            for j in range(batch):
                s, *carry = arrive(first + batch * i + j, *carry)
                slots.append((static_recv[s], move_recv[it, s]))
            deposit(slots, acc)
            return tuple(carry)

        carry = (jnp.int32(kinds), jnp.int32(dists))
        for first, count, batch in BATCHES:
            step_ = functools.partial(arrivals, first, batch)
            carry = step_(0, carry) if count == 1 else lax.fori_loop(0, count, step_, carry)
        tops = jnp.zeros((7, 512), F32)
        here = jnp.concatenate([acc[0:128] + acc[128:256], acc[512:513] + acc[513:514], tops, jnp.zeros((8, 512), F32)], axis=0)
        beside = jnp.concatenate([acc[256:384] + acc[384:512], acc[514:515] + acc[515:516], tops, jnp.zeros((8, 512), F32)], axis=0)
        zero = jnp.zeros((144, 128), F32)
        whole = jnp.concatenate([here, zero], axis=1) + pltpu.roll(jnp.concatenate([beside, zero], axis=1), 1, 1)
        grid[...] = whole.reshape(RT + 2, 8, 640)
        copies, targets = exchange(it)
        if it == 0:
            reduce_stage(1)
        for sent in (move_copies, static_copies) if it == 0 else (move_copies,):
            for i, c in sent.items():
                only(there(group[i][0]), c.wait_send)
        finish(copies, targets)
        if it == 0:
            total = reduce_stage(2)
            scale = jnp.float32(n_rows * n_cols * 128 * 512) / jnp.sum(total, keepdims=True)
        gather_edges(it)
        if it + 1 < ITERS:
            um[1] = 0.5 * um[1] + 0.5 * (grid[...] * scale.reshape(1, 1, 1))
        else:
            density_out[...] = 0.5 * um[1, 0:RT, :, 0:512] + 0.5 * (grid[0:RT, :, 0:512] * scale.reshape(1, 1, 1))


def write_out(value, density, value_out, density_out, sems):
    copies = [
        pltpu.make_async_copy(value, value_out, sems.at[0]),
        pltpu.make_async_copy(density, density_out, sems.at[1]),
    ]
    for c in copies:
        c.start()
    for c in copies:
        c.wait()


def body(n_rows, n_cols, terminal_value, density_start, start_cells, offsets, weights, dest_tiles, end_cells):
    any_ = pl.BlockSpec(memory_space=pltpu.HBM)
    vmem = pltpu.VMEM
    dma = pltpu.SemaphoreType.DMA
    tile = jax.ShapeDtypeStruct((RT, 8, 512), F32)
    value, density = pl.pallas_call(
        functools.partial(kernel, n_rows, n_cols),
        out_shape=(tile, tile),
        in_specs=[any_] * 7,
        out_specs=(pl.BlockSpec(memory_space=pltpu.VMEM),) * 2,
        scratch_shapes=[
            vmem((2, RT + 2, 8, 640), F32), vmem((RT + 2, 8, 640), F32), vmem((RT + 2, 8, 640), F32),
            vmem((RT + 2, 8, 640), F32),
            vmem((4, 8, 128), jnp.int32), vmem((2, 4096), F32), vmem((2, 4, 8, 128), F32), vmem((2, 4, 8, 128), F32),
            vmem((4, 8, 128), F32), vmem((4, 8, 128), jnp.int32), vmem((1, 32), jnp.int32), vmem((3, 4, 8, 128), F32), vmem((1040, 256), BF16),
            vmem((2, 2, 8, 128), F32), vmem((2, 2, 8, 128), F32), vmem((4, 2, 8, 128), F32),
            vmem((GROUP, 2, CAP, 128), F32), vmem((GROUP, 2, CAP, 128), F32),
            vmem((ITERS, GROUP, 2, CAP, 128), F32), vmem((ITERS, GROUP, 2, CAP, 128), F32),
            vmem((528, 512), F32),
            vmem((2, 8, 128), F32), vmem((ITERS, 4, 8, 128), F32),
            vmem((ITERS, 2, 8, 640), F32), vmem((8, 640), F32), vmem((ITERS, 4, 8, 128), F32), vmem((2, 8, 128), F32),
            vmem((ITERS, 2, 8, 256), F32), vmem((2, 8, 128), F32), vmem((8, 256), F32), vmem((8, 128), F32),
            vmem((3, 8, 128), F32), vmem((13, 8, 128), F32),
            dma((7,)),
            dma((8,)), dma((8,)), dma((GROUP,)), dma((GROUP,)),
            dma((ITERS, GROUP)), dma((ITERS, GROUP)), dma((ITERS, 8)), dma((ITERS, 8)), dma((13,)), dma((13,)),
        ],
        compiler_params=pltpu.CompilerParams(collective_id=0, has_side_effects=True, vmem_limit_bytes=20 << 20),
        name="crowd",
    )(*(pltpu.with_memory_space_constraint(x, pltpu.HBM) for x in (
        terminal_value.reshape(RT, 8, 512),
        density_start.reshape(RT, 8, 512),
        start_cells.reshape(4, 8, 128),
        offsets,
        weights.reshape(4, 8, 128),
        dest_tiles.reshape(1, 32),
        end_cells.reshape(4, 8, 128),
    )))
    value, density = pl.pallas_call(
        write_out,
        out_shape=(tile, tile),
        in_specs=[pl.BlockSpec(memory_space=pltpu.VMEM)] * 2,
        out_specs=(pl.BlockSpec(memory_space=pltpu.HBM),) * 2,
        scratch_shapes=[dma((2,))],
        compiler_params=pltpu.CompilerParams(vmem_limit_bytes=1 << 20),
        name="write_out",
    )(value, density)
    return value.reshape(128, 512), density.reshape(128, 512)


def solution(mesh):
    both = ("rows", "cols")
    return jax.shard_map(
        functools.partial(body, mesh.shape["rows"], mesh.shape["cols"]),
        mesh=mesh,
        in_specs=(P("rows", "cols"), P("rows", "cols"), P(both), P(None, both), P(both), P(both), P(both)),
        out_specs=(P("rows", "cols"), P("rows", "cols")),
        check_vma=False,
    )
```

```python
import functools

import jax
import jax.numpy as jnp
from jax import lax
from jax.experimental import pallas as pl
from jax.experimental.pallas import tpu as pltpu
from jax.sharding import PartitionSpec as P

HJB_STEPS = 4
ITERS = 2
CAP = 8
RT = 16
LT = 4
ORDER = ((1, 0), (2, 0), (1, 1), (1, 3), (2, 1), (2, 3), (0, 0), (1, 2), (2, 2), (0, 1), (0, 3), (0, 2))
BATCHES = ((0, 6, 2),)
F32 = jnp.float32
BF16 = jnp.bfloat16
I16 = jnp.int16
GROUP = 12
SELF = 4


def hjb_step(src, dst, den, lane, sub, row_in, side_in):
    tiles, n_t, n_j = {}, RT + 2, LT + 1
    rolled = {}

    def cell(t, j):
        if (t, j) not in tiles:
            tiles[t, j] = src[t, :, 128 * j : 128 * j + 128]
        return tiles[t, j]

    def roll(t, j, shift, axis):
        key = (t, j, shift, axis)
        if key not in rolled:
            rolled[key] = pltpu.roll(cell(t, j), shift, axis)
        return rolled[key]

    for t in range(n_t):
        for j in range(n_j):
            v = cell(t, j)
            up = jnp.where(sub == 0, roll((t - 1) % n_t, j, 1, 0), roll(t, j, 1, 0))
            down = jnp.where(sub == 7, roll((t + 1) % n_t, j, 7, 0), roll(t, j, 7, 0))
            left = jnp.where(lane == 0, roll(t, (j - 1) % n_j, 1, 1), roll(t, j, 1, 1))
            right = jnp.where(lane == 127, roll(t, (j + 1) % n_j, 127, 1), roll(t, j, 127, 1))
            px = jnp.maximum(v - jnp.minimum(up, down), 0.0)
            py = jnp.maximum(v - jnp.minimum(left, right), 0.0)
            d = den[t, :, 128 * j : 128 * j + 128]
            new = 0.5 * v + 0.125 * ((up + down) + (left + right) - (px * px + py * py) + d)
            if t >= RT:
                new = jnp.where(row_in[t - RT], new, 0.0)
            if j == LT:
                new = jnp.where(side_in, new, 0.0)
            dst[t, :, 128 * j : 128 * j + 128] = new


def slopes(u, u1, table, lane, sub):
    def split(block, first, count):
        turned = block.T[0:count]
        high = turned.astype(BF16)
        table[pl.ds(first, count), pl.ds(0, 128)] = high
        table[pl.ds(first, count), pl.ds(128, 128)] = (turned - high.astype(F32)).astype(BF16)

    for j in range(LT + 1):
        js = slice(128 * j, 128 * j + 128)
        tiles = [u[t, :, js] for t in range(RT + 1)]
        ups = [pltpu.roll(x, 7, 0) for x in tiles]
        dx = [jnp.where(sub == 7, ups[t + 1], ups[t]) - tiles[t] for t in range(RT)]
        split(jnp.concatenate(dx, axis=0), 128 * j, 128 if j < LT else 16)
        if j < LT:
            dy = []
            for t in range(RT):
                near = pltpu.roll(tiles[t], 127, 1)
                far = pltpu.roll(u[t, :, 128 * j + 128 : 128 * j + 256], 127, 1)
                right = jnp.where(lane == 127, far, near)
                u1[t, :, js] = right
                dy.append(right - tiles[t])
            split(jnp.concatenate(dy, axis=0), 528 + 128 * j, 128)
            near = pltpu.roll(tiles[RT], 127, 1)
            far = pltpu.roll(u[RT, :, 128 * j + 128 : 128 * j + 256], 127, 1)
            u1[RT, :, js] = jnp.where(lane == 127, far, near)


def sample(table, u, u1, cells, corners):
    one_cell = cells[0]
    key, idx = one_cell >> 7, one_cell & 127
    zero1 = jnp.zeros((8, 128), F32)
    def agents(t, acc):
        a = t + 1
        cell = cells[a]
        row, col = cell >> 9, cell & 511
        u00, u10, u01, u11 = acc
        kk = key - t * (48 * LT)
        def look(lo, hi):
            nonlocal u00, u10, u01, u11
            for r in range(lo, hi):
                for j in range(LT):
                    part = (t * 6 + r // 8, slice(r % 8, r % 8 + 1), slice(128 * j, 128 * j + 128))
                    here = jnp.take_along_axis(jnp.broadcast_to(u[part], (8, 128)), idx, axis=1)
                    next_ = jnp.take_along_axis(jnp.broadcast_to(u1[part], (8, 128)), idx, axis=1)
                    hit = kk == r * LT + j
                    u00 = jnp.where(hit, here, u00)
                    u01 = jnp.where(hit, next_, u01)
                    hit = kk == (r - 1) * LT + j
                    u10 = jnp.where(hit, here, u10)
                    u11 = jnp.where(hit, next_, u11)
        for h in range(2):
            hot, places = [], []
            for b in range(4 * h, 4 * h + 4):
                r = jnp.tile(jnp.broadcast_to(row[b : b + 1], (16, 128)).astype(I16), (8, 1))
                one = jnp.where(lax.broadcasted_iota(I16, (128, 128), 0) == r, BF16(1), BF16(0))
                hot.append(jnp.concatenate([one, one], axis=0))
                places.append(jnp.broadcast_to(col[b : b + 1], (8, 128)))
            picked = jnp.dot(table[...], jnp.concatenate(hot, axis=1), preferred_element_type=F32)
            place = jnp.concatenate(places, axis=1) - lax.broadcasted_iota(jnp.int32, (8, 512), 0)
            zero = jnp.zeros((8, 512), F32)
            d0, d1, e0 = zero, zero, zero
            for i in range(64):
                here = place == 8 * i
                x = picked[8 * i : 8 * i + 8]
                d0 = jnp.where(here, x, d0)
                d1 = jnp.where(place == 8 * i - 1, x, d1)
                e0 = jnp.where(here, picked[528 + 8 * i : 536 + 8 * i], e0)
            d1 = jnp.where(place == 511, picked[512:520], d1)
            look(24 * h, 24 * h + 24)
            for n, v in enumerate((d0, d1, e0)):
                v = jnp.sum(v, axis=0, keepdims=True)
                for b in range(4):
                    corners[n, a, 4 * h + b : 4 * h + b + 1, :] = v[:, 128 * b : 128 * b + 128]
        return u00, u10, u01, u11
    u00, u10, u01, u11 = lax.fori_loop(0, 3, agents, (zero1, zero1, zero1, zero1))
    corners[0, 0] = u10 - u00
    corners[1, 0] = u11 - u01
    corners[2, 0] = u01 - u00


def exact_parts(v):
    high = v.astype(BF16)
    rest = v - high.astype(F32)
    mid = rest.astype(BF16)
    return high, mid, (rest - mid.astype(F32)).astype(BF16)


def place(placing, v):
    out = None
    for part in exact_parts(v):
        term = jnp.dot(placing, part, preferred_element_type=F32)
        out = term if out is None else out + term
    return out


def factors(static, moves, masses, columns):
    cell = static[0].astype(jnp.int32)
    mass = static[1]
    x, y = moves[0], moves[1]
    row, col = cell >> 9, cell & 511
    upper, lower = mass * (1.0 - x), mass * x
    row_iota = lax.broadcasted_iota(I16, (128, 128), 0)
    col_iota = lax.broadcasted_iota(I16, (512, 128), 0)
    spill_iota = lax.broadcasted_iota(I16, (16, 128), 0)
    parts = []
    for v in (upper * (1.0 - y), lower * (1.0 - y), upper * y, lower * y):
        high = v.astype(BF16).astype(F32)
        parts.append((high, v - high))

    def spread(v, b, dtype, copies):
        tile = jnp.broadcast_to(v[b : b + 1], (16, 128)).astype(dtype)
        return jnp.tile(tile, (copies, 1)) if copies > 1 else tile

    zero = BF16(0)
    for b in range(CAP):
        r = spread(row, b, I16, 8)
        q = spread(col, b, I16, 32)
        on_upper = row_iota == r
        on_lower = row_iota == r + I16(1)
        spill = jnp.zeros((16, 128), BF16)
        block = []
        for n in range(4):
            kind, p = n // 2, n % 2
            v = spread(parts[2 * kind][p], b, BF16, 8)
            w = spread(parts[2 * kind + 1][p], b, BF16, 8)
            block.append(jnp.where(on_upper, v, jnp.where(on_lower, w, zero)))
            spill = jnp.where(spill_iota == I16(n), w[0:16], spill)
        block.append(jnp.where(r[0:16] == I16(127), spill, zero))
        masses.append(jnp.concatenate(block, axis=0))
        columns.append(jnp.where(col_iota == q, BF16(1), zero))


def deposit(slots, acc):
    masses, columns = [], []
    for static, moves in slots:
        factors(static, moves, masses, columns)
    acc[...] += lax.dot_general(
        jnp.concatenate(masses, axis=1),
        jnp.concatenate(columns, axis=1),
        (((1,), (1,)), ((), ())),
        preferred_element_type=F32,
    )


def kernel(
    n_rows, n_cols,
    u_in, m_in, cells_in, off_in, w_in, dest_in, end_in,
    value_out, density_out,
    um, ua, ub, grid, cells, off_raw, off, frac, w, ends, dest, corners, table,
    side_send, side_recv, corner_recv,
    static_send, static_recv, move_send, move_recv,
    acc,
    g_side_l, g_side_r, g_from_u, g_from_d, g_from_l, g_from_r, g_from_ul, g_from_ur, g_from_dl, g_from_dr,
    red_send, red_recv,
    load_sem,
    halo_s, halo_r, static_s, static_r, move_s, move_r, g_s, g_r, red_s, red_r,
):
    row = lax.axis_index("rows")
    col = lax.axis_index("cols")

    def at(dr, dc):
        return (lax.rem(row + dr + n_rows, n_rows), lax.rem(col + dc + n_cols, n_cols))

    def remote(src, dst, s, r, to):
        return pltpu.make_async_remote_copy(
            src_ref=src, dst_ref=dst, send_sem=s, recv_sem=r,
            device_id=to, device_id_type=pl.DeviceIdType.MESH,
        )

    loads = [
        (u_in, um.at[0, pl.ds(0, RT), :, pl.ds(0, 512)]),
        (m_in, um.at[1, pl.ds(0, RT), :, pl.ds(0, 512)]),
        (dest_in, dest), (w_in, w), (end_in, ends), (off_in, off_raw), (cells_in, cells),
    ]
    loads = [pltpu.make_async_copy(a, b, load_sem.at[i]) for i, (a, b) in enumerate(loads)]
    for c in loads:
        c.start()

    group = [(dr, k) for dr in (-1, 0, 1) for k in range(n_cols)]
    near = row % 8
    base = row - near
    row_peers = [base + (near + j) % 8 for j in range(1, 8)]
    far_peers = [lax.rem(row + 8 * j, n_rows) for j in range(1, 4)]

    barrier = pltpu.get_barrier_semaphore()
    has_up, has_down = row > 0, row < n_rows - 1
    has_left, has_right = col > 0, col < n_cols - 1

    def there(dr, dc=0):
        rows_ok = {-1: has_up, 0: None, 1: has_down}[dr]
        cols_ok = {-1: has_left, 0: None, 1: has_right}[dc]
        if rows_ok is None or cols_ok is None:
            return cols_ok if rows_ok is None else rows_ok
        return rows_ok & cols_ok

    def only(cond, act):
        if cond is None:
            act()
        else:
            pl.when(cond)(act)

    greet = [(there(dr), at(dr, k)) for dr, k in group if (dr, k) != (0, 0)]
    greet += [(None, (p, col)) for p in row_peers + far_peers]
    for cond, to in greet:
        only(cond, lambda to=to: pl.semaphore_signal(
            barrier, inc=1, device_id=to, device_id_type=pl.DeviceIdType.MESH
        ))
    greeted = len(greet) - n_cols * ((1 - has_up.astype(jnp.int32)) + (1 - has_down.astype(jnp.int32)))

    lane = lax.broadcasted_iota(jnp.int32, (8, 128), 1)
    sub = lax.broadcasted_iota(jnp.int32, (8, 128), 0)
    row_in = (has_down, has_up)
    lane_right = lane < jnp.where(has_right, 8, 0)
    lane_left = lane >= jnp.where(has_left, 120, 128)
    side_in = lane_right | lane_left

    for c in loads[:2]:
        c.wait()
    for v in range(2):
        first = um[v, 0:RT, :, 0:128].reshape(128, 128).T
        last = um[v, 0:RT, :, 384:512].reshape(128, 128).T
        side_send[0, v] = first[0:8]
        side_send[1, v] = last[120:128]
    pl.semaphore_wait(barrier, greeted)

    halo_to = [(-1, 0), (1, 0), (-1, -1), (-1, 1), (1, -1), (1, 1), (0, -1), (0, 1)]
    halo = [
        remote(um.at[:, 0, :, pl.ds(0, 512)], um.at[:, RT, :, pl.ds(0, 512)], halo_s.at[0], halo_r.at[0], at(-1, 0)),
        remote(um.at[:, RT - 1, :, pl.ds(0, 512)], um.at[:, RT + 1, :, pl.ds(0, 512)], halo_s.at[1], halo_r.at[1], at(1, 0)),
        remote(um.at[:, 0, :, pl.ds(0, 128)], corner_recv.at[0], halo_s.at[2], halo_r.at[2], at(-1, -1)),
        remote(um.at[:, 0, :, pl.ds(384, 128)], corner_recv.at[1], halo_s.at[3], halo_r.at[3], at(-1, 1)),
        remote(um.at[:, RT - 1, :, pl.ds(0, 128)], corner_recv.at[2], halo_s.at[4], halo_r.at[4], at(1, -1)),
        remote(um.at[:, RT - 1, :, pl.ds(384, 128)], corner_recv.at[3], halo_s.at[5], halo_r.at[5], at(1, 1)),
        remote(side_send.at[0], side_recv.at[0], halo_s.at[6], halo_r.at[6], at(0, -1)),
        remote(side_send.at[1], side_recv.at[1], halo_s.at[7], halo_r.at[7], at(0, 1)),
    ]
    for c, to in zip(halo, halo_to):
        only(there(*to), c.start)

    def finish(copies, targets):
        for c, (dr, dc) in zip(copies, targets):
            only(there(dr, dc), c.wait_send)
            only(there(-dr, -dc), c.wait_recv)

    for v in range(2):
        for s_, cond in ((2, has_up), (0, has_down)):

            @pl.when(jnp.logical_not(cond))
            def _(s_=s_, v=v):
                missing = jnp.zeros((n_cols, 2, CAP, 128), F32)
                if v == 0:
                    static_recv[n_cols * s_ : n_cols * s_ + n_cols] = missing
                for i in range(ITERS // 2):
                    move_recv[v * (ITERS // 2) + i, n_cols * s_ : n_cols * s_ + n_cols] = missing


    loads[3].wait()
    red_send[0] = w[0] + w[1] + w[2] + w[3]
    stages = [
        [(0, at(0, k)) for k in range(1, n_cols)],
        [(1, (p, col)) for p in row_peers],
        [(2, (p, col)) for p in far_peers],
    ]
    red, count = [], 0
    for stage in stages:
        copies = []
        for s, to in stage:
            copies.append(remote(red_send.at[s], red_recv.at[count], red_s.at[count], red_r.at[count], to))
            count += 1
        red.append(copies)
    for c in red[0]:
        c.start()

    def reduce_stage(s):
        total, first = red_send[s], sum(len(x) for x in red[:s])
        for i, c in enumerate(red[s]):
            c.wait()
            total = total + red_recv[first + i]
        if s + 1 < len(red):
            red_send[s + 1] = total
            for c in red[s + 1]:
                c.start()
        return total

    loads[2].wait()
    d = dest[...]
    along = jnp.broadcast_to(d.astype(F32), (32, 32))
    same = along == along.T
    order_b = lax.broadcasted_iota(jnp.int32, (32, 32), 0)
    order_a = lax.broadcasted_iota(jnp.int32, (32, 32), 1)
    rank = jnp.sum(jnp.where(same & (order_b < order_a), 1.0, 0.0), axis=0, keepdims=True).astype(jnp.int32)
    slot = ((d >> 2) - row + 1) * (n_cols * CAP) + (((d & 3) - col) & 3) * CAP + rank
    slot_iota = lax.broadcasted_iota(jnp.int32, (GROUP * CAP, 32), 0)
    placing = jnp.where(slot_iota == slot, 1.0, 0.0).astype(BF16)

    def send_group(send, recv, ss, rs):
        copies = {}
        for i, (dr, k) in enumerate(group):
            if i != SELF:
                copies[i] = remote(send.at[i], recv.at[i], ss.at[i], rs.at[i], at(dr, k))
                only(there(dr), copies[i].start)
        return copies

    loads[4].wait()
    block_static = jnp.concatenate(
        [ends[...].reshape(32, 128).astype(F32), w[...].reshape(32, 128)], axis=1
    )
    placed = place(placing, block_static)
    for n in range(2):
        static_send[:, n] = placed[:, 128 * n : 128 * n + 128].reshape(GROUP, CAP, 128)
    for n in range(2):
        static_recv[SELF, n] = placed[SELF * CAP : SELF * CAP + CAP, 128 * n : 128 * n + 128]
    static_copies = send_group(static_send, static_recv, static_s, static_r)

    loads[5].wait()
    loads[6].wait()
    for b in range(32):
        both = off_raw[:, 128 * b : 128 * b + 128]
        for n in range(2):
            off[n, b // 8, b % 8 : b % 8 + 1, :] = both[n : n + 1]
    for n in range(2):
        frac[n] = 0.5 + 0.45 * jnp.tanh(off[n])

    finish(halo, halo_to)
    zero_mid = jnp.zeros((112, 128), F32)
    for v in range(2):
        strip = jnp.concatenate([side_recv[0, v], zero_mid, side_recv[1, v]], axis=0).T
        strip = strip.reshape(RT, 8, 128)
        um[v, 0:RT, :, 512:640] = jnp.where(side_in, strip, 0.0) if v == 0 else strip
        below = jnp.where(lane < 64, corner_recv[0, v], corner_recv[1, v])
        above = jnp.where(lane < 64, corner_recv[2, v], corner_recv[3, v])
        if v == 0:
            below = jnp.where(side_in & has_down, below, 0.0)
            above = jnp.where(side_in & has_up, above, 0.0)
            um[0, RT, :, 0:512] = jnp.where(has_down, um[0, RT, :, 0:512], 0.0)
            um[0, RT + 1, :, 0:512] = jnp.where(has_up, um[0, RT + 1, :, 0:512], 0.0)
        um[v, RT, :, 512:640] = below
        um[v, RT + 1, :, 512:640] = above

    def exchange(it):
        full = it + 1 < ITERS
        ss, rs = g_s.at[it], g_r.at[it]
        zero = jnp.zeros((8, 128), F32)

        def assemble(t):
            for j in range(LT + 1):
                js, before = slice(128 * j, 128 * j + 128), slice(128 * j - 128, 128 * j)
                here = beside = prior = zero
                if t < RT:
                    r = [slice(128 * n + 8 * t, 128 * n + 8 * t + 8) for n in range(4)]
                    if j < LT:
                        here = acc[r[0], js] + acc[r[1], js]
                        beside = pltpu.roll(acc[r[2], js] + acc[r[3], js], 1, 1)
                    if j > 0:
                        prior = pltpu.roll(acc[r[2], before] + acc[r[3], before], 1, 1)
                elif t == RT:
                    if j < LT:
                        x = acc[512:520, js]
                        here = jnp.where(sub == 0, x + pltpu.roll(x, 7, 0), 0.0)
                        beside = pltpu.roll(jnp.where(sub == 0, pltpu.roll(x, 6, 0) + pltpu.roll(x, 5, 0), 0.0), 1, 1)
                    if j > 0:
                        x = acc[512:520, before]
                        prior = pltpu.roll(jnp.where(sub == 0, pltpu.roll(x, 6, 0) + pltpu.roll(x, 5, 0), 0.0), 1, 1)
                grid[t, :, js] = here + jnp.where(lane == 0, prior, beside)

        for t in (0, RT - 1, RT):
            assemble(t)
        sends = [
            (grid.at[pl.ds(RT - 1, 2)], g_from_u.at[it], (1, 0)),
            (grid.at[pl.ds(RT - 1, 2), :, pl.ds(384, 256)], g_from_ul.at[it], (1, 1)),
        ]
        if full:
            sends += [
                (grid.at[0], g_from_d, (-1, 0)),
                (grid.at[pl.ds(RT - 1, 2), :, pl.ds(0, 128)], g_from_ur, (1, -1)),
                (grid.at[0, :, pl.ds(384, 256)], g_from_dl, (-1, 1)),
                (grid.at[0, :, pl.ds(0, 128)], g_from_dr, (-1, -1)),
            ]
        copies, targets = [], []

        def send(src, dst, to):
            n = len(copies)
            copies.append(remote(src, dst, ss.at[n], rs.at[n], at(*to)))
            targets.append(to)
            only(there(*to), copies[-1].start)

        for x in sends:
            send(*x)
        for t in list(range(1, RT - 1)) + [RT + 1]:
            assemble(t)
        third = grid[0:RT, :, 384:512].reshape(128, 128).T
        fourth = grid[0:RT, :, 512:640].reshape(128, 128).T
        g_side_r[it, 0] = third[120:128]
        g_side_r[it, 1] = fourth[0:8]
        g_side_r[it, 2] = grid[RT, :, 384:512]
        g_side_r[it, 3] = grid[RT, :, 512:640]
        if full:
            first = grid[0:RT, :, 0:128].reshape(128, 128).T
            g_side_l[0] = first[0:8]
            g_side_l[1] = grid[RT, :, 0:128]
        send(g_side_r.at[it], g_from_l.at[it], (0, 1))
        if full:
            send(g_side_l, g_from_r, (0, -1))
        return copies, targets

    def gather_edges(it):
        full = it + 1 < ITERS
        top = sub == 0
        left0 = (lane == 0) & has_left
        l4, z = slice(512, 640), 0.0
        grid[RT + 1] = jnp.where(has_up, g_from_u[it, 0], z)
        for j in range(LT + 1):
            js = slice(128 * j, 128 * j + 128)
            grid[0, :, js] += jnp.where(top & has_up, g_from_u[it, 1, :, js], z)
        if full:
            grid[RT] += jnp.where(has_down, g_from_d[...], z)
        right_rows = g_from_r[0] if full else jnp.zeros((8, 128), F32)
        strip = jnp.concatenate([right_rows, zero_mid, g_from_l[it, 0]], axis=0).T.reshape(RT, 8, 128)
        grid[0:RT, :, l4] += jnp.where(side_in, strip, z)
        spill = jnp.concatenate([g_from_l[it, 1], jnp.zeros((120, 128), F32)], axis=0).T.reshape(RT, 8, 128)
        grid[0:RT, :, 0:128] += jnp.where(left0, spill, z)
        edge = jnp.where(lane_left, g_from_l[it, 2], z)
        if full:
            edge = edge + jnp.where(lane_right, g_from_r[1], z)
        grid[RT, :, l4] += edge
        grid[RT, :, 0:128] += jnp.where(left0, g_from_l[it, 3], z)
        corner = jnp.where(lane_left, g_from_ul[it, 0, :, 0:128], z)
        corner_top = jnp.where(lane_left, g_from_ul[it, 1, :, 0:128], z)
        if full:
            corner = corner + jnp.where(lane_right, g_from_ur[0], z)
            corner_top = corner_top + jnp.where(lane_right, g_from_ur[1], z)
        grid[RT + 1, :, l4] += jnp.where(has_up, corner, z)
        grid[RT + 1, :, 0:128] += jnp.where(left0 & has_up, g_from_ul[it, 0, :, 128:256], z)
        grid[0, :, l4] += jnp.where(top & has_up, corner_top, z)
        grid[0, :, 0:128] += jnp.where(top & left0 & has_up, g_from_ul[it, 1, :, 128:256], z)
        if full:
            corner = jnp.where(lane_left, g_from_dl[:, 0:128], z) + jnp.where(lane_right, g_from_dr[...], z)
            grid[RT, :, l4] += jnp.where(has_down, corner, z)
            grid[RT, :, 0:128] += jnp.where(left0 & has_down, g_from_dl[:, 128:256], z)
        for j in range(LT + 1):
            js = slice(128 * j, 128 * j + 128)
            folded = pltpu.roll(grid[RT, :, js], 7, 0)
            grid[RT - 1, :, js] += jnp.where((sub == 7) & jnp.logical_not(has_down), folded, z)
        for t in range(RT + 2):
            folded = pltpu.roll(grid[t, :, l4], 127, 1)
            grid[t, :, 384:512] += jnp.where((lane == 127) & jnp.logical_not(has_right), folded, z)

    scale = None
    for it in range(ITERS):
        hjb = functools.partial(hjb_step, lane=lane, sub=sub, row_in=row_in, side_in=side_in)
        den = um.at[1]
        hjb(um.at[0], ua, den)
        hjb(ua, ub, den)
        hjb(ub, ua, den)
        hjb(ua, ub, den)
        if it == 0:
            reduce_stage(0)
        slopes(ub, ua, table, lane, sub)
        sample(table, ub, ua, cells, corners)
        dx0, dx1, dy0 = corners[0], corners[1], corners[2]
        fx, fy = frac[0], frac[1]
        gx = (1.0 - fy) * dx0 + fy * dx1
        gy = (1.0 - fx) * dy0 + fx * (dy0 + (dx1 - dx0))
        hx = 0.5 + 0.45 * jnp.tanh(off[0] - gx)
        hy = 0.5 + 0.45 * jnp.tanh(off[1] - gy)
        placed = place(placing, jnp.concatenate([hx.reshape(32, 128), hy.reshape(32, 128)], axis=1))
        for n in range(2):
            move_send[it, :, n] = placed[:, 128 * n : 128 * n + 128].reshape(GROUP, CAP, 128)
            move_recv[it, SELF, n] = placed[SELF * CAP : SELF * CAP + CAP, 128 * n : 128 * n + 128]
        move_copies = send_group(move_send.at[it], move_recv.at[it], move_s.at[it], move_r.at[it])
        acc[...] = jnp.zeros_like(acc)
        if it + 1 == ITERS:
            value_out[...] = ub[0:RT, :, 0:512]

        step = 4 * (2 * lax.rem(row, 2) - 1)
        kinds = sum(kind * 3**i for i, (kind, _) in enumerate(ORDER))
        dists = sum(k * 4**i for i, (_, k) in enumerate(ORDER))

        def arrive(i, kinds, dists):
            kind, k = lax.rem(kinds, 3) - 1, lax.rem(dists, 4)
            s = SELF + kind * step + k
            from_up, from_down = kind * step > 0, kind * step < 0

            def wait():
                remote(move_send.at[it, s], move_recv.at[it, s], move_s.at[it, s], move_r.at[it, s], at(0, 1)).wait_recv()
                if it == 0:
                    remote(static_send.at[s], static_recv.at[s], static_s.at[s], static_r.at[s], at(0, 1)).wait_recv()

            absent = (from_up & (row == 0)) | (from_down & (row == n_rows - 1))
            pl.when((i > 0) & jnp.logical_not(absent))(wait)
            return s, kinds // 3, dists // 4

        def arrivals(first, batch, i, carry):
            slots = []
            for j in range(batch):
                s, *carry = arrive(first + batch * i + j, *carry)
                slots.append((static_recv[s], move_recv[it, s]))
            deposit(slots, acc)
            return tuple(carry)

        carry = (jnp.int32(kinds), jnp.int32(dists))
        for first, count, batch in BATCHES:
            step_ = functools.partial(arrivals, first, batch)
            carry = step_(0, carry) if count == 1 else lax.fori_loop(0, count, step_, carry)
        copies, targets = exchange(it)
        if it == 0:
            reduce_stage(1)
        for sent in (move_copies, static_copies) if it == 0 else (move_copies,):
            for i, c in sent.items():
                only(there(group[i][0]), c.wait_send)
        finish(copies, targets)
        if it == 0:
            total = reduce_stage(2)
            scale = jnp.float32(n_rows * n_cols * 128 * 512) / jnp.sum(total, keepdims=True)
        gather_edges(it)
        if it + 1 < ITERS:
            um[1] = 0.5 * um[1] + 0.5 * (grid[...] * scale.reshape(1, 1, 1))
        else:
            density_out[...] = 0.5 * um[1, 0:RT, :, 0:512] + 0.5 * (grid[0:RT, :, 0:512] * scale.reshape(1, 1, 1))


def write_out(value, density, value_out, density_out, sems):
    copies = [
        pltpu.make_async_copy(value, value_out, sems.at[0]),
        pltpu.make_async_copy(density, density_out, sems.at[1]),
    ]
    for c in copies:
        c.start()
    for c in copies:
        c.wait()


def body(n_rows, n_cols, terminal_value, density_start, start_cells, offsets, weights, dest_tiles, end_cells):
    any_ = pl.BlockSpec(memory_space=pltpu.HBM)
    vmem = pltpu.VMEM
    dma = pltpu.SemaphoreType.DMA
    tile = jax.ShapeDtypeStruct((RT, 8, 512), F32)
    value, density = pl.pallas_call(
        functools.partial(kernel, n_rows, n_cols),
        out_shape=(tile, tile),
        in_specs=[any_] * 7,
        out_specs=(pl.BlockSpec(memory_space=pltpu.VMEM),) * 2,
        scratch_shapes=[
            vmem((2, RT + 2, 8, 640), F32), vmem((RT + 2, 8, 640), F32), vmem((RT + 2, 8, 640), F32),
            vmem((RT + 2, 8, 640), F32),
            vmem((4, 8, 128), jnp.int32), vmem((2, 4096), F32), vmem((2, 4, 8, 128), F32), vmem((2, 4, 8, 128), F32),
            vmem((4, 8, 128), F32), vmem((4, 8, 128), jnp.int32), vmem((1, 32), jnp.int32), vmem((3, 4, 8, 128), F32), vmem((1040, 256), BF16),
            vmem((2, 2, 8, 128), F32), vmem((2, 2, 8, 128), F32), vmem((4, 2, 8, 128), F32),
            vmem((GROUP, 2, CAP, 128), F32), vmem((GROUP, 2, CAP, 128), F32),
            vmem((ITERS, GROUP, 2, CAP, 128), F32), vmem((ITERS, GROUP, 2, CAP, 128), F32),
            vmem((528, 512), F32),
            vmem((2, 8, 128), F32), vmem((ITERS, 4, 8, 128), F32),
            vmem((ITERS, 2, 8, 640), F32), vmem((8, 640), F32), vmem((ITERS, 4, 8, 128), F32), vmem((2, 8, 128), F32),
            vmem((ITERS, 2, 8, 256), F32), vmem((2, 8, 128), F32), vmem((8, 256), F32), vmem((8, 128), F32),
            vmem((3, 8, 128), F32), vmem((13, 8, 128), F32),
            dma((7,)),
            dma((8,)), dma((8,)), dma((GROUP,)), dma((GROUP,)),
            dma((ITERS, GROUP)), dma((ITERS, GROUP)), dma((ITERS, 8)), dma((ITERS, 8)), dma((13,)), dma((13,)),
        ],
        compiler_params=pltpu.CompilerParams(collective_id=0, has_side_effects=True, vmem_limit_bytes=20 << 20),
        name="crowd",
    )(*(pltpu.with_memory_space_constraint(x, pltpu.HBM) for x in (
        terminal_value.reshape(RT, 8, 512),
        density_start.reshape(RT, 8, 512),
        start_cells.reshape(4, 8, 128),
        offsets,
        weights.reshape(4, 8, 128),
        dest_tiles.reshape(1, 32),
        end_cells.reshape(4, 8, 128),
    )))
    value, density = pl.pallas_call(
        write_out,
        out_shape=(tile, tile),
        in_specs=[pl.BlockSpec(memory_space=pltpu.VMEM)] * 2,
        out_specs=(pl.BlockSpec(memory_space=pltpu.HBM),) * 2,
        scratch_shapes=[dma((2,))],
        compiler_params=pltpu.CompilerParams(vmem_limit_bytes=1 << 20),
        name="write_out",
    )(value, density)
    return value.reshape(128, 512), density.reshape(128, 512)


def solution(mesh):
    both = ("rows", "cols")
    return jax.shard_map(
        functools.partial(body, mesh.shape["rows"], mesh.shape["cols"]),
        mesh=mesh,
        in_specs=(P("rows", "cols"), P("rows", "cols"), P(both), P(None, both), P(both), P(both), P(both)),
        out_specs=(P("rows", "cols"), P("rows", "cols")),
        check_vma=False,
    )
```

```python
import functools

import jax
import jax.numpy as jnp
from jax import lax
from jax.experimental import pallas as pl
from jax.experimental.pallas import tpu as pltpu
from jax.sharding import PartitionSpec as P

HJB_STEPS = 4
ITERS = 2
CAP = 8
RT = 16
LT = 4
ORDER = ((1, 0), (2, 0), (1, 1), (1, 3), (2, 1), (2, 3), (0, 0), (1, 2), (2, 2), (0, 1), (0, 3), (0, 2))
BATCHES = (((0, 3, 2), (6, 3, 2)), ((0, 6, 2),))
F32 = jnp.float32
BF16 = jnp.bfloat16
I16 = jnp.int16
GROUP = 12
SELF = 4


def hjb_step(src, dst, den, lane, sub, row_in, side_in):
    tiles, n_t, n_j = {}, RT + 2, LT + 1
    rolled = {}

    def cell(t, j):
        if (t, j) not in tiles:
            tiles[t, j] = src[t, :, 128 * j : 128 * j + 128]
        return tiles[t, j]

    def roll(t, j, shift, axis):
        key = (t, j, shift, axis)
        if key not in rolled:
            rolled[key] = pltpu.roll(cell(t, j), shift, axis)
        return rolled[key]

    for t in range(n_t):
        for j in range(n_j):
            v = cell(t, j)
            up = jnp.where(sub == 0, roll((t - 1) % n_t, j, 1, 0), roll(t, j, 1, 0))
            down = jnp.where(sub == 7, roll((t + 1) % n_t, j, 7, 0), roll(t, j, 7, 0))
            left = jnp.where(lane == 0, roll(t, (j - 1) % n_j, 1, 1), roll(t, j, 1, 1))
            right = jnp.where(lane == 127, roll(t, (j + 1) % n_j, 127, 1), roll(t, j, 127, 1))
            px = jnp.maximum(v - jnp.minimum(up, down), 0.0)
            py = jnp.maximum(v - jnp.minimum(left, right), 0.0)
            d = den[t, :, 128 * j : 128 * j + 128]
            new = 0.5 * v + 0.125 * ((up + down) + (left + right) - (px * px + py * py) + d)
            if t >= RT:
                new = jnp.where(row_in[t - RT], new, 0.0)
            if j == LT:
                new = jnp.where(side_in, new, 0.0)
            dst[t, :, 128 * j : 128 * j + 128] = new


def slopes(u, u1, table, lane, sub):
    def split(block, first, count):
        turned = block.T[0:count]
        high = turned.astype(BF16)
        table[pl.ds(first, count), pl.ds(0, 128)] = high
        table[pl.ds(first, count), pl.ds(128, 128)] = (turned - high.astype(F32)).astype(BF16)

    for j in range(LT + 1):
        js = slice(128 * j, 128 * j + 128)
        tiles = [u[t, :, js] for t in range(RT + 1)]
        ups = [pltpu.roll(x, 7, 0) for x in tiles]
        dx = [jnp.where(sub == 7, ups[t + 1], ups[t]) - tiles[t] for t in range(RT)]
        split(jnp.concatenate(dx, axis=0), 128 * j, 128 if j < LT else 16)
        if j < LT:
            dy = []
            for t in range(RT):
                near = pltpu.roll(tiles[t], 127, 1)
                far = pltpu.roll(u[t, :, 128 * j + 128 : 128 * j + 256], 127, 1)
                right = jnp.where(lane == 127, far, near)
                u1[t, :, js] = right
                dy.append(right - tiles[t])
            split(jnp.concatenate(dy, axis=0), 528 + 128 * j, 128)
            near = pltpu.roll(tiles[RT], 127, 1)
            far = pltpu.roll(u[RT, :, 128 * j + 128 : 128 * j + 256], 127, 1)
            u1[RT, :, js] = jnp.where(lane == 127, far, near)


def sample(table, u, u1, cells, corners):
    one_cell = cells[0]
    key, idx = one_cell >> 7, one_cell & 127
    zero1 = jnp.zeros((8, 128), F32)
    def agents(t, acc):
        a = t + 1
        cell = cells[a]
        row, col = cell >> 9, cell & 511
        u00, u10, u01, u11 = acc
        kk = key - t * (48 * LT)
        def look(lo, hi):
            nonlocal u00, u10, u01, u11
            for r in range(lo, hi):
                for j in range(LT):
                    part = (t * 6 + r // 8, slice(r % 8, r % 8 + 1), slice(128 * j, 128 * j + 128))
                    here = jnp.take_along_axis(jnp.broadcast_to(u[part], (8, 128)), idx, axis=1)
                    next_ = jnp.take_along_axis(jnp.broadcast_to(u1[part], (8, 128)), idx, axis=1)
                    hit = kk == r * LT + j
                    u00 = jnp.where(hit, here, u00)
                    u01 = jnp.where(hit, next_, u01)
                    hit = kk == (r - 1) * LT + j
                    u10 = jnp.where(hit, here, u10)
                    u11 = jnp.where(hit, next_, u11)
        for h in range(2):
            hot, places = [], []
            for b in range(4 * h, 4 * h + 4):
                r = jnp.tile(jnp.broadcast_to(row[b : b + 1], (16, 128)).astype(I16), (8, 1))
                one = jnp.where(lax.broadcasted_iota(I16, (128, 128), 0) == r, BF16(1), BF16(0))
                hot.append(jnp.concatenate([one, one], axis=0))
                places.append(jnp.broadcast_to(col[b : b + 1], (8, 128)))
            picked = jnp.dot(table[...], jnp.concatenate(hot, axis=1), preferred_element_type=F32)
            place = jnp.concatenate(places, axis=1) - lax.broadcasted_iota(jnp.int32, (8, 512), 0)
            zero = jnp.zeros((8, 512), F32)
            d0, d1, e0 = zero, zero, zero
            for i in range(64):
                here = place == 8 * i
                x = picked[8 * i : 8 * i + 8]
                d0 = jnp.where(here, x, d0)
                d1 = jnp.where(place == 8 * i - 1, x, d1)
                e0 = jnp.where(here, picked[528 + 8 * i : 536 + 8 * i], e0)
            d1 = jnp.where(place == 511, picked[512:520], d1)
            look(24 * h, 24 * h + 24)
            for n, v in enumerate((d0, d1, e0)):
                v = jnp.sum(v, axis=0, keepdims=True)
                for b in range(4):
                    corners[n, a, 4 * h + b : 4 * h + b + 1, :] = v[:, 128 * b : 128 * b + 128]
        return u00, u10, u01, u11
    u00, u10, u01, u11 = lax.fori_loop(0, 3, agents, (zero1, zero1, zero1, zero1))
    corners[0, 0] = u10 - u00
    corners[1, 0] = u11 - u01
    corners[2, 0] = u01 - u00


def exact_parts(v):
    high = v.astype(BF16)
    rest = v - high.astype(F32)
    mid = rest.astype(BF16)
    return high, mid, (rest - mid.astype(F32)).astype(BF16)


def place(placing, v):
    out = None
    for part in exact_parts(v):
        term = jnp.dot(placing, part, preferred_element_type=F32)
        out = term if out is None else out + term
    return out


def factors(static, moves, masses, columns):
    cell = static[0].astype(jnp.int32)
    mass = static[1]
    x, y = moves[0], moves[1]
    row, col = cell >> 9, cell & 511
    upper, lower = mass * (1.0 - x), mass * x
    row_iota = lax.broadcasted_iota(I16, (128, 128), 0)
    col_iota = lax.broadcasted_iota(I16, (512, 128), 0)
    spill_iota = lax.broadcasted_iota(I16, (16, 128), 0)
    parts = []
    for v in (upper * (1.0 - y), lower * (1.0 - y), upper * y, lower * y):
        high = v.astype(BF16).astype(F32)
        parts.append((high, v - high))

    def spread(v, b, dtype, copies):
        tile = jnp.broadcast_to(v[b : b + 1], (16, 128)).astype(dtype)
        return jnp.tile(tile, (copies, 1)) if copies > 1 else tile

    zero = BF16(0)
    for b in range(CAP):
        r = spread(row, b, I16, 8)
        q = spread(col, b, I16, 32)
        on_upper = row_iota == r
        on_lower = row_iota == r + I16(1)
        spill = jnp.zeros((16, 128), BF16)
        block = []
        for n in range(4):
            kind, p = n // 2, n % 2
            v = spread(parts[2 * kind][p], b, BF16, 8)
            w = spread(parts[2 * kind + 1][p], b, BF16, 8)
            block.append(jnp.where(on_upper, v, jnp.where(on_lower, w, zero)))
            spill = jnp.where(spill_iota == I16(n), w[0:16], spill)
        block.append(jnp.where(r[0:16] == I16(127), spill, zero))
        masses.append(jnp.concatenate(block, axis=0))
        columns.append(jnp.where(col_iota == q, BF16(1), zero))


def deposit(slots, acc):
    masses, columns = [], []
    for static, moves in slots:
        factors(static, moves, masses, columns)
    acc[...] += lax.dot_general(
        jnp.concatenate(masses, axis=1),
        jnp.concatenate(columns, axis=1),
        (((1,), (1,)), ((), ())),
        preferred_element_type=F32,
    )


class Place:
    def __init__(self, n_rows, n_cols):
        self.n_rows, self.n_cols = n_rows, n_cols
        self.row, self.col = lax.axis_index("rows"), lax.axis_index("cols")
        self.has_up, self.has_down = self.row > 0, self.row < n_rows - 1
        self.has_left, self.has_right = self.col > 0, self.col < n_cols - 1
        self.lane = lax.broadcasted_iota(jnp.int32, (8, 128), 1)
        self.sub = lax.broadcasted_iota(jnp.int32, (8, 128), 0)
        self.lane_right = self.lane < jnp.where(self.has_right, 8, 0)
        self.lane_left = self.lane >= jnp.where(self.has_left, 120, 128)
        self.side_in = self.lane_right | self.lane_left

    def at(self, dr, dc):
        n_rows, n_cols = self.n_rows, self.n_cols
        return (lax.rem(self.row + dr + n_rows, n_rows), lax.rem(self.col + dc + n_cols, n_cols))

    def there(self, dr, dc=0):
        rows_ok = {-1: self.has_up, 0: None, 1: self.has_down}[dr]
        cols_ok = {-1: self.has_left, 0: None, 1: self.has_right}[dc]
        if rows_ok is None or cols_ok is None:
            return cols_ok if rows_ok is None else rows_ok
        return rows_ok & cols_ok

    def greet(self, peers):
        barrier = pltpu.get_barrier_semaphore()
        count = jnp.int32(0)
        for cond, to in peers:
            only(cond, lambda to=to: pl.semaphore_signal(
                barrier, inc=1, device_id=to, device_id_type=pl.DeviceIdType.MESH
            ))
            count = count + (1 if cond is None else cond.astype(jnp.int32))
        return barrier, count

    def finish(self, copies, targets):
        for c, (dr, dc) in zip(copies, targets):
            only(self.there(dr, dc), c.wait_send)
            only(self.there(-dr, -dc), c.wait_recv)


def only(cond, act):
    if cond is None:
        act()
    else:
        pl.when(cond)(act)


def remote(src, dst, s, r, to):
    return pltpu.make_async_remote_copy(
        src_ref=src, dst_ref=dst, send_sem=s, recv_sem=r,
        device_id=to, device_id_type=pl.DeviceIdType.MESH,
    )


def halo_kernel(
    n_rows, n_cols,
    u_in, m_in, off_in, w_in, dest_in, end_in,
    um, off, frac, static_send, placing_out, mass_out,
    off_raw, w, ends, dest, side_send, side_recv, corner_recv,
    load_sem, halo_s, halo_r,
):
    at_ = Place(n_rows, n_cols)
    at, there, lane = at_.at, at_.there, at_.lane
    row, col, side_in = at_.row, at_.col, at_.side_in
    has_up, has_down = at_.has_up, at_.has_down
    loads = [
        (u_in, um.at[0, pl.ds(0, RT), :, pl.ds(0, 512)]),
        (m_in, um.at[1, pl.ds(0, RT), :, pl.ds(0, 512)]),
        (dest_in, dest), (w_in, w), (end_in, ends), (off_in, off_raw),
    ]
    loads = [pltpu.make_async_copy(a, b, load_sem.at[i]) for i, (a, b) in enumerate(loads)]
    for c in loads:
        c.start()
    halo_to = [(-1, 0), (1, 0), (-1, -1), (-1, 1), (1, -1), (1, 1), (0, -1), (0, 1)]
    barrier, greeted = at_.greet([(there(*to), at(*to)) for to in halo_to])
    for c in loads[:2]:
        c.wait()
    for v in range(2):
        first = um[v, 0:RT, :, 0:128].reshape(128, 128).T
        last = um[v, 0:RT, :, 384:512].reshape(128, 128).T
        side_send[0, v] = first[0:8]
        side_send[1, v] = last[120:128]
    pl.semaphore_wait(barrier, greeted)

    halo = [
        remote(um.at[:, 0, :, pl.ds(0, 512)], um.at[:, RT, :, pl.ds(0, 512)], halo_s.at[0], halo_r.at[0], at(-1, 0)),
        remote(um.at[:, RT - 1, :, pl.ds(0, 512)], um.at[:, RT + 1, :, pl.ds(0, 512)], halo_s.at[1], halo_r.at[1], at(1, 0)),
        remote(um.at[:, 0, :, pl.ds(0, 128)], corner_recv.at[0], halo_s.at[2], halo_r.at[2], at(-1, -1)),
        remote(um.at[:, 0, :, pl.ds(384, 128)], corner_recv.at[1], halo_s.at[3], halo_r.at[3], at(-1, 1)),
        remote(um.at[:, RT - 1, :, pl.ds(0, 128)], corner_recv.at[2], halo_s.at[4], halo_r.at[4], at(1, -1)),
        remote(um.at[:, RT - 1, :, pl.ds(384, 128)], corner_recv.at[3], halo_s.at[5], halo_r.at[5], at(1, 1)),
        remote(side_send.at[0], side_recv.at[0], halo_s.at[6], halo_r.at[6], at(0, -1)),
        remote(side_send.at[1], side_recv.at[1], halo_s.at[7], halo_r.at[7], at(0, 1)),
    ]
    for c, to in zip(halo, halo_to):
        only(there(*to), c.start)

    loads[3].wait()
    mass_out[...] = w[0] + w[1] + w[2] + w[3]

    loads[2].wait()
    d = dest[...]
    along = jnp.broadcast_to(d.astype(F32), (32, 32))
    same = along == along.T
    order_b = lax.broadcasted_iota(jnp.int32, (32, 32), 0)
    order_a = lax.broadcasted_iota(jnp.int32, (32, 32), 1)
    rank = jnp.sum(jnp.where(same & (order_b < order_a), 1.0, 0.0), axis=0, keepdims=True).astype(jnp.int32)
    slot = ((d >> 2) - row + 1) * (n_cols * CAP) + (((d & 3) - col) & 3) * CAP + rank
    slot_iota = lax.broadcasted_iota(jnp.int32, (GROUP * CAP, 32), 0)
    placing = jnp.where(slot_iota == slot, 1.0, 0.0).astype(BF16)
    placing_out[...] = placing

    loads[4].wait()
    block_static = jnp.concatenate(
        [ends[...].reshape(32, 128).astype(F32), w[...].reshape(32, 128)], axis=1
    )
    placed = place(placing, block_static)
    for n in range(2):
        static_send[:, n] = placed[:, 128 * n : 128 * n + 128].reshape(GROUP, CAP, 128)
    loads[5].wait()
    for b in range(32):
        both = off_raw[:, 128 * b : 128 * b + 128]
        for n in range(2):
            off[n, b // 8, b % 8 : b % 8 + 1, :] = both[n : n + 1]
    for n in range(2):
        frac[n] = 0.5 + 0.45 * jnp.tanh(off[n])

    at_.finish(halo, halo_to)
    zero_mid = jnp.zeros((112, 128), F32)
    for v in range(2):
        strip = jnp.concatenate([side_recv[0, v], zero_mid, side_recv[1, v]], axis=0).T
        strip = strip.reshape(RT, 8, 128)
        um[v, 0:RT, :, 512:640] = jnp.where(side_in, strip, 0.0) if v == 0 else strip
        below = jnp.where(lane < 64, corner_recv[0, v], corner_recv[1, v])
        above = jnp.where(lane < 64, corner_recv[2, v], corner_recv[3, v])
        if v == 0:
            below = jnp.where(side_in & has_down, below, 0.0)
            above = jnp.where(side_in & has_up, above, 0.0)
            um[0, RT, :, 0:512] = jnp.where(has_down, um[0, RT, :, 0:512], 0.0)
            um[0, RT + 1, :, 0:512] = jnp.where(has_up, um[0, RT + 1, :, 0:512], 0.0)
        um[v, RT, :, 512:640] = below
        um[v, RT + 1, :, 512:640] = above


def kernel(
    n_rows, n_cols,
    um, off, frac, static_send, placing_in, mass_in, cells_in,
    value_out, density_out,
    ua, ub, grid, relaxed, cells, corners, table,
    static_recv, move_send, move_recv,
    acc,
    g_side_l, g_side_r, g_from_u, g_from_d, g_from_l, g_from_r, g_from_ul, g_from_ur, g_from_dl, g_from_dr,
    red_send, red_recv,
    load_sem,
    static_s, static_r, move_s, move_r, g_s, g_r, red_s, red_r,
):
    at_ = Place(n_rows, n_cols)
    at, there, finish, lane, sub = at_.at, at_.there, at_.finish, at_.lane, at_.sub
    row, col, side_in = at_.row, at_.col, at_.side_in
    has_up, has_down, has_left, has_right = at_.has_up, at_.has_down, at_.has_left, at_.has_right
    lane_right, lane_left = at_.lane_right, at_.lane_left
    row_in = (has_down, has_up)
    load = pltpu.make_async_copy(cells_in, cells, load_sem.at[0])
    load.start()

    group = [(dr, k) for dr in (-1, 0, 1) for k in range(n_cols)]
    near = row % 8
    base = row - near
    row_peers = [base + (near + j) % 8 for j in range(1, 8)]
    far_peers = [lax.rem(row + 8 * j, n_rows) for j in range(1, 4)]
    barrier, greeted = at_.greet(
        [(there(dr), at(dr, k)) for dr, k in group if (dr, k) != (0, 0)]
        + [(None, (p, col)) for p in row_peers + far_peers]
    )
    placing = placing_in[...]
    zero_mid = jnp.zeros((112, 128), F32)

    for v in range(2):
        for s_, cond in ((2, has_up), (0, has_down)):

            @pl.when(jnp.logical_not(cond))
            def _(s_=s_, v=v):
                missing = jnp.zeros((n_cols, 2, CAP, 128), F32)
                if v == 0:
                    static_recv[n_cols * s_ : n_cols * s_ + n_cols] = missing
                for i in range(ITERS // 2):
                    move_recv[v * (ITERS // 2) + i, n_cols * s_ : n_cols * s_ + n_cols] = missing
    for n in range(2):
        static_recv[SELF, n] = static_send[SELF, n]

    red_send[0] = mass_in[...]
    stages = [
        [(0, at(0, k)) for k in range(1, n_cols)],
        [(1, (p, col)) for p in row_peers],
        [(2, (p, col)) for p in far_peers],
    ]
    red, count = [], 0
    for stage in stages:
        copies = []
        for s, to in stage:
            copies.append(remote(red_send.at[s], red_recv.at[count], red_s.at[count], red_r.at[count], to))
            count += 1
        red.append(copies)
    def reduce_stage(s):
        total, first = red_send[s], sum(len(x) for x in red[:s])
        for i, c in enumerate(red[s]):
            c.wait()
            total = total + red_recv[first + i]
        if s + 1 < len(red):
            red_send[s + 1] = total
            for c in red[s + 1]:
                c.start()
        return total

    def send_group(send, recv, ss, rs):
        copies = {}
        for i, (dr, k) in enumerate(group):
            if i != SELF:
                copies[i] = remote(send.at[i], recv.at[i], ss.at[i], rs.at[i], at(dr, k))
                only(there(dr), copies[i].start)
        return copies

    def exchange(it):
        full = it + 1 < ITERS
        ss, rs = g_s.at[it], g_r.at[it]
        zero = jnp.zeros((8, 128), F32)

        def assemble(t):
            for j in range(LT + 1):
                js, before = slice(128 * j, 128 * j + 128), slice(128 * j - 128, 128 * j)
                here = beside = prior = zero
                if t < RT:
                    r = [slice(128 * n + 8 * t, 128 * n + 8 * t + 8) for n in range(4)]
                    if j < LT:
                        here = acc[r[0], js] + acc[r[1], js]
                        beside = pltpu.roll(acc[r[2], js] + acc[r[3], js], 1, 1)
                    if j > 0:
                        prior = pltpu.roll(acc[r[2], before] + acc[r[3], before], 1, 1)
                elif t == RT:
                    if j < LT:
                        x = acc[512:520, js]
                        here = jnp.where(sub == 0, x + pltpu.roll(x, 7, 0), 0.0)
                        beside = pltpu.roll(jnp.where(sub == 0, pltpu.roll(x, 6, 0) + pltpu.roll(x, 5, 0), 0.0), 1, 1)
                    if j > 0:
                        x = acc[512:520, before]
                        prior = pltpu.roll(jnp.where(sub == 0, pltpu.roll(x, 6, 0) + pltpu.roll(x, 5, 0), 0.0), 1, 1)
                grid[t, :, js] = here + jnp.where(lane == 0, prior, beside)

        for t in (0, RT - 1, RT):
            assemble(t)
        sends = [
            (grid.at[pl.ds(RT - 1, 2)], g_from_u.at[it], (1, 0)),
            (grid.at[pl.ds(RT - 1, 2), :, pl.ds(384, 256)], g_from_ul.at[it], (1, 1)),
        ]
        if full:
            sends += [
                (grid.at[0], g_from_d, (-1, 0)),
                (grid.at[pl.ds(RT - 1, 2), :, pl.ds(0, 128)], g_from_ur, (1, -1)),
                (grid.at[0, :, pl.ds(384, 256)], g_from_dl, (-1, 1)),
                (grid.at[0, :, pl.ds(0, 128)], g_from_dr, (-1, -1)),
            ]
        copies, targets = [], []

        def send(src, dst, to):
            n = len(copies)
            copies.append(remote(src, dst, ss.at[n], rs.at[n], at(*to)))
            targets.append(to)
            only(there(*to), copies[-1].start)

        for x in sends:
            send(*x)
        for t in list(range(1, RT - 1)) + [RT + 1]:
            assemble(t)
        third = grid[0:RT, :, 384:512].reshape(128, 128).T
        fourth = grid[0:RT, :, 512:640].reshape(128, 128).T
        g_side_r[it, 0] = third[120:128]
        g_side_r[it, 1] = fourth[0:8]
        g_side_r[it, 2] = grid[RT, :, 384:512]
        g_side_r[it, 3] = grid[RT, :, 512:640]
        if full:
            first = grid[0:RT, :, 0:128].reshape(128, 128).T
            g_side_l[0] = first[0:8]
            g_side_l[1] = grid[RT, :, 0:128]
        send(g_side_r.at[it], g_from_l.at[it], (0, 1))
        if full:
            send(g_side_l, g_from_r, (0, -1))
        return copies, targets

    def gather_edges(it):
        full = it + 1 < ITERS
        top = sub == 0
        left0 = (lane == 0) & has_left
        l4, z = slice(512, 640), 0.0
        grid[RT + 1] = jnp.where(has_up, g_from_u[it, 0], z)
        for j in range(LT + 1):
            js = slice(128 * j, 128 * j + 128)
            grid[0, :, js] += jnp.where(top & has_up, g_from_u[it, 1, :, js], z)
        if full:
            grid[RT] += jnp.where(has_down, g_from_d[...], z)
        right_rows = g_from_r[0] if full else jnp.zeros((8, 128), F32)
        strip = jnp.concatenate([right_rows, zero_mid, g_from_l[it, 0]], axis=0).T.reshape(RT, 8, 128)
        grid[0:RT, :, l4] += jnp.where(side_in, strip, z)
        spill = jnp.concatenate([g_from_l[it, 1], jnp.zeros((120, 128), F32)], axis=0).T.reshape(RT, 8, 128)
        grid[0:RT, :, 0:128] += jnp.where(left0, spill, z)
        edge = jnp.where(lane_left, g_from_l[it, 2], z)
        if full:
            edge = edge + jnp.where(lane_right, g_from_r[1], z)
        grid[RT, :, l4] += edge
        grid[RT, :, 0:128] += jnp.where(left0, g_from_l[it, 3], z)
        corner = jnp.where(lane_left, g_from_ul[it, 0, :, 0:128], z)
        corner_top = jnp.where(lane_left, g_from_ul[it, 1, :, 0:128], z)
        if full:
            corner = corner + jnp.where(lane_right, g_from_ur[0], z)
            corner_top = corner_top + jnp.where(lane_right, g_from_ur[1], z)
        grid[RT + 1, :, l4] += jnp.where(has_up, corner, z)
        grid[RT + 1, :, 0:128] += jnp.where(left0 & has_up, g_from_ul[it, 0, :, 128:256], z)
        grid[0, :, l4] += jnp.where(top & has_up, corner_top, z)
        grid[0, :, 0:128] += jnp.where(top & left0 & has_up, g_from_ul[it, 1, :, 128:256], z)
        if full:
            corner = jnp.where(lane_left, g_from_dl[:, 0:128], z) + jnp.where(lane_right, g_from_dr[...], z)
            grid[RT, :, l4] += jnp.where(has_down, corner, z)
            grid[RT, :, 0:128] += jnp.where(left0 & has_down, g_from_dl[:, 128:256], z)
        for j in range(LT + 1):
            js = slice(128 * j, 128 * j + 128)
            folded = pltpu.roll(grid[RT, :, js], 7, 0)
            grid[RT - 1, :, js] += jnp.where((sub == 7) & jnp.logical_not(has_down), folded, z)
        for t in range(RT + 2):
            folded = pltpu.roll(grid[t, :, l4], 127, 1)
            grid[t, :, 384:512] += jnp.where((lane == 127) & jnp.logical_not(has_right), folded, z)

    scale = None
    for it in range(ITERS):
        hjb = functools.partial(hjb_step, lane=lane, sub=sub, row_in=row_in, side_in=side_in)
        den = um.at[1] if it == 0 else relaxed
        hjb(um.at[0], ua, den)
        hjb(ua, ub, den)
        hjb(ub, ua, den)
        hjb(ua, ub, den)
        if it == 0:
            load.wait()
        slopes(ub, ua, table, lane, sub)
        sample(table, ub, ua, cells, corners)
        if it == 0:
            pl.semaphore_wait(barrier, greeted)
            static_copies = send_group(static_send, static_recv, static_s, static_r)
            for c in red[0]:
                c.start()
        dx0, dx1, dy0 = corners[0], corners[1], corners[2]
        fx, fy = frac[0], frac[1]
        gx = (1.0 - fy) * dx0 + fy * dx1
        gy = (1.0 - fx) * dy0 + fx * (dy0 + (dx1 - dx0))
        hx = 0.5 + 0.45 * jnp.tanh(off[0] - gx)
        hy = 0.5 + 0.45 * jnp.tanh(off[1] - gy)
        placed = place(placing, jnp.concatenate([hx.reshape(32, 128), hy.reshape(32, 128)], axis=1))
        for n in range(2):
            move_send[it, :, n] = placed[:, 128 * n : 128 * n + 128].reshape(GROUP, CAP, 128)
            move_recv[it, SELF, n] = placed[SELF * CAP : SELF * CAP + CAP, 128 * n : 128 * n + 128]
        move_copies = send_group(move_send.at[it], move_recv.at[it], move_s.at[it], move_r.at[it])
        acc[...] = jnp.zeros_like(acc)
        if it + 1 == ITERS:
            value_out[...] = ub[0:RT, :, 0:512]

        step = 4 * (2 * lax.rem(row, 2) - 1)
        kinds = sum(kind * 3**i for i, (kind, _) in enumerate(ORDER))
        dists = sum(k * 4**i for i, (_, k) in enumerate(ORDER))

        def arrive(i, kinds, dists):
            kind, k = lax.rem(kinds, 3) - 1, lax.rem(dists, 4)
            s = SELF + kind * step + k
            from_up, from_down = kind * step > 0, kind * step < 0

            def wait():
                remote(move_send.at[it, s], move_recv.at[it, s], move_s.at[it, s], move_r.at[it, s], at(0, 1)).wait_recv()
                if it == 0:
                    remote(static_send.at[s], static_recv.at[s], static_s.at[s], static_r.at[s], at(0, 1)).wait_recv()

            absent = (from_up & (row == 0)) | (from_down & (row == n_rows - 1))
            pl.when((i > 0) & jnp.logical_not(absent))(wait)
            return s, kinds // 3, dists // 4

        def arrivals(first, batch, i, carry):
            slots = []
            for j in range(batch):
                s, *carry = arrive(first + batch * i + j, *carry)
                slots.append((static_recv[s], move_recv[it, s]))
            deposit(slots, acc)
            return tuple(carry)

        carry = (jnp.int32(kinds), jnp.int32(dists))
        for n, (first, count, batch) in enumerate(BATCHES[it]):
            if n > 0:
                reduce_stage(0)
            carry = lax.fori_loop(0, count, functools.partial(arrivals, first, batch), carry)
        copies, targets = exchange(it)
        if it == 0:
            reduce_stage(1)
        for sent in (move_copies, static_copies) if it == 0 else (move_copies,):
            for i, c in sent.items():
                only(there(group[i][0]), c.wait_send)
        finish(copies, targets)
        if it == 0:
            total = reduce_stage(2)
            scale = jnp.float32(n_rows * n_cols * 128 * 512) / jnp.sum(total, keepdims=True)
        gather_edges(it)
        if it + 1 < ITERS:
            relaxed[...] = 0.5 * um[1] + 0.5 * (grid[...] * scale.reshape(1, 1, 1))
        else:
            density_out[...] = 0.5 * relaxed[0:RT, :, 0:512] + 0.5 * (grid[0:RT, :, 0:512] * scale.reshape(1, 1, 1))


def write_out(value, density, value_out, density_out, sems):
    copies = [
        pltpu.make_async_copy(value, value_out, sems.at[0]),
        pltpu.make_async_copy(density, density_out, sems.at[1]),
    ]
    for c in copies:
        c.start()
    for c in copies:
        c.wait()


def body(n_rows, n_cols, terminal_value, density_start, start_cells, offsets, weights, dest_tiles, end_cells):
    any_ = pl.BlockSpec(memory_space=pltpu.HBM)
    vmem = pltpu.VMEM
    dma = pltpu.SemaphoreType.DMA
    tile = jax.ShapeDtypeStruct((RT, 8, 512), F32)
    whole = pl.BlockSpec(memory_space=pltpu.VMEM)
    stay = lambda x: pltpu.with_memory_space_constraint(x, pltpu.HBM)
    shape = jax.ShapeDtypeStruct
    prepared = pl.pallas_call(
        functools.partial(halo_kernel, n_rows, n_cols),
        out_shape=(
            shape((2, RT + 2, 8, 640), F32), shape((2, 4, 8, 128), F32), shape((2, 4, 8, 128), F32),
            shape((GROUP, 2, CAP, 128), F32), shape((GROUP * CAP, 32), BF16), shape((8, 128), F32),
        ),
        in_specs=[any_] * 6,
        out_specs=(whole,) * 6,
        scratch_shapes=[
            vmem((2, 4096), F32), vmem((4, 8, 128), F32), vmem((4, 8, 128), jnp.int32), vmem((1, 32), jnp.int32),
            vmem((2, 2, 8, 128), F32), vmem((2, 2, 8, 128), F32), vmem((4, 2, 8, 128), F32),
            dma((6,)), dma((8,)), dma((8,)),
        ],
        compiler_params=pltpu.CompilerParams(collective_id=1, has_side_effects=True, vmem_limit_bytes=8 << 20),
        name="halos",
    )(
        stay(terminal_value.reshape(RT, 8, 512)),
        stay(density_start.reshape(RT, 8, 512)),
        stay(offsets),
        stay(weights.reshape(4, 8, 128)),
        stay(dest_tiles.reshape(1, 32)),
        stay(end_cells.reshape(4, 8, 128)),
    )
    value, density = pl.pallas_call(
        functools.partial(kernel, n_rows, n_cols),
        out_shape=(tile, tile),
        in_specs=[whole] * 6 + [any_],
        out_specs=(whole, whole),
        scratch_shapes=[
            vmem((RT + 2, 8, 640), F32), vmem((RT + 2, 8, 640), F32), vmem((RT + 2, 8, 640), F32), vmem((RT + 2, 8, 640), F32),
            vmem((4, 8, 128), jnp.int32), vmem((3, 4, 8, 128), F32), vmem((1040, 256), BF16),
            vmem((GROUP, 2, CAP, 128), F32), vmem((ITERS, GROUP, 2, CAP, 128), F32), vmem((ITERS, GROUP, 2, CAP, 128), F32),
            vmem((528, 512), F32),
            vmem((2, 8, 128), F32), vmem((ITERS, 4, 8, 128), F32),
            vmem((ITERS, 2, 8, 640), F32), vmem((8, 640), F32), vmem((ITERS, 4, 8, 128), F32), vmem((2, 8, 128), F32),
            vmem((ITERS, 2, 8, 256), F32), vmem((2, 8, 128), F32), vmem((8, 256), F32), vmem((8, 128), F32),
            vmem((3, 8, 128), F32), vmem((13, 8, 128), F32),
            dma((1,)),
            dma((GROUP,)), dma((GROUP,)),
            dma((ITERS, GROUP)), dma((ITERS, GROUP)), dma((ITERS, 8)), dma((ITERS, 8)), dma((13,)), dma((13,)),
        ],
        compiler_params=pltpu.CompilerParams(collective_id=0, has_side_effects=True, vmem_limit_bytes=20 << 20),
        name="crowd",
    )(*prepared, stay(start_cells.reshape(4, 8, 128)))
    value, density = pl.pallas_call(
        write_out,
        out_shape=(tile, tile),
        in_specs=[pl.BlockSpec(memory_space=pltpu.VMEM)] * 2,
        out_specs=(pl.BlockSpec(memory_space=pltpu.HBM),) * 2,
        scratch_shapes=[dma((2,))],
        compiler_params=pltpu.CompilerParams(vmem_limit_bytes=1 << 20),
        name="write_out",
    )(value, density)
    return value.reshape(128, 512), density.reshape(128, 512)


def solution(mesh):
    both = ("rows", "cols")
    return jax.shard_map(
        functools.partial(body, mesh.shape["rows"], mesh.shape["cols"]),
        mesh=mesh,
        in_specs=(P("rows", "cols"), P("rows", "cols"), P(both), P(None, both), P(both), P(both), P(both)),
        out_specs=(P("rows", "cols"), P("rows", "cols")),
        check_vma=False,
    )
```

```python
import functools

import jax
import jax.numpy as jnp
from jax import lax
from jax.experimental import pallas as pl
from jax.experimental.pallas import tpu as pltpu
from jax.sharding import PartitionSpec as P

HJB_STEPS = 4
ITERS = 2
CAP = 8
RT = 16
LT = 4
ORDER = ((1, 0), (2, 0), (1, 1), (1, 3), (2, 1), (2, 3), (0, 0), (1, 2), (2, 2), (0, 1), (0, 3), (0, 2))
BATCHES = (((0, 3, 2), (6, 3, 2)), ((0, 6, 2),))
F32 = jnp.float32
BF16 = jnp.bfloat16
I16 = jnp.int16
GROUP = 12
SELF = 4


def hjb_step(src, dst, den, lane, sub, row_in, side_in):
    tiles, n_t, n_j = {}, RT + 2, LT + 1
    rolled = {}

    def cell(t, j):
        if (t, j) not in tiles:
            tiles[t, j] = src[t, :, 128 * j : 128 * j + 128]
        return tiles[t, j]

    def roll(t, j, shift, axis):
        key = (t, j, shift, axis)
        if key not in rolled:
            rolled[key] = pltpu.roll(cell(t, j), shift, axis)
        return rolled[key]

    for t in range(n_t):
        for j in range(n_j):
            v = cell(t, j)
            up = jnp.where(sub == 0, roll((t - 1) % n_t, j, 1, 0), roll(t, j, 1, 0))
            down = jnp.where(sub == 7, roll((t + 1) % n_t, j, 7, 0), roll(t, j, 7, 0))
            left = jnp.where(lane == 0, roll(t, (j - 1) % n_j, 1, 1), roll(t, j, 1, 1))
            right = jnp.where(lane == 127, roll(t, (j + 1) % n_j, 127, 1), roll(t, j, 127, 1))
            px = jnp.maximum(v - jnp.minimum(up, down), 0.0)
            py = jnp.maximum(v - jnp.minimum(left, right), 0.0)
            d = den[t, :, 128 * j : 128 * j + 128]
            new = 0.5 * v + 0.125 * ((up + down) + (left + right) - (px * px + py * py) + d)
            if t >= RT:
                new = jnp.where(row_in[t - RT], new, 0.0)
            if j == LT:
                new = jnp.where(side_in, new, 0.0)
            dst[t, :, 128 * j : 128 * j + 128] = new


def slopes(u, u1, table, lane, sub):
    def split(block, first, count):
        turned = block.T[0:count]
        high = turned.astype(BF16)
        table[pl.ds(first, count), pl.ds(0, 128)] = high
        table[pl.ds(first, count), pl.ds(128, 128)] = (turned - high.astype(F32)).astype(BF16)

    for j in range(LT + 1):
        js = slice(128 * j, 128 * j + 128)
        tiles = [u[t, :, js] for t in range(RT + 1)]
        ups = [pltpu.roll(x, 7, 0) for x in tiles]
        dx = [jnp.where(sub == 7, ups[t + 1], ups[t]) - tiles[t] for t in range(RT)]
        split(jnp.concatenate(dx, axis=0), 128 * j, 128 if j < LT else 16)
        if j < LT:
            dy = []
            for t in range(RT):
                near = pltpu.roll(tiles[t], 127, 1)
                far = pltpu.roll(u[t, :, 128 * j + 128 : 128 * j + 256], 127, 1)
                right = jnp.where(lane == 127, far, near)
                u1[t, :, js] = right
                dy.append(right - tiles[t])
            split(jnp.concatenate(dy, axis=0), 528 + 128 * j, 128)
            near = pltpu.roll(tiles[RT], 127, 1)
            far = pltpu.roll(u[RT, :, 128 * j + 128 : 128 * j + 256], 127, 1)
            u1[RT, :, js] = jnp.where(lane == 127, far, near)


def sample(table, u, u1, cells, corners):
    one_cell = cells[0]
    key, idx = one_cell >> 7, one_cell & 127
    zero1 = jnp.zeros((8, 128), F32)
    def agents(t, acc):
        a = t + 1
        cell = cells[a]
        row, col = cell >> 9, cell & 511
        u00, u10, u01, u11 = acc
        kk = key - t * (48 * LT)
        def look(lo, hi):
            nonlocal u00, u10, u01, u11
            for r in range(lo, hi):
                for j in range(LT):
                    part = (t * 6 + r // 8, slice(r % 8, r % 8 + 1), slice(128 * j, 128 * j + 128))
                    here = jnp.take_along_axis(jnp.broadcast_to(u[part], (8, 128)), idx, axis=1)
                    next_ = jnp.take_along_axis(jnp.broadcast_to(u1[part], (8, 128)), idx, axis=1)
                    hit = kk == r * LT + j
                    u00 = jnp.where(hit, here, u00)
                    u01 = jnp.where(hit, next_, u01)
                    hit = kk == (r - 1) * LT + j
                    u10 = jnp.where(hit, here, u10)
                    u11 = jnp.where(hit, next_, u11)
        for h in range(2):
            hot, places = [], []
            for b in range(4 * h, 4 * h + 4):
                r = jnp.tile(jnp.broadcast_to(row[b : b + 1], (16, 128)).astype(I16), (8, 1))
                one = jnp.where(lax.broadcasted_iota(I16, (128, 128), 0) == r, BF16(1), BF16(0))
                hot.append(jnp.concatenate([one, one], axis=0))
                places.append(jnp.broadcast_to(col[b : b + 1], (8, 128)))
            picked = jnp.dot(table[...], jnp.concatenate(hot, axis=1), preferred_element_type=F32)
            place = jnp.concatenate(places, axis=1) - lax.broadcasted_iota(jnp.int32, (8, 512), 0)
            zero = jnp.zeros((8, 512), F32)
            d0, d1, e0 = zero, zero, zero
            for i in range(64):
                here = place == 8 * i
                x = picked[8 * i : 8 * i + 8]
                d0 = jnp.where(here, x, d0)
                d1 = jnp.where(place == 8 * i - 1, x, d1)
                e0 = jnp.where(here, picked[528 + 8 * i : 536 + 8 * i], e0)
            d1 = jnp.where(place == 511, picked[512:520], d1)
            look(24 * h, 24 * h + 24)
            for n, v in enumerate((d0, d1, e0)):
                v = jnp.sum(v, axis=0, keepdims=True)
                for b in range(4):
                    corners[n, a, 4 * h + b : 4 * h + b + 1, :] = v[:, 128 * b : 128 * b + 128]
        return u00, u10, u01, u11
    u00, u10, u01, u11 = lax.fori_loop(0, 3, agents, (zero1, zero1, zero1, zero1))
    corners[0, 0] = u10 - u00
    corners[1, 0] = u11 - u01
    corners[2, 0] = u01 - u00


def exact_parts(v):
    high = v.astype(BF16)
    rest = v - high.astype(F32)
    mid = rest.astype(BF16)
    return high, mid, (rest - mid.astype(F32)).astype(BF16)


def place(placing, v):
    out = None
    for part in exact_parts(v):
        term = jnp.dot(placing, part, preferred_element_type=F32)
        out = term if out is None else out + term
    return out


def factors(static, moves, masses, columns):
    cell = static[0].astype(jnp.int32)
    mass = static[1]
    x, y = moves[0], moves[1]
    row, col = cell >> 9, cell & 511
    upper, lower = mass * (1.0 - x), mass * x
    row_iota = lax.broadcasted_iota(I16, (128, 128), 0)
    col_iota = lax.broadcasted_iota(I16, (512, 128), 0)
    spill_iota = lax.broadcasted_iota(I16, (16, 128), 0)
    parts = []
    for v in (upper * (1.0 - y), lower * (1.0 - y), upper * y, lower * y):
        high = v.astype(BF16).astype(F32)
        parts.append((high, v - high))

    def spread(v, b, dtype, copies):
        tile = jnp.broadcast_to(v[b : b + 1], (16, 128)).astype(dtype)
        return jnp.tile(tile, (copies, 1)) if copies > 1 else tile

    zero = BF16(0)
    for b in range(CAP):
        r = spread(row, b, I16, 8)
        q = spread(col, b, I16, 32)
        on_upper = row_iota == r
        on_lower = row_iota == r + I16(1)
        spill = jnp.zeros((16, 128), BF16)
        block = []
        for n in range(4):
            kind, p = n // 2, n % 2
            v = spread(parts[2 * kind][p], b, BF16, 8)
            w = spread(parts[2 * kind + 1][p], b, BF16, 8)
            block.append(jnp.where(on_upper, v, jnp.where(on_lower, w, zero)))
            spill = jnp.where(spill_iota == I16(n), w[0:16], spill)
        block.append(jnp.where(r[0:16] == I16(127), spill, zero))
        masses.append(jnp.concatenate(block, axis=0))
        columns.append(jnp.where(col_iota == q, BF16(1), zero))


def deposit(slots, acc):
    masses, columns = [], []
    for static, moves in slots:
        factors(static, moves, masses, columns)
    acc[...] += lax.dot_general(
        jnp.concatenate(masses, axis=1),
        jnp.concatenate(columns, axis=1),
        (((1,), (1,)), ((), ())),
        preferred_element_type=F32,
    )


class Place:
    def __init__(self, n_rows, n_cols):
        self.n_rows, self.n_cols = n_rows, n_cols
        self.row, self.col = lax.axis_index("rows"), lax.axis_index("cols")
        self.has_up, self.has_down = self.row > 0, self.row < n_rows - 1
        self.has_left, self.has_right = self.col > 0, self.col < n_cols - 1
        self.lane = lax.broadcasted_iota(jnp.int32, (8, 128), 1)
        self.sub = lax.broadcasted_iota(jnp.int32, (8, 128), 0)
        self.lane_right = self.lane < jnp.where(self.has_right, 8, 0)
        self.lane_left = self.lane >= jnp.where(self.has_left, 120, 128)
        self.side_in = self.lane_right | self.lane_left

    def at(self, dr, dc):
        n_rows, n_cols = self.n_rows, self.n_cols
        return (lax.rem(self.row + dr + n_rows, n_rows), lax.rem(self.col + dc + n_cols, n_cols))

    def there(self, dr, dc=0):
        rows_ok = {-1: self.has_up, 0: None, 1: self.has_down}[dr]
        cols_ok = {-1: self.has_left, 0: None, 1: self.has_right}[dc]
        if rows_ok is None or cols_ok is None:
            return cols_ok if rows_ok is None else rows_ok
        return rows_ok & cols_ok

    def greet(self, peers):
        barrier = pltpu.get_barrier_semaphore()
        count = jnp.int32(0)
        for cond, to in peers:
            only(cond, lambda to=to: pl.semaphore_signal(
                barrier, inc=1, device_id=to, device_id_type=pl.DeviceIdType.MESH
            ))
            count = count + (1 if cond is None else cond.astype(jnp.int32))
        return barrier, count

    def finish(self, copies, targets):
        for c, (dr, dc) in zip(copies, targets):
            only(self.there(dr, dc), c.wait_send)
            only(self.there(-dr, -dc), c.wait_recv)


def only(cond, act):
    if cond is None:
        act()
    else:
        pl.when(cond)(act)


def remote(src, dst, s, r, to):
    return pltpu.make_async_remote_copy(
        src_ref=src, dst_ref=dst, send_sem=s, recv_sem=r,
        device_id=to, device_id_type=pl.DeviceIdType.MESH,
    )


def halo_kernel(
    n_rows, n_cols,
    u_in, m_in, off_in, w_in, dest_in, end_in,
    um, off, frac, static_send, placing_out, mass_out,
    off_raw, w, ends, dest, side_send, side_recv, corner_recv,
    load_sem, halo_s, halo_r,
):
    at_ = Place(n_rows, n_cols)
    at, there, lane = at_.at, at_.there, at_.lane
    row, col, side_in = at_.row, at_.col, at_.side_in
    has_up, has_down = at_.has_up, at_.has_down
    loads = [
        (u_in, um.at[0, pl.ds(0, RT), :, pl.ds(0, 512)]),
        (m_in, um.at[1, pl.ds(0, RT), :, pl.ds(0, 512)]),
        (dest_in, dest), (w_in, w), (end_in, ends), (off_in, off_raw),
    ]
    loads = [pltpu.make_async_copy(a, b, load_sem.at[i]) for i, (a, b) in enumerate(loads)]
    for c in loads:
        c.start()
    halo_to = [(-1, 0), (1, 0), (-1, -1), (-1, 1), (1, -1), (1, 1), (0, -1), (0, 1)]
    barrier, greeted = at_.greet([(there(*to), at(*to)) for to in halo_to])
    for c in loads[:2]:
        c.wait()
    for v in range(2):
        first = um[v, 0:RT, :, 0:128].reshape(128, 128).T
        last = um[v, 0:RT, :, 384:512].reshape(128, 128).T
        side_send[0, v] = first[0:8]
        side_send[1, v] = last[120:128]
    pl.semaphore_wait(barrier, greeted)

    halo = [
        remote(um.at[:, 0, :, pl.ds(0, 512)], um.at[:, RT, :, pl.ds(0, 512)], halo_s.at[0], halo_r.at[0], at(-1, 0)),
        remote(um.at[:, RT - 1, :, pl.ds(0, 512)], um.at[:, RT + 1, :, pl.ds(0, 512)], halo_s.at[1], halo_r.at[1], at(1, 0)),
        remote(um.at[:, 0, :, pl.ds(0, 128)], corner_recv.at[0], halo_s.at[2], halo_r.at[2], at(-1, -1)),
        remote(um.at[:, 0, :, pl.ds(384, 128)], corner_recv.at[1], halo_s.at[3], halo_r.at[3], at(-1, 1)),
        remote(um.at[:, RT - 1, :, pl.ds(0, 128)], corner_recv.at[2], halo_s.at[4], halo_r.at[4], at(1, -1)),
        remote(um.at[:, RT - 1, :, pl.ds(384, 128)], corner_recv.at[3], halo_s.at[5], halo_r.at[5], at(1, 1)),
        remote(side_send.at[0], side_recv.at[0], halo_s.at[6], halo_r.at[6], at(0, -1)),
        remote(side_send.at[1], side_recv.at[1], halo_s.at[7], halo_r.at[7], at(0, 1)),
    ]
    for c, to in zip(halo, halo_to):
        only(there(*to), c.start)

    loads[3].wait()
    mass_out[...] = w[0] + w[1] + w[2] + w[3]

    loads[2].wait()
    d = dest[...]
    along = jnp.broadcast_to(d.astype(F32), (32, 32))
    same = along == along.T
    order_b = lax.broadcasted_iota(jnp.int32, (32, 32), 0)
    order_a = lax.broadcasted_iota(jnp.int32, (32, 32), 1)
    rank = jnp.sum(jnp.where(same & (order_b < order_a), 1.0, 0.0), axis=0, keepdims=True).astype(jnp.int32)
    slot = ((d >> 2) - row + 1) * (n_cols * CAP) + (((d & 3) - col) & 3) * CAP + rank
    slot_iota = lax.broadcasted_iota(jnp.int32, (GROUP * CAP, 32), 0)
    placing = jnp.where(slot_iota == slot, 1.0, 0.0).astype(BF16)
    placing_out[...] = placing

    loads[4].wait()
    block_static = jnp.concatenate(
        [ends[...].reshape(32, 128).astype(F32), w[...].reshape(32, 128)], axis=1
    )
    placed = place(placing, block_static)
    for n in range(2):
        static_send[:, n] = placed[:, 128 * n : 128 * n + 128].reshape(GROUP, CAP, 128)
    loads[5].wait()
    for b in range(32):
        both = off_raw[:, 128 * b : 128 * b + 128]
        for n in range(2):
            off[n, b // 8, b % 8 : b % 8 + 1, :] = both[n : n + 1]
    for n in range(2):
        frac[n] = 0.5 + 0.45 * jnp.tanh(off[n])

    at_.finish(halo, halo_to)
    zero_mid = jnp.zeros((112, 128), F32)
    for v in range(2):
        strip = jnp.concatenate([side_recv[0, v], zero_mid, side_recv[1, v]], axis=0).T
        strip = strip.reshape(RT, 8, 128)
        um[v, 0:RT, :, 512:640] = jnp.where(side_in, strip, 0.0) if v == 0 else strip
        below = jnp.where(lane < 64, corner_recv[0, v], corner_recv[1, v])
        above = jnp.where(lane < 64, corner_recv[2, v], corner_recv[3, v])
        if v == 0:
            below = jnp.where(side_in & has_down, below, 0.0)
            above = jnp.where(side_in & has_up, above, 0.0)
            um[0, RT, :, 0:512] = jnp.where(has_down, um[0, RT, :, 0:512], 0.0)
            um[0, RT + 1, :, 0:512] = jnp.where(has_up, um[0, RT + 1, :, 0:512], 0.0)
        um[v, RT, :, 512:640] = below
        um[v, RT + 1, :, 512:640] = above


def kernel(
    n_rows, n_cols,
    um, off, frac, static_send, placing_in, mass_in, cells_in,
    value_out, density_out,
    ua, ub, grid, relaxed, cells, corners, table,
    static_recv, move_send, move_recv,
    acc,
    g_side_l, g_side_r, g_down, g_from_u, g_from_d, g_from_l, g_from_r, g_from_ul, g_from_ur, g_from_dl, g_from_dr,
    red_send, red_recv,
    load_sem,
    static_s, static_r, move_s, move_r, g_s, g_r, red_s, red_r,
):
    at_ = Place(n_rows, n_cols)
    at, there, finish, lane, sub = at_.at, at_.there, at_.finish, at_.lane, at_.sub
    row, col, side_in = at_.row, at_.col, at_.side_in
    has_up, has_down, has_left, has_right = at_.has_up, at_.has_down, at_.has_left, at_.has_right
    lane_right, lane_left = at_.lane_right, at_.lane_left
    row_in = (has_down, has_up)
    load = pltpu.make_async_copy(cells_in, cells, load_sem.at[0])
    load.start()

    group = [(dr, k) for dr in (-1, 0, 1) for k in range(n_cols)]
    near = row % 8
    base = row - near
    row_peers = [base + (near + j) % 8 for j in range(1, 8)]
    far_peers = [lax.rem(row + 8 * j, n_rows) for j in range(1, 4)]
    barrier, greeted = at_.greet(
        [(there(dr), at(dr, k)) for dr, k in group if (dr, k) != (0, 0)]
        + [(None, (p, col)) for p in row_peers + far_peers]
    )
    placing = placing_in[...]
    zero_mid = jnp.zeros((112, 128), F32)

    for v in range(2):
        for s_, cond in ((2, has_up), (0, has_down)):

            @pl.when(jnp.logical_not(cond))
            def _(s_=s_, v=v):
                missing = jnp.zeros((n_cols, 2, CAP, 128), F32)
                if v == 0:
                    static_recv[n_cols * s_ : n_cols * s_ + n_cols] = missing
                for i in range(ITERS // 2):
                    move_recv[v * (ITERS // 2) + i, n_cols * s_ : n_cols * s_ + n_cols] = missing
    for n in range(2):
        static_recv[SELF, n] = static_send[SELF, n]

    red_send[0] = mass_in[...]
    stages = [
        [(0, at(0, k)) for k in range(1, n_cols)],
        [(1, (p, col)) for p in row_peers],
        [(2, (p, col)) for p in far_peers],
    ]
    red, count = [], 0
    for stage in stages:
        copies = []
        for s, to in stage:
            copies.append(remote(red_send.at[s], red_recv.at[count], red_s.at[count], red_r.at[count], to))
            count += 1
        red.append(copies)
    def reduce_stage(s):
        total, first = red_send[s], sum(len(x) for x in red[:s])
        for i, c in enumerate(red[s]):
            c.wait()
            total = total + red_recv[first + i]
        if s + 1 < len(red):
            red_send[s + 1] = total
            for c in red[s + 1]:
                c.start()
        return total

    def send_group(send, recv, ss, rs):
        copies = {}
        for i, (dr, k) in enumerate(group):
            if i != SELF:
                copies[i] = remote(send.at[i], recv.at[i], ss.at[i], rs.at[i], at(dr, k))
                only(there(dr), copies[i].start)
        return copies

    def exchange(it):
        full = it + 1 < ITERS
        ss, rs = g_s.at[it], g_r.at[it]
        zero = jnp.zeros((8, 128), F32)

        def assemble(t):
            for j in range(LT + 1):
                js, before = slice(128 * j, 128 * j + 128), slice(128 * j - 128, 128 * j)
                here = beside = prior = zero
                if t < RT:
                    r = [slice(128 * n + 8 * t, 128 * n + 8 * t + 8) for n in range(4)]
                    if j < LT:
                        here = acc[r[0], js] + acc[r[1], js]
                        beside = pltpu.roll(acc[r[2], js] + acc[r[3], js], 1, 1)
                    if j > 0:
                        prior = pltpu.roll(acc[r[2], before] + acc[r[3], before], 1, 1)
                elif t == RT:
                    if j < LT:
                        x = acc[512:520, js]
                        here = jnp.where(sub == 0, x + pltpu.roll(x, 7, 0), 0.0)
                        beside = pltpu.roll(jnp.where(sub == 0, pltpu.roll(x, 6, 0) + pltpu.roll(x, 5, 0), 0.0), 1, 1)
                    if j > 0:
                        x = acc[512:520, before]
                        prior = pltpu.roll(jnp.where(sub == 0, pltpu.roll(x, 6, 0) + pltpu.roll(x, 5, 0), 0.0), 1, 1)
                grid[t, :, js] = here + jnp.where(lane == 0, prior, beside)

        for t in (0, RT - 1, RT):
            assemble(t)
        for j in range(LT + 1):
            js = slice(128 * j, 128 * j + 128)
            g_down[it, :, js] = jnp.where(sub == 0, grid[RT, :, js], grid[RT - 1, :, js])
        sends = [
            (g_down.at[it], g_from_u.at[it], (1, 0)),
            (g_down.at[it, :, pl.ds(384, 256)], g_from_ul.at[it], (1, 1)),
        ]
        if full:
            sends += [
                (grid.at[0], g_from_d, (-1, 0)),
                (g_down.at[it, :, pl.ds(0, 128)], g_from_ur, (1, -1)),
                (grid.at[0, :, pl.ds(384, 256)], g_from_dl, (-1, 1)),
                (grid.at[0, :, pl.ds(0, 128)], g_from_dr, (-1, -1)),
            ]
        copies, targets = [], []

        def send(src, dst, to):
            n = len(copies)
            copies.append(remote(src, dst, ss.at[n], rs.at[n], at(*to)))
            targets.append(to)
            only(there(*to), copies[-1].start)

        for x in sends:
            send(*x)
        for t in list(range(1, RT - 1)) + [RT + 1]:
            assemble(t)
        third = grid[0:RT, :, 384:512].reshape(128, 128).T
        fourth = grid[0:RT, :, 512:640].reshape(128, 128).T
        g_side_r[it, 0] = third[120:128]
        g_side_r[it, 1] = fourth[0:8]
        g_side_r[it, 2] = grid[RT, :, 384:512]
        g_side_r[it, 3] = grid[RT, :, 512:640]
        if full:
            first = grid[0:RT, :, 0:128].reshape(128, 128).T
            g_side_l[0] = first[0:8]
            g_side_l[1] = grid[RT, :, 0:128]
        send(g_side_r.at[it], g_from_l.at[it], (0, 1))
        if full:
            send(g_side_l, g_from_r, (0, -1))
        return copies, targets

    def gather_edges(it):
        full = it + 1 < ITERS
        top = sub == 0
        left0 = (lane == 0) & has_left
        l4, z = slice(512, 640), 0.0
        above = (sub > 0) & has_up
        for j in range(LT + 1):
            js = slice(128 * j, 128 * j + 128)
            grid[0, :, js] += jnp.where(top & has_up, g_from_u[it, :, js], z)
            if full:
                grid[RT + 1, :, js] = jnp.where(above, g_from_u[it, :, js], z)
        if full:
            grid[RT] += jnp.where(has_down, g_from_d[...], z)
        right_rows = g_from_r[0] if full else jnp.zeros((8, 128), F32)
        strip = jnp.concatenate([right_rows, zero_mid, g_from_l[it, 0]], axis=0).T.reshape(RT, 8, 128)
        grid[0:RT, :, l4] += jnp.where(side_in, strip, z)
        spill = jnp.concatenate([g_from_l[it, 1], jnp.zeros((120, 128), F32)], axis=0).T.reshape(RT, 8, 128)
        grid[0:RT, :, 0:128] += jnp.where(left0, spill, z)
        edge = jnp.where(lane_left, g_from_l[it, 2], z)
        if full:
            edge = edge + jnp.where(lane_right, g_from_r[1], z)
        grid[RT, :, l4] += edge
        grid[RT, :, 0:128] += jnp.where(left0, g_from_l[it, 3], z)
        corner = jnp.where(lane_left, g_from_ul[it, :, 0:128], z)
        if full:
            corner = corner + jnp.where(lane_right, g_from_ur[...], z)
            grid[RT + 1, :, l4] += jnp.where(above, corner, z)
            grid[RT + 1, :, 0:128] += jnp.where(left0 & above, g_from_ul[it, :, 128:256], z)
        grid[0, :, l4] += jnp.where(top & has_up, corner, z)
        grid[0, :, 0:128] += jnp.where(top & left0 & has_up, g_from_ul[it, :, 128:256], z)
        if full:
            corner = jnp.where(lane_left, g_from_dl[:, 0:128], z) + jnp.where(lane_right, g_from_dr[...], z)
            grid[RT, :, l4] += jnp.where(has_down, corner, z)
            grid[RT, :, 0:128] += jnp.where(left0 & has_down, g_from_dl[:, 128:256], z)
        for j in range(LT + 1):
            js = slice(128 * j, 128 * j + 128)
            folded = pltpu.roll(grid[RT, :, js], 7, 0)
            grid[RT - 1, :, js] += jnp.where((sub == 7) & jnp.logical_not(has_down), folded, z)
        for t in range(RT + 2 if full else RT):
            folded = pltpu.roll(grid[t, :, l4], 127, 1)
            grid[t, :, 384:512] += jnp.where((lane == 127) & jnp.logical_not(has_right), folded, z)

    scale = None
    for it in range(ITERS):
        hjb = functools.partial(hjb_step, lane=lane, sub=sub, row_in=row_in, side_in=side_in)
        den = um.at[1] if it == 0 else relaxed
        hjb(um.at[0], ua, den)
        hjb(ua, ub, den)
        hjb(ub, ua, den)
        hjb(ua, ub, den)
        if it == 0:
            load.wait()
        slopes(ub, ua, table, lane, sub)
        sample(table, ub, ua, cells, corners)
        if it == 0:
            pl.semaphore_wait(barrier, greeted)
            static_copies = send_group(static_send, static_recv, static_s, static_r)
            for c in red[0]:
                c.start()
        dx0, dx1, dy0 = corners[0], corners[1], corners[2]
        fx, fy = frac[0], frac[1]
        gx = (1.0 - fy) * dx0 + fy * dx1
        gy = (1.0 - fx) * dy0 + fx * (dy0 + (dx1 - dx0))
        hx = 0.5 + 0.45 * jnp.tanh(off[0] - gx)
        hy = 0.5 + 0.45 * jnp.tanh(off[1] - gy)
        placed = place(placing, jnp.concatenate([hx.reshape(32, 128), hy.reshape(32, 128)], axis=1))
        for n in range(2):
            move_send[it, :, n] = placed[:, 128 * n : 128 * n + 128].reshape(GROUP, CAP, 128)
            move_recv[it, SELF, n] = placed[SELF * CAP : SELF * CAP + CAP, 128 * n : 128 * n + 128]
        move_copies = send_group(move_send.at[it], move_recv.at[it], move_s.at[it], move_r.at[it])
        acc[...] = jnp.zeros_like(acc)
        if it + 1 == ITERS:
            value_out[...] = ub[0:RT, :, 0:512]

        step = 4 * (2 * lax.rem(row, 2) - 1)
        kinds = sum(kind * 3**i for i, (kind, _) in enumerate(ORDER))
        dists = sum(k * 4**i for i, (_, k) in enumerate(ORDER))

        def arrive(i, kinds, dists):
            kind, k = lax.rem(kinds, 3) - 1, lax.rem(dists, 4)
            s = SELF + kind * step + k
            from_up, from_down = kind * step > 0, kind * step < 0

            def wait():
                remote(move_send.at[it, s], move_recv.at[it, s], move_s.at[it, s], move_r.at[it, s], at(0, 1)).wait_recv()
                if it == 0:
                    remote(static_send.at[s], static_recv.at[s], static_s.at[s], static_r.at[s], at(0, 1)).wait_recv()

            absent = (from_up & (row == 0)) | (from_down & (row == n_rows - 1))
            pl.when((i > 0) & jnp.logical_not(absent))(wait)
            return s, kinds // 3, dists // 4

        def arrivals(first, batch, i, carry):
            slots = []
            for j in range(batch):
                s, *carry = arrive(first + batch * i + j, *carry)
                slots.append((static_recv[s], move_recv[it, s]))
            deposit(slots, acc)
            return tuple(carry)

        carry = (jnp.int32(kinds), jnp.int32(dists))
        for n, (first, count, batch) in enumerate(BATCHES[it]):
            if n > 0:
                reduce_stage(0)
            carry = lax.fori_loop(0, count, functools.partial(arrivals, first, batch), carry)
        copies, targets = exchange(it)
        if it == 0:
            reduce_stage(1)
        for sent in (move_copies, static_copies) if it == 0 else (move_copies,):
            for i, c in sent.items():
                only(there(group[i][0]), c.wait_send)
        finish(copies, targets)
        if it == 0:
            total = reduce_stage(2)
            scale = jnp.float32(n_rows * n_cols * 128 * 512) / jnp.sum(total, keepdims=True)
        gather_edges(it)
        if it + 1 < ITERS:
            relaxed[...] = 0.5 * um[1] + 0.5 * (grid[...] * scale.reshape(1, 1, 1))
        else:
            density_out[...] = 0.5 * relaxed[0:RT, :, 0:512] + 0.5 * (grid[0:RT, :, 0:512] * scale.reshape(1, 1, 1))


def write_out(value, density, value_out, density_out, sems):
    copies = [
        pltpu.make_async_copy(value, value_out, sems.at[0]),
        pltpu.make_async_copy(density, density_out, sems.at[1]),
    ]
    for c in copies:
        c.start()
    for c in copies:
        c.wait()


def body(n_rows, n_cols, terminal_value, density_start, start_cells, offsets, weights, dest_tiles, end_cells):
    any_ = pl.BlockSpec(memory_space=pltpu.HBM)
    vmem = pltpu.VMEM
    dma = pltpu.SemaphoreType.DMA
    tile = jax.ShapeDtypeStruct((RT, 8, 512), F32)
    whole = pl.BlockSpec(memory_space=pltpu.VMEM)
    stay = lambda x: pltpu.with_memory_space_constraint(x, pltpu.HBM)
    shape = jax.ShapeDtypeStruct
    prepared = pl.pallas_call(
        functools.partial(halo_kernel, n_rows, n_cols),
        out_shape=(
            shape((2, RT + 2, 8, 640), F32), shape((2, 4, 8, 128), F32), shape((2, 4, 8, 128), F32),
            shape((GROUP, 2, CAP, 128), F32), shape((GROUP * CAP, 32), BF16), shape((8, 128), F32),
        ),
        in_specs=[any_] * 6,
        out_specs=(whole,) * 6,
        scratch_shapes=[
            vmem((2, 4096), F32), vmem((4, 8, 128), F32), vmem((4, 8, 128), jnp.int32), vmem((1, 32), jnp.int32),
            vmem((2, 2, 8, 128), F32), vmem((2, 2, 8, 128), F32), vmem((4, 2, 8, 128), F32),
            dma((6,)), dma((8,)), dma((8,)),
        ],
        compiler_params=pltpu.CompilerParams(collective_id=1, has_side_effects=True, vmem_limit_bytes=8 << 20),
        name="halos",
    )(
        stay(terminal_value.reshape(RT, 8, 512)),
        stay(density_start.reshape(RT, 8, 512)),
        stay(offsets),
        stay(weights.reshape(4, 8, 128)),
        stay(dest_tiles.reshape(1, 32)),
        stay(end_cells.reshape(4, 8, 128)),
    )
    value, density = pl.pallas_call(
        functools.partial(kernel, n_rows, n_cols),
        out_shape=(tile, tile),
        in_specs=[whole] * 6 + [any_],
        out_specs=(whole, whole),
        scratch_shapes=[
            vmem((RT + 2, 8, 640), F32), vmem((RT + 2, 8, 640), F32), vmem((RT + 2, 8, 640), F32), vmem((RT + 2, 8, 640), F32),
            vmem((4, 8, 128), jnp.int32), vmem((3, 4, 8, 128), F32), vmem((1040, 256), BF16),
            vmem((GROUP, 2, CAP, 128), F32), vmem((ITERS, GROUP, 2, CAP, 128), F32), vmem((ITERS, GROUP, 2, CAP, 128), F32),
            vmem((528, 512), F32),
            vmem((2, 8, 128), F32), vmem((ITERS, 4, 8, 128), F32), vmem((ITERS, 8, 640), F32),
            vmem((ITERS, 8, 640), F32), vmem((8, 640), F32), vmem((ITERS, 4, 8, 128), F32), vmem((2, 8, 128), F32),
            vmem((ITERS, 8, 256), F32), vmem((8, 128), F32), vmem((8, 256), F32), vmem((8, 128), F32),
            vmem((3, 8, 128), F32), vmem((13, 8, 128), F32),
            dma((1,)),
            dma((GROUP,)), dma((GROUP,)),
            dma((ITERS, GROUP)), dma((ITERS, GROUP)), dma((ITERS, 8)), dma((ITERS, 8)), dma((13,)), dma((13,)),
        ],
        compiler_params=pltpu.CompilerParams(collective_id=0, has_side_effects=True, vmem_limit_bytes=20 << 20),
        name="crowd",
    )(*prepared, stay(start_cells.reshape(4, 8, 128)))
    value, density = pl.pallas_call(
        write_out,
        out_shape=(tile, tile),
        in_specs=[pl.BlockSpec(memory_space=pltpu.VMEM)] * 2,
        out_specs=(pl.BlockSpec(memory_space=pltpu.HBM),) * 2,
        scratch_shapes=[dma((2,))],
        compiler_params=pltpu.CompilerParams(vmem_limit_bytes=1 << 20),
        name="write_out",
    )(value, density)
    return value.reshape(128, 512), density.reshape(128, 512)


def solution(mesh):
    both = ("rows", "cols")
    return jax.shard_map(
        functools.partial(body, mesh.shape["rows"], mesh.shape["cols"]),
        mesh=mesh,
        in_specs=(P("rows", "cols"), P("rows", "cols"), P(both), P(None, both), P(both), P(both), P(both)),
        out_specs=(P("rows", "cols"), P("rows", "cols")),
        check_vma=False,
    )
```

```python
import functools

import jax
import jax.numpy as jnp
from jax import lax
from jax.experimental import pallas as pl
from jax.experimental.pallas import tpu as pltpu
from jax.sharding import PartitionSpec as P

HJB_STEPS = 4
ITERS = 2
CAP = 8
RT = 16
LT = 4
ORDER = ((1, 0), (2, 0), (1, 1), (1, 3), (2, 1), (2, 3), (0, 0), (1, 2), (2, 2), (0, 1), (0, 3), (0, 2))
BATCHES = (((0, 3, 2), (6, 3, 2)), ((0, 6, 2),))
F32 = jnp.float32
BF16 = jnp.bfloat16
I16 = jnp.int16
GROUP = 12
SELF = 4


def hjb_step(src, dst, den, lane, sub, row_in, side_in):
    tiles, n_t, n_j = {}, RT + 2, LT + 1
    rolled = {}

    def cell(t, j):
        if (t, j) not in tiles:
            tiles[t, j] = src[t, :, 128 * j : 128 * j + 128]
        return tiles[t, j]

    def roll(t, j, shift, axis):
        key = (t, j, shift, axis)
        if key not in rolled:
            rolled[key] = pltpu.roll(cell(t, j), shift, axis)
        return rolled[key]

    for t in range(n_t):
        for j in range(n_j):
            v = cell(t, j)
            up = jnp.where(sub == 0, roll((t - 1) % n_t, j, 1, 0), roll(t, j, 1, 0))
            down = jnp.where(sub == 7, roll((t + 1) % n_t, j, 7, 0), roll(t, j, 7, 0))
            left = jnp.where(lane == 0, roll(t, (j - 1) % n_j, 1, 1), roll(t, j, 1, 1))
            right = jnp.where(lane == 127, roll(t, (j + 1) % n_j, 127, 1), roll(t, j, 127, 1))
            px = jnp.maximum(v - jnp.minimum(up, down), 0.0)
            py = jnp.maximum(v - jnp.minimum(left, right), 0.0)
            d = den[t, :, 128 * j : 128 * j + 128]
            new = 0.5 * v + 0.125 * ((up + down) + (left + right) - (px * px + py * py) + d)
            if t >= RT:
                new = jnp.where(row_in[t - RT], new, 0.0)
            if j == LT:
                new = jnp.where(side_in, new, 0.0)
            dst[t, :, 128 * j : 128 * j + 128] = new


def slopes(u, u1, table, lane, sub):
    def split(block, first, count):
        turned = block.T[0:count]
        high = turned.astype(BF16)
        table[pl.ds(first, count), pl.ds(0, 128)] = high
        table[pl.ds(first, count), pl.ds(128, 128)] = (turned - high.astype(F32)).astype(BF16)

    for j in range(LT + 1):
        js = slice(128 * j, 128 * j + 128)
        tiles = [u[t, :, js] for t in range(RT + 1)]
        ups = [pltpu.roll(x, 7, 0) for x in tiles]
        dx = [jnp.where(sub == 7, ups[t + 1], ups[t]) - tiles[t] for t in range(RT)]
        split(jnp.concatenate(dx, axis=0), 128 * j, 128 if j < LT else 16)
        if j < LT:
            dy = []
            for t in range(RT):
                near = pltpu.roll(tiles[t], 127, 1)
                far = pltpu.roll(u[t, :, 128 * j + 128 : 128 * j + 256], 127, 1)
                right = jnp.where(lane == 127, far, near)
                u1[t, :, js] = right
                dy.append(right - tiles[t])
            split(jnp.concatenate(dy, axis=0), 528 + 128 * j, 128)
            near = pltpu.roll(tiles[RT], 127, 1)
            far = pltpu.roll(u[RT, :, 128 * j + 128 : 128 * j + 256], 127, 1)
            u1[RT, :, js] = jnp.where(lane == 127, far, near)


def sample(table, u, u1, cells, corners):
    one_cell = cells[0]
    key, idx = one_cell >> 7, one_cell & 127
    zero1 = jnp.zeros((8, 128), F32)
    def agents(t, acc):
        a = t + 1
        cell = cells[a]
        row, col = cell >> 9, cell & 511
        u00, u10, u01, u11 = acc
        kk = key - t * (48 * LT)
        def look(lo, hi):
            nonlocal u00, u10, u01, u11
            for r in range(lo, hi):
                for j in range(LT):
                    part = (t * 6 + r // 8, slice(r % 8, r % 8 + 1), slice(128 * j, 128 * j + 128))
                    here = jnp.take_along_axis(jnp.broadcast_to(u[part], (8, 128)), idx, axis=1)
                    next_ = jnp.take_along_axis(jnp.broadcast_to(u1[part], (8, 128)), idx, axis=1)
                    hit = kk == r * LT + j
                    u00 = jnp.where(hit, here, u00)
                    u01 = jnp.where(hit, next_, u01)
                    hit = kk == (r - 1) * LT + j
                    u10 = jnp.where(hit, here, u10)
                    u11 = jnp.where(hit, next_, u11)
        for h in range(2):
            hot, places = [], []
            for b in range(4 * h, 4 * h + 4):
                r = jnp.tile(jnp.broadcast_to(row[b : b + 1], (16, 128)).astype(I16), (8, 1))
                one = jnp.where(lax.broadcasted_iota(I16, (128, 128), 0) == r, BF16(1), BF16(0))
                hot.append(jnp.concatenate([one, one], axis=0))
                places.append(jnp.broadcast_to(col[b : b + 1], (8, 128)))
            picked = jnp.dot(table[...], jnp.concatenate(hot, axis=1), preferred_element_type=F32)
            place = jnp.concatenate(places, axis=1) - lax.broadcasted_iota(jnp.int32, (8, 512), 0)
            zero = jnp.zeros((8, 512), F32)
            d0, d1, e0 = zero, zero, zero
            for i in range(64):
                here = place == 8 * i
                x = picked[8 * i : 8 * i + 8]
                d0 = jnp.where(here, x, d0)
                d1 = jnp.where(place == 8 * i - 1, x, d1)
                e0 = jnp.where(here, picked[528 + 8 * i : 536 + 8 * i], e0)
            d1 = jnp.where(place == 511, picked[512:520], d1)
            look(24 * h, 24 * h + 24)
            for n, v in enumerate((d0, d1, e0)):
                v = jnp.sum(v, axis=0, keepdims=True)
                for b in range(4):
                    corners[n, a, 4 * h + b : 4 * h + b + 1, :] = v[:, 128 * b : 128 * b + 128]
        return u00, u10, u01, u11
    u00, u10, u01, u11 = lax.fori_loop(0, 3, agents, (zero1, zero1, zero1, zero1))
    corners[0, 0] = u10 - u00
    corners[1, 0] = u11 - u01
    corners[2, 0] = u01 - u00


def exact_parts(v):
    high = v.astype(BF16)
    rest = v - high.astype(F32)
    mid = rest.astype(BF16)
    return high, mid, (rest - mid.astype(F32)).astype(BF16)


def place(placing, v):
    out = None
    for part in exact_parts(v):
        term = jnp.dot(placing, part, preferred_element_type=F32)
        out = term if out is None else out + term
    return out


def factors(static, moves, masses, columns):
    cell = static[0].astype(jnp.int32)
    mass = static[1]
    x, y = moves[0], moves[1]
    row, col = cell >> 9, cell & 511
    upper, lower = mass * (1.0 - x), mass * x
    row_iota = lax.broadcasted_iota(I16, (128, 128), 0)
    col_iota = lax.broadcasted_iota(I16, (512, 128), 0)
    spill_iota = lax.broadcasted_iota(I16, (16, 128), 0)
    parts = []
    for v in (upper * (1.0 - y), lower * (1.0 - y), upper * y, lower * y):
        high = v.astype(BF16).astype(F32)
        parts.append((high, v - high))

    def spread(v, b, dtype, copies):
        tile = jnp.broadcast_to(v[b : b + 1], (16, 128)).astype(dtype)
        return jnp.tile(tile, (copies, 1)) if copies > 1 else tile

    zero = BF16(0)
    for b in range(CAP):
        r = spread(row, b, I16, 8)
        q = spread(col, b, I16, 32)
        on_upper = row_iota == r
        on_lower = row_iota == r + I16(1)
        spill = jnp.zeros((16, 128), BF16)
        block = []
        for n in range(4):
            kind, p = n // 2, n % 2
            v = spread(parts[2 * kind][p], b, BF16, 8)
            w = spread(parts[2 * kind + 1][p], b, BF16, 8)
            block.append(jnp.where(on_upper, v, jnp.where(on_lower, w, zero)))
            spill = jnp.where(spill_iota == I16(n), w[0:16], spill)
        block.append(jnp.where(r[0:16] == I16(127), spill, zero))
        masses.append(jnp.concatenate(block, axis=0))
        columns.append(jnp.where(col_iota == q, BF16(1), zero))


def deposit(slots, acc):
    masses, columns = [], []
    for static, moves in slots:
        factors(static, moves, masses, columns)
    acc[...] += lax.dot_general(
        jnp.concatenate(masses, axis=1),
        jnp.concatenate(columns, axis=1),
        (((1,), (1,)), ((), ())),
        preferred_element_type=F32,
    )


class Place:
    def __init__(self, n_rows, n_cols):
        self.n_rows, self.n_cols = n_rows, n_cols
        self.row, self.col = lax.axis_index("rows"), lax.axis_index("cols")
        self.has_up, self.has_down = self.row > 0, self.row < n_rows - 1
        self.has_left, self.has_right = self.col > 0, self.col < n_cols - 1
        self.lane = lax.broadcasted_iota(jnp.int32, (8, 128), 1)
        self.sub = lax.broadcasted_iota(jnp.int32, (8, 128), 0)
        self.lane_right = self.lane < jnp.where(self.has_right, 8, 0)
        self.lane_left = self.lane >= jnp.where(self.has_left, 120, 128)
        self.side_in = self.lane_right | self.lane_left

    def at(self, dr, dc):
        n_rows, n_cols = self.n_rows, self.n_cols
        return (lax.rem(self.row + dr + n_rows, n_rows), lax.rem(self.col + dc + n_cols, n_cols))

    def there(self, dr, dc=0):
        rows_ok = {-1: self.has_up, 0: None, 1: self.has_down}[dr]
        cols_ok = {-1: self.has_left, 0: None, 1: self.has_right}[dc]
        if rows_ok is None or cols_ok is None:
            return cols_ok if rows_ok is None else rows_ok
        return rows_ok & cols_ok

    def greet(self, peers):
        barrier = pltpu.get_barrier_semaphore()
        count = jnp.int32(0)
        for cond, to in peers:
            only(cond, lambda to=to: pl.semaphore_signal(
                barrier, inc=1, device_id=to, device_id_type=pl.DeviceIdType.MESH
            ))
            count = count + (1 if cond is None else cond.astype(jnp.int32))
        return barrier, count

    def finish(self, copies, targets):
        for c, (dr, dc) in zip(copies, targets):
            only(self.there(dr, dc), c.wait_send)
            only(self.there(-dr, -dc), c.wait_recv)


def only(cond, act):
    if cond is None:
        act()
    else:
        pl.when(cond)(act)


def remote(src, dst, s, r, to):
    return pltpu.make_async_remote_copy(
        src_ref=src, dst_ref=dst, send_sem=s, recv_sem=r,
        device_id=to, device_id_type=pl.DeviceIdType.MESH,
    )


def halo_kernel(
    n_rows, n_cols,
    u_in, m_in, off_in, w_in, dest_in, end_in,
    um, off, frac, static_send, placing_out, mass_out,
    off_raw, w, ends, dest, side_send, side_recv, corner_recv,
    load_sem, halo_s, halo_r,
):
    at_ = Place(n_rows, n_cols)
    at, there, lane = at_.at, at_.there, at_.lane
    row, col, side_in = at_.row, at_.col, at_.side_in
    has_up, has_down = at_.has_up, at_.has_down
    loads = [
        (u_in, um.at[0, pl.ds(0, RT), :, pl.ds(0, 512)]),
        (m_in, um.at[1, pl.ds(0, RT), :, pl.ds(0, 512)]),
        (dest_in, dest), (w_in, w), (end_in, ends), (off_in, off_raw),
    ]
    loads = [pltpu.make_async_copy(a, b, load_sem.at[i]) for i, (a, b) in enumerate(loads)]
    for c in loads:
        c.start()
    halo_to = [(-1, 0), (1, 0), (-1, -1), (-1, 1), (1, -1), (1, 1), (0, -1), (0, 1)]
    barrier, greeted = at_.greet([(there(*to), at(*to)) for to in halo_to])
    for c in loads[:2]:
        c.wait()
    for v in range(2):
        first = um[v, 0:RT, :, 0:128].reshape(128, 128).T
        last = um[v, 0:RT, :, 384:512].reshape(128, 128).T
        side_send[0, v] = first[0:8]
        side_send[1, v] = last[120:128]
    pl.semaphore_wait(barrier, greeted)

    halo = [
        remote(um.at[:, 0, :, pl.ds(0, 512)], um.at[:, RT, :, pl.ds(0, 512)], halo_s.at[0], halo_r.at[0], at(-1, 0)),
        remote(um.at[:, RT - 1, :, pl.ds(0, 512)], um.at[:, RT + 1, :, pl.ds(0, 512)], halo_s.at[1], halo_r.at[1], at(1, 0)),
        remote(um.at[:, 0, :, pl.ds(0, 128)], corner_recv.at[0], halo_s.at[2], halo_r.at[2], at(-1, -1)),
        remote(um.at[:, 0, :, pl.ds(384, 128)], corner_recv.at[1], halo_s.at[3], halo_r.at[3], at(-1, 1)),
        remote(um.at[:, RT - 1, :, pl.ds(0, 128)], corner_recv.at[2], halo_s.at[4], halo_r.at[4], at(1, -1)),
        remote(um.at[:, RT - 1, :, pl.ds(384, 128)], corner_recv.at[3], halo_s.at[5], halo_r.at[5], at(1, 1)),
        remote(side_send.at[0], side_recv.at[0], halo_s.at[6], halo_r.at[6], at(0, -1)),
        remote(side_send.at[1], side_recv.at[1], halo_s.at[7], halo_r.at[7], at(0, 1)),
    ]
    for c, to in zip(halo, halo_to):
        only(there(*to), c.start)

    loads[3].wait()
    mass_out[...] = w[0] + w[1] + w[2] + w[3]

    loads[2].wait()
    d = dest[...]
    along = jnp.broadcast_to(d.astype(F32), (32, 32))
    same = along == along.T
    order_b = lax.broadcasted_iota(jnp.int32, (32, 32), 0)
    order_a = lax.broadcasted_iota(jnp.int32, (32, 32), 1)
    rank = jnp.sum(jnp.where(same & (order_b < order_a), 1.0, 0.0), axis=0, keepdims=True).astype(jnp.int32)
    slot = ((d >> 2) - row + 1) * (n_cols * CAP) + (((d & 3) - col) & 3) * CAP + rank
    slot_iota = lax.broadcasted_iota(jnp.int32, (GROUP * CAP, 32), 0)
    placing = jnp.where(slot_iota == slot, 1.0, 0.0).astype(BF16)
    placing_out[...] = placing

    loads[4].wait()
    block_static = jnp.concatenate(
        [ends[...].reshape(32, 128).astype(F32), w[...].reshape(32, 128)], axis=1
    )
    placed = place(placing, block_static)
    for n in range(2):
        static_send[:, n] = placed[:, 128 * n : 128 * n + 128].reshape(GROUP, CAP, 128)
    loads[5].wait()
    for b in range(32):
        both = off_raw[:, 128 * b : 128 * b + 128]
        for n in range(2):
            off[n, b // 8, b % 8 : b % 8 + 1, :] = both[n : n + 1]
    for n in range(2):
        frac[n] = 0.5 + 0.45 * jnp.tanh(off[n])

    at_.finish(halo, halo_to)
    zero_mid = jnp.zeros((112, 128), F32)
    for v in range(2):
        strip = jnp.concatenate([side_recv[0, v], zero_mid, side_recv[1, v]], axis=0).T
        strip = strip.reshape(RT, 8, 128)
        um[v, 0:RT, :, 512:640] = jnp.where(side_in, strip, 0.0) if v == 0 else strip
        below = jnp.where(lane < 64, corner_recv[0, v], corner_recv[1, v])
        above = jnp.where(lane < 64, corner_recv[2, v], corner_recv[3, v])
        if v == 0:
            below = jnp.where(side_in & has_down, below, 0.0)
            above = jnp.where(side_in & has_up, above, 0.0)
            um[0, RT, :, 0:512] = jnp.where(has_down, um[0, RT, :, 0:512], 0.0)
            um[0, RT + 1, :, 0:512] = jnp.where(has_up, um[0, RT + 1, :, 0:512], 0.0)
        um[v, RT, :, 512:640] = below
        um[v, RT + 1, :, 512:640] = above


def kernel(
    n_rows, n_cols,
    um, off, frac, static_send, placing_in, mass_in, cells_in,
    value_out, density_out,
    ua, ub, grid, relaxed, cells, corners, table,
    static_recv, move_send, move_recv,
    acc,
    g_side_l, g_side_r, g_down, g_from_u, g_from_d, g_from_l, g_from_r, g_from_ul, g_from_ur, g_from_dl, g_from_dr,
    red_send, red_recv,
    load_sem,
    static_s, static_r, move_s, move_r, g_s, g_r, red_s, red_r,
):
    at_ = Place(n_rows, n_cols)
    at, there, finish, lane, sub = at_.at, at_.there, at_.finish, at_.lane, at_.sub
    row, col, side_in = at_.row, at_.col, at_.side_in
    has_up, has_down, has_left, has_right = at_.has_up, at_.has_down, at_.has_left, at_.has_right
    lane_right, lane_left = at_.lane_right, at_.lane_left
    row_in = (has_down, has_up)
    load = pltpu.make_async_copy(cells_in, cells, load_sem.at[0])
    load.start()

    group = [(dr, k) for dr in (-1, 0, 1) for k in range(n_cols)]
    near = row % 8
    base = row - near
    row_peers = [base + (near + j) % 8 for j in range(1, 8)]
    far_peers = [lax.rem(row + 8 * j, n_rows) for j in range(1, 4)]
    barrier, greeted = at_.greet(
        [(there(dr), at(dr, k)) for dr, k in group if (dr, k) != (0, 0)]
        + [(None, (p, col)) for p in row_peers + far_peers]
    )
    placing = placing_in[...]
    zero_mid = jnp.zeros((112, 128), F32)

    for v in range(2):
        for s_, cond in ((2, has_up), (0, has_down)):

            @pl.when(jnp.logical_not(cond))
            def _(s_=s_, v=v):
                missing = jnp.zeros((n_cols, 2, CAP, 128), F32)
                if v == 0:
                    static_recv[n_cols * s_ : n_cols * s_ + n_cols] = missing
                for i in range(ITERS // 2):
                    move_recv[v * (ITERS // 2) + i, n_cols * s_ : n_cols * s_ + n_cols] = missing
    for n in range(2):
        static_recv[SELF, n] = static_send[SELF, n]

    red_send[0] = mass_in[...]
    stages = [
        [(0, at(0, k)) for k in range(1, n_cols)],
        [(1, (p, col)) for p in row_peers],
        [(2, (p, col)) for p in far_peers],
    ]
    red, count = [], 0
    for stage in stages:
        copies = []
        for s, to in stage:
            copies.append(remote(red_send.at[s], red_recv.at[count], red_s.at[count], red_r.at[count], to))
            count += 1
        red.append(copies)
    def reduce_stage(s):
        total, first = red_send[s], sum(len(x) for x in red[:s])
        for i, c in enumerate(red[s]):
            c.wait()
            total = total + red_recv[first + i]
        if s + 1 < len(red):
            red_send[s + 1] = total
            for c in red[s + 1]:
                c.start()
        return total

    def send_group(send, recv, ss, rs):
        copies = {}
        for i, (dr, k) in enumerate(group):
            if i != SELF:
                copies[i] = remote(send.at[i], recv.at[i], ss.at[i], rs.at[i], at(dr, k))
                only(there(dr), copies[i].start)
        return copies

    def exchange(it):
        full = it + 1 < ITERS
        ss, rs = g_s.at[it], g_r.at[it]
        zero = jnp.zeros((8, 128), F32)

        def assemble(t):
            for j in range(LT + 1):
                js, before = slice(128 * j, 128 * j + 128), slice(128 * j - 128, 128 * j)
                here = beside = prior = zero
                if t < RT:
                    r = [slice(128 * n + 8 * t, 128 * n + 8 * t + 8) for n in range(4)]
                    if j < LT:
                        here = acc[r[0], js] + acc[r[1], js]
                        beside = pltpu.roll(acc[r[2], js] + acc[r[3], js], 1, 1)
                    if j > 0:
                        prior = pltpu.roll(acc[r[2], before] + acc[r[3], before], 1, 1)
                elif t == RT:
                    if j < LT:
                        x = acc[512:520, js]
                        here = jnp.where(sub == 0, x + pltpu.roll(x, 7, 0), 0.0)
                        beside = pltpu.roll(jnp.where(sub == 0, pltpu.roll(x, 6, 0) + pltpu.roll(x, 5, 0), 0.0), 1, 1)
                    if j > 0:
                        x = acc[512:520, before]
                        prior = pltpu.roll(jnp.where(sub == 0, pltpu.roll(x, 6, 0) + pltpu.roll(x, 5, 0), 0.0), 1, 1)
                grid[t, :, js] = here + jnp.where(lane == 0, prior, beside)

        for t in (0, RT - 1, RT):
            assemble(t)
        for j in range(LT + 1):
            js = slice(128 * j, 128 * j + 128)
            g_down[it, :, js] = jnp.where(sub == 0, grid[RT, :, js], grid[RT - 1, :, js])
        sends = [
            (g_down.at[it], g_from_u.at[it], (1, 0)),
            (g_down.at[it, :, pl.ds(384, 256)], g_from_ul.at[it], (1, 1)),
        ]
        if full:
            sends += [
                (grid.at[0], g_from_d, (-1, 0)),
                (g_down.at[it, :, pl.ds(0, 128)], g_from_ur, (1, -1)),
                (grid.at[0, :, pl.ds(384, 256)], g_from_dl, (-1, 1)),
                (grid.at[0, :, pl.ds(0, 128)], g_from_dr, (-1, -1)),
            ]
        copies, targets = [], []

        def send(src, dst, to):
            n = len(copies)
            copies.append(remote(src, dst, ss.at[n], rs.at[n], at(*to)))
            targets.append(to)
            only(there(*to), copies[-1].start)

        for x in sends:
            send(*x)
        for t in list(range(1, RT - 1)) + [RT + 1]:
            assemble(t)
        fourth = grid[0:RT, :, 512:640].reshape(128, 128).T
        if full:
            g_side_r[it, 0] = grid[0:RT, :, 384:512].reshape(128, 128).T[120:128]
        g_side_r[it, 1] = fourth[0:8]
        g_side_r[it, 2] = grid[RT, :, 384:512]
        g_side_r[it, 3] = grid[RT, :, 512:640]
        if full:
            first = grid[0:RT, :, 0:128].reshape(128, 128).T
            g_side_l[0] = first[0:8]
            g_side_l[1] = grid[RT, :, 0:128]
        sent = pl.ds(0, 4) if full else pl.ds(1, 3)
        send(g_side_r.at[it, sent], g_from_l.at[it, sent], (0, 1))
        if full:
            send(g_side_l, g_from_r, (0, -1))
        return copies, targets

    def gather_edges(it):
        full = it + 1 < ITERS
        top = sub == 0
        left0 = (lane == 0) & has_left
        l4, z = slice(512, 640), 0.0
        above = (sub > 0) & has_up
        for j in range(LT + 1):
            js = slice(128 * j, 128 * j + 128)
            grid[0, :, js] += jnp.where(top & has_up, g_from_u[it, :, js], z)
            if full:
                grid[RT + 1, :, js] = jnp.where(above, g_from_u[it, :, js], z)
        if full:
            grid[RT] += jnp.where(has_down, g_from_d[...], z)
        if full:
            strip = jnp.concatenate([g_from_r[0], zero_mid, g_from_l[it, 0]], axis=0).T.reshape(RT, 8, 128)
            grid[0:RT, :, l4] += jnp.where(side_in, strip, z)
        spill = jnp.concatenate([g_from_l[it, 1], jnp.zeros((120, 128), F32)], axis=0).T.reshape(RT, 8, 128)
        grid[0:RT, :, 0:128] += jnp.where(left0, spill, z)
        edge = jnp.where(lane_left, g_from_l[it, 2], z)
        if full:
            edge = edge + jnp.where(lane_right, g_from_r[1], z)
        grid[RT, :, l4] += edge
        grid[RT, :, 0:128] += jnp.where(left0, g_from_l[it, 3], z)
        corner = jnp.where(lane_left, g_from_ul[it, :, 0:128], z)
        if full:
            corner = corner + jnp.where(lane_right, g_from_ur[...], z)
            grid[RT + 1, :, l4] += jnp.where(above, corner, z)
            grid[RT + 1, :, 0:128] += jnp.where(left0 & above, g_from_ul[it, :, 128:256], z)
        grid[0, :, l4] += jnp.where(top & has_up, corner, z)
        grid[0, :, 0:128] += jnp.where(top & left0 & has_up, g_from_ul[it, :, 128:256], z)
        if full:
            corner = jnp.where(lane_left, g_from_dl[:, 0:128], z) + jnp.where(lane_right, g_from_dr[...], z)
            grid[RT, :, l4] += jnp.where(has_down, corner, z)
            grid[RT, :, 0:128] += jnp.where(left0 & has_down, g_from_dl[:, 128:256], z)
        for j in range(LT + 1):
            js = slice(128 * j, 128 * j + 128)
            folded = pltpu.roll(grid[RT, :, js], 7, 0)
            grid[RT - 1, :, js] += jnp.where((sub == 7) & jnp.logical_not(has_down), folded, z)
        for t in range(RT + 2 if full else RT):
            folded = pltpu.roll(grid[t, :, l4], 127, 1)
            grid[t, :, 384:512] += jnp.where((lane == 127) & jnp.logical_not(has_right), folded, z)

    scale = None
    for it in range(ITERS):
        hjb = functools.partial(hjb_step, lane=lane, sub=sub, row_in=row_in, side_in=side_in)
        den = um.at[1] if it == 0 else relaxed
        hjb(um.at[0], ua, den)
        hjb(ua, ub, den)
        hjb(ub, ua, den)
        hjb(ua, ub, den)
        if it == 0:
            load.wait()
        slopes(ub, ua, table, lane, sub)
        sample(table, ub, ua, cells, corners)
        if it == 0:
            pl.semaphore_wait(barrier, greeted)
            static_copies = send_group(static_send, static_recv, static_s, static_r)
            for c in red[0]:
                c.start()
        dx0, dx1, dy0 = corners[0], corners[1], corners[2]
        fx, fy = frac[0], frac[1]
        gx = (1.0 - fy) * dx0 + fy * dx1
        gy = (1.0 - fx) * dy0 + fx * (dy0 + (dx1 - dx0))
        hx = 0.5 + 0.45 * jnp.tanh(off[0] - gx)
        hy = 0.5 + 0.45 * jnp.tanh(off[1] - gy)
        placed = place(placing, jnp.concatenate([hx.reshape(32, 128), hy.reshape(32, 128)], axis=1))
        for n in range(2):
            move_send[it, :, n] = placed[:, 128 * n : 128 * n + 128].reshape(GROUP, CAP, 128)
            move_recv[it, SELF, n] = placed[SELF * CAP : SELF * CAP + CAP, 128 * n : 128 * n + 128]
        move_copies = send_group(move_send.at[it], move_recv.at[it], move_s.at[it], move_r.at[it])
        acc[...] = jnp.zeros_like(acc)
        if it + 1 == ITERS:
            value_out[...] = ub[0:RT, :, 0:512]

        step = 4 * (2 * lax.rem(row, 2) - 1)
        kinds = sum(kind * 3**i for i, (kind, _) in enumerate(ORDER))
        dists = sum(k * 4**i for i, (_, k) in enumerate(ORDER))

        def arrive(i, kinds, dists):
            kind, k = lax.rem(kinds, 3) - 1, lax.rem(dists, 4)
            s = SELF + kind * step + k
            from_up, from_down = kind * step > 0, kind * step < 0

            def wait():
                remote(move_send.at[it, s], move_recv.at[it, s], move_s.at[it, s], move_r.at[it, s], at(0, 1)).wait_recv()
                if it == 0:
                    remote(static_send.at[s], static_recv.at[s], static_s.at[s], static_r.at[s], at(0, 1)).wait_recv()

            absent = (from_up & (row == 0)) | (from_down & (row == n_rows - 1))
            pl.when((i > 0) & jnp.logical_not(absent))(wait)
            return s, kinds // 3, dists // 4

        def arrivals(first, batch, i, carry):
            slots = []
            for j in range(batch):
                s, *carry = arrive(first + batch * i + j, *carry)
                slots.append((static_recv[s], move_recv[it, s]))
            deposit(slots, acc)
            return tuple(carry)

        carry = (jnp.int32(kinds), jnp.int32(dists))
        for n, (first, count, batch) in enumerate(BATCHES[it]):
            if n > 0:
                reduce_stage(0)
            carry = lax.fori_loop(0, count, functools.partial(arrivals, first, batch), carry)
        copies, targets = exchange(it)
        if it == 0:
            reduce_stage(1)
        for sent in (move_copies, static_copies) if it == 0 else (move_copies,):
            for i, c in sent.items():
                only(there(group[i][0]), c.wait_send)
        finish(copies, targets)
        if it == 0:
            total = reduce_stage(2)
            scale = jnp.float32(n_rows * n_cols * 128 * 512) / jnp.sum(total, keepdims=True)
        gather_edges(it)
        if it + 1 < ITERS:
            relaxed[...] = 0.5 * um[1] + 0.5 * (grid[...] * scale.reshape(1, 1, 1))
        else:
            density_out[...] = 0.5 * relaxed[0:RT, :, 0:512] + 0.5 * (grid[0:RT, :, 0:512] * scale.reshape(1, 1, 1))


def write_out(value, density, value_out, density_out, sems):
    copies = [
        pltpu.make_async_copy(value, value_out, sems.at[0]),
        pltpu.make_async_copy(density, density_out, sems.at[1]),
    ]
    for c in copies:
        c.start()
    for c in copies:
        c.wait()


def body(n_rows, n_cols, terminal_value, density_start, start_cells, offsets, weights, dest_tiles, end_cells):
    any_ = pl.BlockSpec(memory_space=pltpu.HBM)
    vmem = pltpu.VMEM
    dma = pltpu.SemaphoreType.DMA
    tile = jax.ShapeDtypeStruct((RT, 8, 512), F32)
    whole = pl.BlockSpec(memory_space=pltpu.VMEM)
    stay = lambda x: pltpu.with_memory_space_constraint(x, pltpu.HBM)
    shape = jax.ShapeDtypeStruct
    prepared = pl.pallas_call(
        functools.partial(halo_kernel, n_rows, n_cols),
        out_shape=(
            shape((2, RT + 2, 8, 640), F32), shape((2, 4, 8, 128), F32), shape((2, 4, 8, 128), F32),
            shape((GROUP, 2, CAP, 128), F32), shape((GROUP * CAP, 32), BF16), shape((8, 128), F32),
        ),
        in_specs=[any_] * 6,
        out_specs=(whole,) * 6,
        scratch_shapes=[
            vmem((2, 4096), F32), vmem((4, 8, 128), F32), vmem((4, 8, 128), jnp.int32), vmem((1, 32), jnp.int32),
            vmem((2, 2, 8, 128), F32), vmem((2, 2, 8, 128), F32), vmem((4, 2, 8, 128), F32),
            dma((6,)), dma((8,)), dma((8,)),
        ],
        compiler_params=pltpu.CompilerParams(collective_id=1, has_side_effects=True, vmem_limit_bytes=8 << 20),
        name="halos",
    )(
        stay(terminal_value.reshape(RT, 8, 512)),
        stay(density_start.reshape(RT, 8, 512)),
        stay(offsets),
        stay(weights.reshape(4, 8, 128)),
        stay(dest_tiles.reshape(1, 32)),
        stay(end_cells.reshape(4, 8, 128)),
    )
    value, density = pl.pallas_call(
        functools.partial(kernel, n_rows, n_cols),
        out_shape=(tile, tile),
        in_specs=[whole] * 6 + [any_],
        out_specs=(whole, whole),
        scratch_shapes=[
            vmem((RT + 2, 8, 640), F32), vmem((RT + 2, 8, 640), F32), vmem((RT + 2, 8, 640), F32), vmem((RT + 2, 8, 640), F32),
            vmem((4, 8, 128), jnp.int32), vmem((3, 4, 8, 128), F32), vmem((1040, 256), BF16),
            vmem((GROUP, 2, CAP, 128), F32), vmem((ITERS, GROUP, 2, CAP, 128), F32), vmem((ITERS, GROUP, 2, CAP, 128), F32),
            vmem((528, 512), F32),
            vmem((2, 8, 128), F32), vmem((ITERS, 4, 8, 128), F32), vmem((ITERS, 8, 640), F32),
            vmem((ITERS, 8, 640), F32), vmem((8, 640), F32), vmem((ITERS, 4, 8, 128), F32), vmem((2, 8, 128), F32),
            vmem((ITERS, 8, 256), F32), vmem((8, 128), F32), vmem((8, 256), F32), vmem((8, 128), F32),
            vmem((3, 8, 128), F32), vmem((13, 8, 128), F32),
            dma((1,)),
            dma((GROUP,)), dma((GROUP,)),
            dma((ITERS, GROUP)), dma((ITERS, GROUP)), dma((ITERS, 8)), dma((ITERS, 8)), dma((13,)), dma((13,)),
        ],
        compiler_params=pltpu.CompilerParams(collective_id=0, has_side_effects=True, vmem_limit_bytes=20 << 20),
        name="crowd",
    )(*prepared, stay(start_cells.reshape(4, 8, 128)))
    value, density = pl.pallas_call(
        write_out,
        out_shape=(tile, tile),
        in_specs=[pl.BlockSpec(memory_space=pltpu.VMEM)] * 2,
        out_specs=(pl.BlockSpec(memory_space=pltpu.HBM),) * 2,
        scratch_shapes=[dma((2,))],
        compiler_params=pltpu.CompilerParams(vmem_limit_bytes=1 << 20),
        name="write_out",
    )(value, density)
    return value.reshape(128, 512), density.reshape(128, 512)


def solution(mesh):
    both = ("rows", "cols")
    return jax.shard_map(
        functools.partial(body, mesh.shape["rows"], mesh.shape["cols"]),
        mesh=mesh,
        in_specs=(P("rows", "cols"), P("rows", "cols"), P(both), P(None, both), P(both), P(both), P(both)),
        out_specs=(P("rows", "cols"), P("rows", "cols")),
        check_vma=False,
    )
```
